256 devices in a mesh: row: 16 (over x_hi, y, core), col: 16 (over x_lo, z).
Axes of the slice: x: 4 (x_hi: 2, x_lo: 2; x = x_hi * 2 + x_lo), y: 4, z: 8, core: 2. Of those that a mesh axis runs over, the one named last changes fastest.
Arguments:
- object_field: float32 [2, 6144, 6144], P(None, 'row', 'col'), may hold values from -4 to 4
- illumination: float32 [2, 256, 256], replicated, may hold values from -4 to 4
- measured: float32 [16, 16, 8, 256, 256], P('row', 'col'), may hold values from 0.05 to 4
- positions: int32 [16, 16, 8, 2], P('row', 'col'), may hold values from 0 to 383
- frame_counts: int32 [16, 16], P('row', 'col'), may hold values from 1 to 8, as said below
- first_count: int32 [16, 16], P('row', 'col'), may hold values from 0 to 4
Outputs:
- new_object: float32 [2, 6144, 6144], P(None, 'row', 'col')
- new_illumination: float32 [2, 256, 256], replicated
The draws below stay inside these ranges and needn't reach their ends.
Inputs may be any that keep to these rules, and one draw needn't show every extreme that they name: `frame_counts`: some tile has exactly 8 live frames in every draw; slots from a tile's count on are unused.
All inputs are finite; a program needn't handle non-finite values.
Results may differ from the reference program's by a relative error of at most 0.0003.
Values sent between devices are 32-bit elements; how exact they have to be, the bound alone decides.
A program may use at most 64 MiB of HBM per device.

```python
import math
import jax
import jax.numpy as jnp
from jax import lax

TILE = 384
PROBE = 256
FRAMES = 8
TR = 16
TC = 16
NX = 6144
NY = 6144


def draw_frame_counts(key, part):
    key_drawn = jax.random.fold_in(key, 101)
    key_heavy = jax.random.fold_in(key, 202)
    key_chosen = jax.random.fold_in(key, 303)
    lowest = max(1, FRAMES // 4)
    highest = max(lowest, FRAMES // 2)
    drawn = jax.random.randint(key_drawn, (TR, TC), lowest, highest + 1)
    is_heavy = jax.random.randint(key_heavy, (TR, TC), 0, 8) == 0
    chosen = jax.random.randint(key_chosen, (), 0, TR * TC)
    flat_index = jnp.arange(TR * TC, dtype=jnp.int32).reshape(TR, TC)
    return jnp.where(is_heavy | (flat_index == chosen), FRAMES, drawn).astype(jnp.int32)


def touch_ends(result, own_key, smallest, largest):
    longest = result.shape.index(max(result.shape))
    spots = []
    for shift in (0, 1):
        where = [jax.random.randint(jax.random.fold_in(own_key, axis), (), 0, length) for axis, length in enumerate(result.shape)]
        where[longest] = (where[longest] + shift) % result.shape[longest]
        spots.append(tuple(where))
    return result.at[spots[0]].set(smallest).at[spots[1]].set(largest)


def block_levels(stream_key, extent, cuts, smallest, largest):
    def one(axis_at, blocks):
        steps = jax.random.uniform(jax.random.fold_in(jax.random.fold_in(stream_key, 6), axis_at), (blocks,), jnp.float32, smallest / len(cuts), largest / len(cuts))
        return jnp.repeat(jnp.exp(steps), extent[axis_at] // blocks).reshape((-1,) + (1,) * (len(extent) - axis_at - 1))

    level = one(*cuts[0])
    for cut in cuts[1:]:
        level = level * one(*cut)
    return level


def noise(stream_key, extent, scale, reach, split=(), kind=jnp.bfloat16):
    entries = scale * jax.random.normal(stream_key, extent, jnp.float32)
    if split:
        entries = entries * block_levels(stream_key, extent, split, -0.22, 0.18)
    return jnp.clip(entries, -reach, reach).astype(kind)


def setup_inputs(seed: int = 0) -> dict:
    streams_of = jax.random.split(jax.random.key(seed), 7)
    return {
        "object_field": noise(streams_of[0], (2, NX, NY), 0.7, 4.0, ((1, 16), (2, 16)), jnp.float32),
        "illumination": noise(streams_of[1], (2, PROBE, PROBE), 0.7, 4.0, (), jnp.float32),
        "measured": jnp.clip(jnp.exp(math.log(4.0) - 4.3820266 * jax.random.uniform(streams_of[2], (TR, TC, FRAMES, PROBE, PROBE), jnp.float32) ** block_levels(streams_of[2], (TR, TC, FRAMES, PROBE, PROBE), ((0, 16), (1, 16)), -0.2, 0.2)), 0.05, 4.0),
        "positions": touch_ends(jax.random.randint(streams_of[3], (TR, TC, FRAMES, 2), 0, TILE), jax.random.fold_in(streams_of[3], 1), 0, TILE - 1).astype(jnp.int32),
        "frame_counts": draw_frame_counts(jax.random.fold_in(streams_of[6], 71), 0),
        "first_count": touch_ends(jax.random.randint(streams_of[5], (TR, TC), 0, FRAMES // 2 + 1), jax.random.fold_in(streams_of[5], 1), 0, (FRAMES // 2 + 1) - 1).astype(jnp.int32),
    }


def dft_tables(length):
    index_row = jnp.arange(length, dtype=jnp.int32)
    product = index_row[:, None] * index_row[None, :] % length
    angle = product.astype(jnp.float32) * (2.0 * math.pi / length)
    scale = 1.0 / math.sqrt(length)
    return (jnp.cos(angle) * scale, -jnp.sin(angle) * scale)

def matmul(left, right):
    return jnp.dot(left, right, precision=lax.Precision.HIGHEST)

def complex_product(left_real, left_imag, right_real, right_imag):
    return (matmul(left_real, right_real) - matmul(left_imag, right_imag), matmul(left_real, right_imag) + matmul(left_imag, right_real))

def frame_gradients(object_patch, illumination, intensity, tables):
    table_real, table_imag = tables
    patch_real, patch_imag = (object_patch[0], object_patch[1])
    probe_real, probe_imag = (illumination[0], illumination[1])
    exit_real = probe_real * patch_real - probe_imag * patch_imag
    exit_imag = probe_real * patch_imag + probe_imag * patch_real
    half_real, half_imag = complex_product(table_real, table_imag, exit_real, exit_imag)
    wave_real, wave_imag = complex_product(half_real, half_imag, table_real, table_imag)
    residue = wave_real * wave_real + wave_imag * wave_imag - intensity
    back_real, back_imag = complex_product(table_real, -table_imag, residue * wave_real, residue * wave_imag)
    grad_real, grad_imag = complex_product(back_real, back_imag, table_real, -table_imag)
    object_term = jnp.stack([probe_real * grad_real + probe_imag * grad_imag, probe_real * grad_imag - probe_imag * grad_real])
    probe_term = jnp.stack([patch_real * grad_real + patch_imag * grad_imag, patch_real * grad_imag - patch_imag * grad_real])
    return (object_term, probe_term)

def reference(object_field, illumination, measured, positions, frame_counts, first_count):
    tables = dft_tables(PROBE)
    step_size = 0.5 / math.sqrt(TR * TC * FRAMES)
    anchor = jnp.zeros((), jnp.int32)
    for batch_index in range(2):
        padded = jnp.pad(object_field, ((0, 0), (0, PROBE), (0, PROBE)))

        def add_frame(slot_index, running):
            slot_index = jnp.asarray(slot_index).astype(jnp.int32)
            tile_row = slot_index // (TC * FRAMES)
            tile_col = slot_index // FRAMES % TC
            frame_slot = slot_index % FRAMES
            live_frames = frame_counts[tile_row, tile_col]
            first_frames = jnp.minimum(first_count[tile_row, tile_col], live_frames)
            if batch_index == 0:
                is_live = frame_slot < first_frames
            else:
                is_live = (frame_slot >= first_frames) & (frame_slot < live_frames)

            def accumulate(state):
                grad_object, grad_probe = state
                row_start = (tile_row * TILE + positions[tile_row, tile_col, frame_slot, 0]).astype(jnp.int32)
                col_start = (tile_col * TILE + positions[tile_row, tile_col, frame_slot, 1]).astype(jnp.int32)
                object_patch = lax.dynamic_slice(padded, (anchor, row_start, col_start), (2, PROBE, PROBE))
                intensity = measured[tile_row, tile_col, frame_slot]
                object_term, probe_term = frame_gradients(object_patch, illumination, intensity, tables)
                current = lax.dynamic_slice(grad_object, (anchor, row_start, col_start), (2, PROBE, PROBE))
                grad_object = lax.dynamic_update_slice(grad_object, current + object_term, (anchor, row_start, col_start))
                return (grad_object, grad_probe + probe_term)

            def unchanged(state):
                return state
            return lax.cond(is_live, accumulate, unchanged, running)
        start_state = (jnp.zeros_like(padded), jnp.zeros_like(illumination))
        grad_object, grad_probe = lax.fori_loop(0, TR * TC * FRAMES, add_frame, start_state)
        object_field = object_field - 0.1 * grad_object[:, :NX, :NY]
        illumination = illumination - step_size * grad_probe
    return (object_field, illumination)
```

```python
import functools
import math

import jax
import jax.numpy as jnp
import numpy as np
from jax import lax
from jax.experimental import pallas as pl
from jax.experimental.pallas import tpu as pltpu
from jax.sharding import PartitionSpec as P

MESH = pl.DeviceIdType.MESH
TILE, PROBE, EXT = 384, 256, 640
N_ROW = N_COL = 16
F32, BF16 = jnp.float32, jnp.bfloat16
VMEM_SPEC = pl.BlockSpec(memory_space=pltpu.VMEM)
SMEM_SPEC = pl.BlockSpec(memory_space=pltpu.SMEM)
ANY_SPEC = pl.BlockSpec(memory_space=pl.ANY)


def split_bf16(table):
    high = table.astype(np.float32).astype(BF16)
    low = (table - high.astype(np.float64)).astype(np.float32).astype(BF16)
    return high, low


def dft_tables():
    n = np.arange(128)[:, None]
    parts = []
    for parity in (0, 1):
        k = 2 * np.arange(128)[None, :] + parity
        angle = ((n * k) % 256) * (2.0 * np.pi / 256.0)
        c, s = np.cos(angle) / 16.0, np.sin(angle) / 16.0
        table = np.block([[c, -s], [s, c]])
        parts.append((split_bf16(table), split_bf16(table.T)))
    order = []
    for transposed in (0, 1):
        for parity in (0, 1):
            order.extend(parts[parity][transposed])
    return np.stack(order)


def deinterleave_table():
    table = np.zeros((256, 256), np.float32)
    index = np.arange(128)
    table[2 * index, index] = 1.0
    table[2 * index + 1, 128 + index] = 1.0
    return table.astype(BF16)


def place():
    row, col = lax.axis_index("row"), lax.axis_index("col")
    return row, col


def remote(src, dst, send_sem, recv_sem, device):
    return pltpu.make_async_remote_copy(
        src_ref=src, dst_ref=dst, send_sem=send_sem, recv_sem=recv_sem,
        device_id=device, device_id_type=MESH,
    )


def greet_neighbours(barrier, row, col):
    for has, device in (
        (row > 0, (row - 1, col)),
        (row < N_ROW - 1, (row + 1, col)),
        (col > 0, (row, col - 1)),
        (col < N_COL - 1, (row, col + 1)),
    ):
        @pl.when(has)
        def _(device=device):
            pl.semaphore_signal(barrier, inc=1, device_id=device, device_id_type=MESH)


def neighbour_count(row, col):
    one, none = jnp.int32(1), jnp.int32(0)
    has = (row > 0, row < N_ROW - 1, col > 0, col < N_COL - 1)
    return sum(jnp.where(h, one, none) for h in has)


LEFT_CHUNKS = ((0, 0, 256), (1, 0, 256), (0, 256, 128), (1, 256, 128))


class Halo:
    def __init__(self, ext, left_sems, up_sems, corner_sems, row, col):
        self.ext, self.row, self.col = ext, row, col
        self.left_sems, self.up_sems, self.corner_sems = left_sems, up_sems, corner_sems

    def left(self, index):
        channel, start, rows = LEFT_CHUNKS[index]
        return remote(
            self.ext.at[channel, pl.ds(0, 2), pl.ds(start, rows), :],
            self.ext.at[channel, pl.ds(3, 2), pl.ds(start, rows), :],
            self.left_sems.at[0, index], self.left_sems.at[1, index],
            (self.row, jnp.maximum(self.col - 1, 0)),
        )

    def up(self, channel):
        return remote(
            self.ext.at[channel, pl.ds(0, 3), pl.ds(0, 256), :],
            self.ext.at[channel, pl.ds(0, 3), pl.ds(384, 256), :],
            self.up_sems.at[0, channel], self.up_sems.at[1, channel],
            (jnp.maximum(self.row - 1, 0), self.col),
        )

    def corner(self, channel):
        return remote(
            self.ext.at[channel, pl.ds(3, 2), pl.ds(0, 256), :],
            self.ext.at[channel, pl.ds(3, 2), pl.ds(384, 256), :],
            self.corner_sems.at[0, channel], self.corner_sems.at[1, channel],
            (jnp.maximum(self.row - 1, 0), self.col),
        )

    def clear_edges(self):
        @pl.when(self.col == N_COL - 1)
        def _():
            for channel in range(2):
                for block in (3, 4):
                    self.ext[channel, block] = jnp.zeros((EXT, 128), F32)

        @pl.when(self.row == N_ROW - 1)
        def _():
            for channel in range(2):
                for block in range(5):
                    self.ext[channel, block, 384:640] = jnp.zeros((256, 128), F32)

    @property
    def sends_left(self):
        return self.col > 0

    @property
    def sends_up(self):
        return self.row > 0

    @property
    def takes_right(self):
        return self.col < N_COL - 1

    @property
    def takes_below(self):
        return self.row < N_ROW - 1

    def forward_corner(self, channel):
        @pl.when(self.takes_right)
        def _():
            self.left(channel).wait_recv()

            @pl.when(self.sends_up)
            def _():
                self.corner(channel).start()

    def finish(self):
        for index in range(4):
            @pl.when(self.sends_left)
            def _(index=index):
                self.left(index).wait_send()

        for index in (2, 3):
            @pl.when(self.takes_right)
            def _(index=index):
                self.left(index).wait_recv()

        for channel in range(2):
            @pl.when(self.sends_up)
            def _(channel=channel):
                self.up(channel).wait_send()

                @pl.when(self.takes_right)
                def _():
                    self.corner(channel).wait_send()

            @pl.when(self.takes_below)
            def _(channel=channel):
                self.up(channel).wait_recv()

                @pl.when(self.takes_right)
                def _():
                    self.corner(channel).wait_recv()


def fetch_kernel(object_ref, measured_ref, order_ref, ext_ref, sorted_ref,
                 turned, load_sems, left_sems, up_sems, corner_sems):
    row, col = place()
    barrier = pltpu.get_barrier_semaphore()
    greet_neighbours(barrier, row, col)
    loads = []
    for channel in range(2):
        for block in range(3):
            load = pltpu.make_async_copy(
                object_ref.at[channel, :, pl.ds(block * 128, 128)],
                ext_ref.at[channel, block, pl.ds(0, TILE), :],
                load_sems.at[channel * 3 + block],
            )
            load.start()
            loads.append(load)
    halo = Halo(ext_ref, left_sems, up_sems, corner_sems, row, col)
    halo.clear_edges()
    for load in loads:
        load.wait()
    pl.semaphore_wait(barrier, neighbour_count(row, col))

    @pl.when(halo.sends_left)
    def _():
        for index in range(4):
            halo.left(index).start()

    @pl.when(halo.sends_up)
    def _():
        for channel in range(2):
            halo.up(channel).start()

    def sort_frame(frame, carry):
        value = measured_ref[frame]
        total = jnp.zeros((256, 256), F32)
        for _ in range(3):
            piece = value.astype(BF16)
            value = value - piece.astype(F32)
            total = total + jnp.dot(piece, order_ref[...], preferred_element_type=F32)
        for block in range(2):
            turned[block] = total[:, block * 128:block * 128 + 128]
        for block in range(2):
            for parity in range(2):
                sorted_ref[frame, parity, :, block * 128:block * 128 + 128] = (
                    turned[block, pl.ds(parity, 128, stride=2), :])
        return carry

    lax.fori_loop(0, measured_ref.shape[0], sort_frame, 0)
    for channel in range(2):
        halo.forward_corner(channel)
    halo.finish()


def fetch(object_field, measured, order):
    dma = pltpu.SemaphoreType.DMA
    frames = measured.shape[0]
    return pl.pallas_call(
        fetch_kernel,
        name="fetch",
        out_shape=(
            jax.ShapeDtypeStruct((2, 5, EXT, 128), F32),
            jax.ShapeDtypeStruct((frames, 2, 128, 256), F32),
        ),
        in_specs=[ANY_SPEC, VMEM_SPEC, VMEM_SPEC],
        out_specs=(VMEM_SPEC, VMEM_SPEC),
        scratch_shapes=[
            pltpu.VMEM((2, 256, 128), F32), dma((6,)), dma((2, 4)), dma((2, 2)), dma((2, 2))],
        compiler_params=pltpu.CompilerParams(collective_id=0, has_side_effects=True),
    )(object_field, measured, order)


def halves(value):
    high = value.astype(BF16)
    low = (value - high.astype(F32)).astype(BF16)
    return high, low


def dot(left, right):
    return jnp.dot(left, right, preferred_element_type=F32)


def times_table(value, tables, index):
    high, low = halves(value)
    return dot(high, tables[index]) + dot(low, tables[index]) + dot(high, tables[index + 1])


def table_times(tables, index, value):
    high, low = halves(value)
    return dot(tables[index], high) + dot(tables[index + 1], high) + dot(tables[index], low)


def beside(a, b):
    return jnp.concatenate([a, b], axis=1)


def above(a, b):
    return jnp.concatenate([a, b], axis=0)


def frames_kernel(batch, counts_ref, first_ref, positions_ref, ext_ref, probe_ref, sorted_ref,
                  tables, grad_ref, probe_grad_ref):
    live = counts_ref[0, 0]
    first = jnp.minimum(first_ref[0, 0], live)
    start, end = (0, first) if batch == 0 else (first, live)
    for channel in range(2):
        for block in range(5):
            grad_ref[channel, block] = jnp.zeros((EXT, 128), F32)
    probe_grad_ref[...] = jnp.zeros_like(probe_grad_ref)
    lanes = lax.broadcasted_iota(jnp.int32, (256, 128), 1)

    def add_frame(frame, carry):
        row_start = positions_ref[frame, 0]
        col_start = positions_ref[frame, 1]
        block0 = col_start // 128
        shift = col_start - block0 * 128
        rows = pl.ds(row_start, 256)
        back_shift = jnp.bitwise_and(128 - shift, 127)

        window = []
        for channel in range(2):
            turned = [
                pltpu.roll(ext_ref[channel, block0 + block, rows, :], back_shift, 1)
                for block in range(3)
            ]
            keep = lanes < 128 - shift
            window.append([jnp.where(keep, turned[b], turned[b + 1]) for b in range(2)])
        probe = [[probe_ref[channel * 512 + b * 256: channel * 512 + b * 256 + 256, :]
                  for b in range(2)] for channel in range(2)]
        exit_re = [probe[0][b] * window[0][b] - probe[1][b] * window[1][b] for b in range(2)]
        exit_im = [probe[0][b] * window[1][b] + probe[1][b] * window[0][b] for b in range(2)]
        y0 = times_table(beside(exit_re[0] + exit_re[1], exit_im[0] + exit_im[1]), tables, 0)
        y1 = times_table(beside(exit_re[0] - exit_re[1], exit_im[0] - exit_im[1]), tables, 2)

        def stacked(t0, t1):
            return above(beside(t0[:, :128], t1[:, :128]), beside(t0[:, 128:], t1[:, 128:]))

        w0 = table_times(tables, 4, stacked(y0[:128] + y0[128:], y1[:128] + y1[128:]))
        w1 = table_times(tables, 6, stacked(y0[:128] - y0[128:], y1[:128] - y1[128:]))

        def weighted(w, parity):
            re, im = w[:128], w[128:]
            residue = re * re + im * im - sorted_ref[frame, parity]
            return above(residue * re, residue * im)

        u0 = table_times(tables, 0, weighted(w0, 0))
        u1 = table_times(tables, 2, weighted(w1, 1))
        top, bottom = u0 + u1, u0 - u1
        z_re = above(top[:128], bottom[:128])
        z_im = above(top[128:], bottom[128:])
        v0 = times_table(beside(z_re[:, :128], z_im[:, :128]), tables, 4)
        v1 = times_table(beside(z_re[:, 128:], z_im[:, 128:]), tables, 6)
        back_re = [v0[:, :128] + v1[:, :128], v0[:, :128] - v1[:, :128]]
        back_im = [v0[:, 128:] + v1[:, 128:], v0[:, 128:] - v1[:, 128:]]

        for b in range(2):
            r0 = b * 256
            probe_grad_ref[r0:r0 + 256, :] += window[0][b] * back_re[b] + window[1][b] * back_im[b]
            probe_grad_ref[512 + r0:768 + r0, :] += (
                window[0][b] * back_im[b] - window[1][b] * back_re[b])
        before = lanes < shift
        zero = jnp.zeros((256, 128), F32)
        for channel in range(2):
            if channel == 0:
                term = [probe[0][b] * back_re[b] + probe[1][b] * back_im[b] for b in range(2)]
            else:
                term = [probe[0][b] * back_im[b] - probe[1][b] * back_re[b] for b in range(2)]
            turned = [pltpu.roll(term[b], shift, 1) for b in range(2)]
            adds = [
                jnp.where(before, zero, turned[0]),
                jnp.where(before, turned[0], turned[1]),
                jnp.where(before, turned[1], zero),
            ]
            for block in range(3):
                at = (channel, block0 + block, rows, slice(None))
                grad_ref[at] = grad_ref[at] + adds[block]
        return carry

    lax.fori_loop(start, end, add_frame, 0)


def frames(batch, counts, first, positions, ext, probe, ordered, tables):
    return pl.pallas_call(
        functools.partial(frames_kernel, batch),
        name=f"frames{batch}",
        out_shape=(
            jax.ShapeDtypeStruct((2, 5, EXT, 128), F32),
            jax.ShapeDtypeStruct((1024, 128), F32),
        ),
        in_specs=[SMEM_SPEC, SMEM_SPEC, SMEM_SPEC] + [VMEM_SPEC] * 4,
        out_specs=(VMEM_SPEC, VMEM_SPEC),
    )(counts, first, positions, ext, probe, ordered, tables)


class Reduce:
    def __init__(self, grad, half, quarter, piece, got_half, got_quarter, got_piece, got_z,
                 full, sums, sems, row, col):
        self.grad, self.half, self.quarter, self.piece = grad, half, quarter, piece
        self.got_half, self.got_quarter = got_half, got_quarter
        self.got_piece, self.got_z = got_piece, got_z
        self.full, self.sums, self.sems = full, sums, sems
        self.row, self.col = row, col
        self.core = row % 2
        self.y = (row % 8) // 2
        self.x = (row // 8) * 2 + col // 8
        self.z = col % 8

    def partner(self):
        return (self.row + 1 - 2 * self.core, self.col)

    def x_peer(self, step):
        x = (self.x + step) % 4
        return x, ((x // 2) * 8 + self.row % 8, (x % 2) * 8 + self.z)

    def y_peer(self, step):
        y = (self.y + step) % 4
        return y, ((self.row // 8) * 8 + y * 2 + self.core, self.col)

    def z_peer(self, step):
        z = (self.z + step) % 8
        return z, (self.row, (self.col // 8) * 8 + z)

    def peers(self):
        found = [self.partner()]
        found += [self.x_peer(step)[1] for step in range(1, 4)]
        found += [self.y_peer(step)[1] for step in range(1, 4)]
        found += [self.z_peer(step)[1] for step in range(1, 8)]
        return found

    def copy(self, src, dst, index, device):
        return remote(src, dst, self.sems.at[0, index], self.sems.at[1, index], device)

    def pair(self):
        other = pl.multiple_of((1 - self.core) * 512, 512)
        return self.copy(self.grad.at[pl.ds(other, 512), :], self.got_half, 0, self.partner())

    def over_x(self, step):
        x, device = self.x_peer(step)
        return self.copy(self.half.at[pl.ds(pl.multiple_of(x * 128, 128), 128), :],
                         self.got_quarter.at[step - 1], step, device)

    def over_y(self, step):
        y, device = self.y_peer(step)
        return self.copy(self.quarter.at[pl.ds(pl.multiple_of(y * 32, 32), 32), :],
                         self.got_piece.at[step - 1], 3 + step, device)

    def over_z(self, step):
        _, device = self.z_peer(step)
        return self.copy(self.piece, self.got_z.at[self.z], 6 + step, device)

    def back_y(self, step):
        _, device = self.y_peer(step)
        mine = self.sums.at[pl.ds(pl.multiple_of(self.full_at(), 32), 32), :]
        return self.copy(mine, mine, 13 + step, device)

    def back_x(self, step):
        _, device = self.x_peer(step)
        mine = self.sums.at[pl.ds(pl.multiple_of(self.core * 512 + self.x * 128, 128), 128), :]
        return self.copy(mine, mine, 16 + step, device)

    def back_pair(self):
        mine = self.sums.at[pl.ds(pl.multiple_of(self.core * 512, 512), 512), :]
        return self.copy(mine, mine, 20, self.partner())

    def full_at(self):
        return self.core * 512 + self.x * 128 + self.y * 32

    def stages(self):
        def begin():
            self.pair().start()

        def to_x():
            self.pair().wait_recv()
            mine = pl.multiple_of(self.core * 512, 512)
            self.half[...] = self.grad[pl.ds(mine, 512), :] + self.got_half[...]
            for step in range(1, 4):
                self.over_x(step).start()

        def to_y():
            for step in range(1, 4):
                self.over_x(step).wait_recv()
            mine = pl.multiple_of(self.x * 128, 128)
            self.quarter[...] = (self.half[pl.ds(mine, 128), :] + self.got_quarter[0]) + (
                self.got_quarter[1] + self.got_quarter[2])
            for step in range(1, 4):
                self.over_y(step).start()

        def to_z():
            for step in range(1, 4):
                self.over_y(step).wait_recv()
            mine = pl.multiple_of(self.y * 32, 32)
            self.piece[...] = (self.quarter[pl.ds(mine, 32), :] + self.got_piece[0]) + (
                self.got_piece[1] + self.got_piece[2])
            for step in range(1, 8):
                self.over_z(step).start()
            self.got_z[self.z] = self.piece[...]

        def from_z():
            for step in range(1, 8):
                z = (self.z + 8 - step) % 8
                self.copy(self.piece, self.got_z.at[z], 6 + step, self.z_peer(step)[1]).wait_recv()
            total = self.got_z[0]
            for z in range(1, 8):
                total = total + self.got_z[z]
            self.sums[pl.ds(pl.multiple_of(self.full_at(), 32), 32), :] = total
            for step in range(1, 4):
                self.back_y(step).start()

        def from_y():
            for step in range(1, 4):
                y = (self.y + 4 - step) % 4
                at = pl.multiple_of(self.core * 512 + self.x * 128 + y * 32, 32)
                theirs = self.sums.at[pl.ds(at, 32), :]
                self.copy(theirs, theirs, 13 + step, self.y_peer(step)[1]).wait_recv()
            for step in range(1, 4):
                self.back_x(step).start()

        def from_x():
            for step in range(1, 4):
                x = (self.x + 4 - step) % 4
                at = pl.multiple_of(self.core * 512 + x * 128, 128)
                theirs = self.sums.at[pl.ds(at, 128), :]
                self.copy(theirs, theirs, 16 + step, self.x_peer(step)[1]).wait_recv()
            self.back_pair().start()

        def end():
            at = pl.multiple_of((1 - self.core) * 512, 512)
            theirs = self.sums.at[pl.ds(at, 512), :]
            self.copy(theirs, theirs, 20, self.partner()).wait_recv()
            self.pair().wait_send()
            for step in range(1, 4):
                self.over_x(step).wait_send()
                self.over_y(step).wait_send()
                self.back_x(step).wait_send()
                self.back_y(step).wait_send()
            for step in range(1, 8):
                self.over_z(step).wait_send()
            self.back_pair().wait_send()

        return begin, to_x, to_y, to_z, from_z, from_y, from_x, end


RIGHT_CHUNKS = ((0, 256, 128), (1, 256, 128), (0, 0, 256), (1, 0, 256))


def exchange_kernel(refetch, object_ref, grad_ref, probe_ref, probe_grad_ref, out_ref, probe_out,
                    from_above, from_left, joined,
                    half, quarter, piece, got_half, got_quarter, got_piece, got_z, sums,
                    down_sems, right_sems, reduce_sems, *halo_sems):
    row, col = place()
    reduce = Reduce(probe_grad_ref, half, quarter, piece, got_half, got_quarter, got_piece, got_z,
                    None, sums, reduce_sems, row, col)
    begin, to_x, to_y, to_z, from_z, from_y, from_x, end = reduce.stages()
    barrier = pltpu.get_barrier_semaphore()
    greet_neighbours(barrier, row, col)
    for device in reduce.peers():
        pl.semaphore_signal(barrier, inc=1, device_id=device, device_id_type=MESH)
    sends_down, takes_above = row < N_ROW - 1, row > 0
    sends_right, takes_left = col < N_COL - 1, col > 0
    if refetch:
        halo = Halo(out_ref, *halo_sems, row, col)
        halo.clear_edges()

    @pl.when(row == 0)
    def _():
        for channel in range(2):
            for block in range(5):
                from_above[channel, block] = jnp.zeros((256, 128), F32)

    @pl.when(col == 0)
    def _():
        for channel in range(2):
            for block in range(2):
                from_left[channel, block] = jnp.zeros((TILE, 128), F32)

    pl.semaphore_wait(barrier, 14 + neighbour_count(row, col))

    def down(channel, part):
        blocks = pl.ds(3, 2) if part == 0 else pl.ds(0, 3)
        return remote(
            grad_ref.at[channel, blocks, pl.ds(384, 256), :],
            from_above.at[channel, blocks, :, :],
            down_sems.at[0, channel, part], down_sems.at[1, channel, part],
            (jnp.minimum(row + 1, N_ROW - 1), col),
        )

    def right(index):
        channel, start, rows = RIGHT_CHUNKS[index]
        if index < 2:
            source = grad_ref.at[channel, pl.ds(3, 2), pl.ds(start, rows), :]
        else:
            source = joined.at[channel]
        return remote(
            source, from_left.at[channel, :, pl.ds(start, rows), :],
            right_sems.at[0, index], right_sems.at[1, index],
            (row, jnp.minimum(col + 1, N_COL - 1)),
        )

    begin()

    @pl.when(sends_right)
    def _():
        right(0).start()
        right(1).start()

    @pl.when(sends_down)
    def _():
        for part in range(2):
            for channel in range(2):
                down(channel, part).start()

    def take_above(channel, part):
        @pl.when(takes_above)
        def _():
            down(channel, part).wait_recv()

    def join(channel):
        take_above(channel, 0)
        for block in range(2):
            joined[channel, block] = (
                grad_ref[channel, 3 + block, 0:256] + from_above[channel, 3 + block])

        @pl.when(sends_right)
        def _():
            right(2 + channel).start()

    def take_left(index):
        @pl.when(takes_left)
        def _():
            right(index).wait_recv()

    def put(channel, block, start, rows, value):
        if refetch:
            out_ref[channel, block, start:start + rows] = value
        else:
            out_ref[channel, start:start + rows, block * 128:block * 128 + 128] = value

    def update_low(channel):
        rows = slice(256, 384)
        for block in range(3):
            grad = grad_ref[channel, block, rows]
            if block < 2:
                grad = grad + from_left[channel, block, rows]
            put(channel, block, 256, 128, object_ref[channel, block, rows] - 0.1 * grad)

    def update_top(channel):
        rows = slice(0, 256)
        for block in range(3):
            grad = grad_ref[channel, block, rows] + from_above[channel, block]
            if block < 2:
                grad = grad + from_left[channel, block, rows]
            put(channel, block, 0, 256, object_ref[channel, block, rows] - 0.1 * grad)

    def send_left(index):
        if refetch:
            @pl.when(halo.sends_left)
            def _():
                halo.left(index).start()

    def send_up(channel):
        if refetch:
            @pl.when(halo.sends_up)
            def _():
                halo.up(channel).start()

    to_x()
    join(0)
    to_y()
    join(1)
    for channel in range(2):
        take_left(channel)
        update_low(channel)
        send_left(2 + channel)
    to_z()
    take_above(0, 1)
    take_left(2)
    update_top(0)
    send_left(0)
    send_up(0)
    from_z()
    take_above(1, 1)
    from_y()
    take_left(3)
    update_top(1)
    send_left(1)
    send_up(1)
    from_x()
    if refetch:
        halo.forward_corner(0)
    end()
    step_size = 0.5 / math.sqrt(N_ROW * N_COL * 8)
    probe_out[...] = probe_ref[...] - step_size * sums[...]
    if refetch:
        halo.forward_corner(1)
        halo.finish()

    @pl.when(sends_down)
    def _():
        for part in range(2):
            for channel in range(2):
                down(channel, part).wait_send()

    @pl.when(sends_right)
    def _():
        for index in range(4):
            right(index).wait_send()


def exchange(refetch, ext, grad, probe, probe_grad):
    dma = pltpu.SemaphoreType.DMA
    out = (2, 5, EXT, 128) if refetch else (2, TILE, TILE)
    halo_sems = [dma((2, 4)), dma((2, 2)), dma((2, 2))] if refetch else []
    return pl.pallas_call(
        functools.partial(exchange_kernel, refetch),
        name=f"exchange{int(refetch)}",
        out_shape=(jax.ShapeDtypeStruct(out, F32), jax.ShapeDtypeStruct((1024, 128), F32)),
        in_specs=[VMEM_SPEC] * 4,
        out_specs=(VMEM_SPEC, VMEM_SPEC),
        scratch_shapes=[
            pltpu.VMEM((2, 5, 256, 128), F32),
            pltpu.VMEM((2, 2, TILE, 128), F32),
            pltpu.VMEM((2, 2, 256, 128), F32),
            pltpu.VMEM((512, 128), F32),
            pltpu.VMEM((128, 128), F32),
            pltpu.VMEM((32, 128), F32),
            pltpu.VMEM((512, 128), F32),
            pltpu.VMEM((3, 128, 128), F32),
            pltpu.VMEM((3, 32, 128), F32),
            pltpu.VMEM((8, 32, 128), F32),
            pltpu.VMEM((1024, 128), F32),
            dma((2, 2, 2)),
            dma((2, 4)),
            dma((2, 21)),
        ] + halo_sems,
        compiler_params=pltpu.CompilerParams(
            collective_id=1 + int(refetch), has_side_effects=True),
    )(ext, grad, probe, probe_grad)


def to_blocks(probe):
    return probe.reshape(2, 256, 2, 128).transpose(0, 2, 1, 3).reshape(1024, 128)


def from_blocks(blocks):
    return blocks.reshape(2, 2, 256, 128).transpose(0, 2, 1, 3).reshape(2, 256, 256)


def per_device(object_field, illumination, measured, positions, frame_counts, first_count):
    tables = jnp.asarray(dft_tables())
    order = jnp.asarray(deinterleave_table())
    positions = positions[0, 0]
    probe = to_blocks(illumination)
    ext, ordered = fetch(object_field, measured[0, 0], order)
    grad, probe_grad = frames(
        0, frame_counts, first_count, positions, ext, probe, ordered, tables)
    ext, probe = exchange(True, ext, grad, probe, probe_grad)
    grad, probe_grad = frames(
        1, frame_counts, first_count, positions, ext, probe, ordered, tables)
    new_object, probe = exchange(False, ext, grad, probe, probe_grad)
    return new_object, from_blocks(probe)


def solution(mesh):
    in_specs = (
        P(None, "row", "col"),
        P(),
        P("row", "col", None, None, None),
        P("row", "col", None, None),
        P("row", "col"),
        P("row", "col"),
    )
    out_specs = (P(None, "row", "col"), P())
    return jax.shard_map(
        per_device, mesh=mesh, in_specs=in_specs, out_specs=out_specs, check_vma=False
    )
```

```python
import functools
import math

import jax
import jax.numpy as jnp
import numpy as np
from jax import lax
from jax.experimental import pallas as pl
from jax.experimental.pallas import tpu as pltpu
from jax.sharding import PartitionSpec as P

MESH = pl.DeviceIdType.MESH
TILE, PROBE, EXT = 384, 256, 640
N_ROW = N_COL = 16
F32, BF16 = jnp.float32, jnp.bfloat16
FETCH_VMEM, FRAMES_VMEM, EXCHANGE_VMEM = 14 << 20, 16 << 20, 18 << 20
VMEM_SPEC = pl.BlockSpec(memory_space=pltpu.VMEM)
SMEM_SPEC = pl.BlockSpec(memory_space=pltpu.SMEM)
HBM_SPEC = pl.BlockSpec(memory_space=pltpu.HBM)


def split_bf16(table):
    high = table.astype(np.float32).astype(BF16)
    low = (table - high.astype(np.float64)).astype(np.float32).astype(BF16)
    return high, low


def dft_tables():
    n = np.arange(128)[:, None]
    parts = []
    for parity in (0, 1):
        k = 2 * np.arange(128)[None, :] + parity
        angle = ((n * k) % 256) * (2.0 * np.pi / 256.0)
        c, s = np.cos(angle) / 16.0, np.sin(angle) / 16.0
        table = np.block([[c, -s], [s, c]])
        parts.append((split_bf16(table), split_bf16(table.T)))
    order = []
    for transposed in (0, 1):
        for parity in (0, 1):
            order.extend(parts[parity][transposed])
    return np.stack(order)


def deinterleave_table():
    table = np.zeros((256, 256), np.float32)
    index = np.arange(128)
    table[2 * index, index] = 1.0
    table[2 * index + 1, 128 + index] = 1.0
    return table.astype(BF16)


def place():
    row, col = lax.axis_index("row"), lax.axis_index("col")
    return row, col


def remote(src, dst, send_sem, recv_sem, device):
    return pltpu.make_async_remote_copy(
        src_ref=src, dst_ref=dst, send_sem=send_sem, recv_sem=recv_sem,
        device_id=device, device_id_type=MESH,
    )


UP_DETOUR = ((8, 15), (14, 15), (6, 7), (7, 15))
DOWN_DETOUR = ((7, 0), (1, 0), (9, 8), (8, 0))


def is_at(row, col, device):
    return (row == device[0]) & (col == device[1])


def place_of(device):
    return jnp.int32(device[0]), jnp.int32(device[1])


def greet_detour(barrier, row, col, detour):
    for hop in range(3):
        for here, there in ((detour[hop], detour[hop + 1]), (detour[hop + 1], detour[hop])):
            @pl.when(is_at(row, col, here))
            def _(there=there):
                pl.semaphore_signal(
                    barrier, inc=1, device_id=place_of(there), device_id_type=MESH)


def detour_count(row, col, detour):
    one, two, none = jnp.int32(1), jnp.int32(2), jnp.int32(0)
    ends = is_at(row, col, detour[0]) | is_at(row, col, detour[3])
    middles = is_at(row, col, detour[1]) | is_at(row, col, detour[2])
    return jnp.where(ends, one, none) + jnp.where(middles, two, none)


def greet_neighbours(barrier, row, col):
    for has, device in (
        (row > 0, (row - 1, col)),
        (row < N_ROW - 1, (row + 1, col)),
        (col > 0, (row, col - 1)),
        (col < N_COL - 1, (row, col + 1)),
    ):
        @pl.when(has)
        def _(device=device):
            pl.semaphore_signal(barrier, inc=1, device_id=device, device_id_type=MESH)


def neighbour_count(row, col):
    one, none = jnp.int32(1), jnp.int32(0)
    has = (row > 0, row < N_ROW - 1, col > 0, col < N_COL - 1)
    return sum(jnp.where(h, one, none) for h in has)


CHUNKS = ((0, 64), (64, 64), (128, 64), (192, 64), (256, 64), (320, 64))
TOPS = 4
LOWS = (4, 5)
EVERY = 6


class Halo:
    def __init__(self, ext, detour, left_sems, up_sems, corner_sems, detour_sems, row, col):
        self.ext, self.row, self.col = ext, row, col
        self.left_sems, self.up_sems, self.corner_sems = left_sems, up_sems, corner_sems
        self.detour, self.detour_sems = detour, detour_sems
        self.stops = [is_at(row, col, UP_DETOUR[hop]) for hop in range(3)]
        self.sends_left, self.takes_right = col > 0, col < N_COL - 1
        self.sends_up, self.takes_below = row > 0, row < N_ROW - 1
        self.sends_direct = self.sends_up & jnp.logical_not(self.stops[0])

    def left(self, index):
        start, rows = CHUNKS[index]
        return remote(
            self.ext.at[:, pl.ds(0, 2), pl.ds(start, rows), :],
            self.ext.at[:, pl.ds(3, 2), pl.ds(start, rows), :],
            self.left_sems.at[0, index], self.left_sems.at[1, index],
            (self.row, jnp.maximum(self.col - 1, 0)),
        )

    def over(self, index, blocks, sems):
        start, rows = CHUNKS[index]
        return remote(
            self.ext.at[:, blocks, pl.ds(start, rows), :],
            self.ext.at[:, blocks, pl.ds(384 + start, rows), :],
            sems.at[0, index], sems.at[1, index],
            (jnp.maximum(self.row - 1, 0), self.col),
        )

    def up(self, index):
        return self.over(index, pl.ds(0, 3), self.up_sems)

    def corner(self, index):
        return self.over(index, pl.ds(3, 2), self.corner_sems)

    def detour_hop(self, hop, index):
        start, rows = CHUNKS[index]
        first, last = hop == 0, hop == 2
        source = self.ext if first else self.detour
        target = self.ext.at[:, pl.ds(0, 3), pl.ds(384 + start, rows), :] if last else (
            self.detour.at[:, :, pl.ds(start, rows), :])
        return remote(
            source.at[:, pl.ds(0, 3), pl.ds(start, rows), :], target,
            self.detour_sems.at[0, index],
            self.up_sems.at[1, index] if last else self.detour_sems.at[1, index],
            place_of(UP_DETOUR[hop + 1]),
        )

    def pass_on(self, index):
        for hop in (1, 2):
            @pl.when(self.stops[hop])
            def _(hop=hop):
                self.detour_hop(hop - 1, index).wait_recv()
                self.detour_hop(hop, index).start()

    def clear_edges(self):
        @pl.when(self.col == N_COL - 1)
        def _():
            for channel in range(2):
                for block in (3, 4):
                    self.ext[channel, block] = jnp.zeros((EXT, 128), F32)

        @pl.when(self.row == N_ROW - 1)
        def _():
            for channel in range(2):
                for block in range(5):
                    self.ext[channel, block, 384:640] = jnp.zeros((256, 128), F32)

    def send_left(self, index):
        @pl.when(self.sends_left)
        def _():
            self.left(index).start()

    def send_up(self, index):
        @pl.when(self.sends_direct)
        def _():
            self.up(index).start()

        @pl.when(self.stops[0])
        def _():
            self.detour_hop(0, index).start()

    def forward_corner(self, index):
        @pl.when(self.takes_right)
        def _():
            self.left(index).wait_recv()

            @pl.when(self.sends_up)
            def _():
                self.corner(index).start()

    def finish(self):
        @pl.when(self.takes_right)
        def _():
            for index in LOWS:
                self.left(index).wait_recv()

        @pl.when(self.takes_below)
        def _():
            for index in range(TOPS):
                self.up(index).wait_recv()

        @pl.when(self.takes_below & self.takes_right)
        def _():
            for index in range(TOPS):
                self.corner(index).wait_recv()

        @pl.when(self.sends_left)
        def _():
            for index in range(EVERY):
                self.left(index).wait_send()

        @pl.when(self.sends_direct)
        def _():
            for index in range(TOPS):
                self.up(index).wait_send()

        for hop in range(3):
            @pl.when(self.stops[hop])
            def _(hop=hop):
                for index in range(TOPS):
                    self.detour_hop(hop, index).wait_send()

        @pl.when(self.sends_up & self.takes_right)
        def _():
            for index in range(TOPS):
                self.corner(index).wait_send()


def halo_sems():
    dma = pltpu.SemaphoreType.DMA
    return [pltpu.VMEM((2, 3, 256, 128), F32), dma((2, EVERY)), dma((2, TOPS)), dma((2, TOPS)),
            dma((2, TOPS))]


def fetch_kernel(object_ref, measured_ref, order_ref, ext_ref, sorted_ref,
                 turned, measured, load_sems, *sems):
    row, col = place()
    barrier = pltpu.get_barrier_semaphore()
    greet_neighbours(barrier, row, col)
    greet_detour(barrier, row, col, UP_DETOUR)
    loads = []
    for channel in range(2):
        for block in range(3):
            load = pltpu.make_async_copy(
                object_ref.at[channel, :, pl.ds(block * 128, 128)],
                ext_ref.at[channel, block, pl.ds(0, TILE), :],
                load_sems.at[channel * 3 + block],
            )
            load.start()
            loads.append(load)
    load_frames = pltpu.make_async_copy(measured_ref, measured, load_sems.at[6])
    load_frames.start()
    halo = Halo(ext_ref, *sems, row, col)
    halo.clear_edges()
    for load in loads:
        load.wait()
    pl.semaphore_wait(barrier, neighbour_count(row, col) + detour_count(row, col, UP_DETOUR))
    for index in range(EVERY):
        halo.send_left(index)
    for index in range(TOPS):
        halo.send_up(index)

    def sort_frame(frame, carry):
        value = measured[frame]
        total = jnp.zeros((256, 256), F32)
        for _ in range(3):
            piece = value.astype(BF16)
            value = value - piece.astype(F32)
            total = total + jnp.dot(piece, order_ref[...], preferred_element_type=F32)
        for block in range(2):
            turned[block] = total[:, block * 128:block * 128 + 128]
        for block in range(2):
            for parity in range(2):
                sorted_ref[frame, parity, :, block * 128:block * 128 + 128] = (
                    turned[block, pl.ds(parity, 128, stride=2), :])
        return carry

    load_frames.wait()
    share = measured.shape[0] // TOPS
    for index in range(TOPS):
        lax.fori_loop(index * share, (index + 1) * share, sort_frame, 0)
        halo.pass_on(index)
        halo.forward_corner(index)
    halo.finish()


def fetch(object_field, measured, order):
    dma = pltpu.SemaphoreType.DMA
    count = measured.shape[0]
    return pl.pallas_call(
        fetch_kernel,
        name="fetch",
        out_shape=(
            jax.ShapeDtypeStruct((2, 5, EXT, 128), F32),
            jax.ShapeDtypeStruct((count, 2, 128, 256), F32),
        ),
        in_specs=[HBM_SPEC, HBM_SPEC, VMEM_SPEC],
        out_specs=(VMEM_SPEC, VMEM_SPEC),
        scratch_shapes=[
            pltpu.VMEM((2, 256, 128), F32), pltpu.VMEM((count, 256, 256), F32), dma((7,)),
        ] + halo_sems(),
        compiler_params=pltpu.CompilerParams(
            collective_id=0, has_side_effects=True, vmem_limit_bytes=FETCH_VMEM),
    )(object_field, measured, order)


def halves(value):
    high = value.astype(BF16)
    low = (value - high.astype(F32)).astype(BF16)
    return high, low


def dot(left, right):
    return jnp.dot(left, right, preferred_element_type=F32)


def times_table(value, tables, index):
    high, low = halves(value)
    return dot(high, tables[index]) + dot(low, tables[index]) + dot(high, tables[index + 1])


def table_times(tables, index, value):
    high, low = halves(value)
    return dot(tables[index], high) + dot(tables[index + 1], high) + dot(tables[index], low)


def beside(a, b):
    return jnp.concatenate([a, b], axis=1)


def above(a, b):
    return jnp.concatenate([a, b], axis=0)


def frames_kernel(batch, counts_ref, first_ref, positions_ref, ext_ref, probe_ref, sorted_ref,
                  tables, grad_ref, probe_grad_ref):
    live = counts_ref[0, 0]
    first = jnp.minimum(first_ref[0, 0], live)
    start, end = (0, first) if batch == 0 else (first, live)
    for channel in range(2):
        for block in range(5):
            grad_ref[channel, block] = jnp.zeros((EXT, 128), F32)
    probe_grad_ref[...] = jnp.zeros_like(probe_grad_ref)
    lanes = lax.broadcasted_iota(jnp.int32, (256, 128), 1)

    def add_frame(frame, carry):
        row_start = positions_ref[0, frame]
        col_start = positions_ref[1, frame]
        block0 = col_start // 128
        shift = col_start - block0 * 128
        rows = pl.ds(row_start, 256)
        back_shift = jnp.bitwise_and(128 - shift, 127)

        window = []
        for channel in range(2):
            turned = [
                pltpu.roll(ext_ref[channel, block0 + block, rows, :], back_shift, 1)
                for block in range(3)
            ]
            keep = lanes < 128 - shift
            window.append([jnp.where(keep, turned[b], turned[b + 1]) for b in range(2)])
        probe = [[probe_ref[channel, :, b * 128:b * 128 + 128] for b in range(2)]
                 for channel in range(2)]
        exit_re = [probe[0][b] * window[0][b] - probe[1][b] * window[1][b] for b in range(2)]
        exit_im = [probe[0][b] * window[1][b] + probe[1][b] * window[0][b] for b in range(2)]
        y0 = times_table(beside(exit_re[0] + exit_re[1], exit_im[0] + exit_im[1]), tables, 0)
        y1 = times_table(beside(exit_re[0] - exit_re[1], exit_im[0] - exit_im[1]), tables, 2)

        def stacked(t0, t1):
            return above(beside(t0[:, :128], t1[:, :128]), beside(t0[:, 128:], t1[:, 128:]))

        w0 = table_times(tables, 4, stacked(y0[:128] + y0[128:], y1[:128] + y1[128:]))
        w1 = table_times(tables, 6, stacked(y0[:128] - y0[128:], y1[:128] - y1[128:]))

        def weighted(w, parity):
            re, im = w[:128], w[128:]
            residue = re * re + im * im - sorted_ref[frame, parity]
            return above(residue * re, residue * im)

        u0 = table_times(tables, 0, weighted(w0, 0))
        u1 = table_times(tables, 2, weighted(w1, 1))
        top, bottom = u0 + u1, u0 - u1
        z_re = above(top[:128], bottom[:128])
        z_im = above(top[128:], bottom[128:])
        v0 = times_table(beside(z_re[:, :128], z_im[:, :128]), tables, 4)
        v1 = times_table(beside(z_re[:, 128:], z_im[:, 128:]), tables, 6)
        back_re = [v0[:, :128] + v1[:, :128], v0[:, :128] - v1[:, :128]]
        back_im = [v0[:, 128:] + v1[:, 128:], v0[:, 128:] - v1[:, 128:]]

        for b in range(2):
            at = slice(b * 128, b * 128 + 128)
            probe_grad_ref[0, :, at] += window[0][b] * back_re[b] + window[1][b] * back_im[b]
            probe_grad_ref[1, :, at] += window[0][b] * back_im[b] - window[1][b] * back_re[b]
        before = lanes < shift
        zero = jnp.zeros((256, 128), F32)
        for channel in range(2):
            if channel == 0:
                term = [probe[0][b] * back_re[b] + probe[1][b] * back_im[b] for b in range(2)]
            else:
                term = [probe[0][b] * back_im[b] - probe[1][b] * back_re[b] for b in range(2)]
            turned = [pltpu.roll(term[b], shift, 1) for b in range(2)]
            adds = [
                jnp.where(before, zero, turned[0]),
                jnp.where(before, turned[0], turned[1]),
                jnp.where(before, turned[1], zero),
            ]
            for block in range(3):
                at = (channel, block0 + block, rows, slice(None))
                grad_ref[at] = grad_ref[at] + adds[block]
        return carry

    lax.fori_loop(start, end, add_frame, 0)


def frames(batch, counts, first, positions, ext, probe, ordered, tables):
    return pl.pallas_call(
        functools.partial(frames_kernel, batch),
        name=f"frames{batch}",
        out_shape=(
            jax.ShapeDtypeStruct((2, 5, EXT, 128), F32),
            jax.ShapeDtypeStruct((2, PROBE, PROBE), F32),
        ),
        in_specs=[SMEM_SPEC, SMEM_SPEC, SMEM_SPEC] + [VMEM_SPEC] * 4,
        out_specs=(VMEM_SPEC, VMEM_SPEC),
        compiler_params=pltpu.CompilerParams(vmem_limit_bytes=FRAMES_VMEM),
    )(counts, first, positions, ext, probe, ordered, tables)


AROUND = tuple((i, j) for i in range(4) for j in range(4) if i or j)


class Reduce:
    def __init__(self, grad, half, got_half, got_plane, got_z, sums, sems, row, col):
        self.grad, self.half, self.got_half = grad, half, got_half
        self.got_plane, self.got_z, self.sums, self.sems = got_plane, got_z, sums, sems
        self.row, self.col, self.core = row, col, row % 2
        self.y = (row % 8) // 2
        self.x = (row // 8) * 2 + col // 8
        self.z = col % 8

    def partner(self):
        return (self.row + 1 - 2 * self.core, self.col)

    def plane(self, i, j):
        x, y = (self.x + i) % 4, (self.y + j) % 4
        device = ((x // 2) * 8 + y * 2 + self.core, (x % 2) * 8 + self.z)
        return pl.ds(pl.multiple_of((x * 4 + y) * 16, 16), 16), device

    def over_z_to(self, step):
        z = (self.z + step) % 8
        return z, (self.row, (self.col // 8) * 8 + z)

    def peers(self):
        found = [self.partner()]
        found += [self.plane(i, j)[1] for i, j in AROUND]
        found += [self.over_z_to(step)[1] for step in range(1, 8)]
        return found

    def copy(self, src, dst, index, device):
        return remote(src, dst, self.sems.at[0, index], self.sems.at[1, index], device)

    def pair(self):
        return self.copy(self.grad.at[1 - self.core], self.got_half, 0, self.partner())

    def out(self, n):
        rows, device = self.plane(*AROUND[n])
        return self.copy(self.half.at[rows, :], self.got_plane.at[n], 1 + n, device)

    def along(self, step):
        return self.copy(
            self.got_z.at[self.z], self.got_z.at[self.z], 15 + step, self.over_z_to(step)[1])

    def back(self, n):
        rows = self.plane(0, 0)[0]
        mine = self.sums.at[self.core, rows, :]
        return self.copy(mine, mine, 23 + n, self.plane(*AROUND[n])[1])

    def back_pair(self):
        mine = self.sums.at[self.core]
        return self.copy(mine, mine, 38, self.partner())

    def begin(self):
        self.pair().start()

    def to_plane(self):
        self.pair().wait_recv()
        self.half[...] = self.grad[self.core] + self.got_half[...]
        for n in range(15):
            self.out(n).start()

    def to_z(self):
        for n in range(15):
            self.out(n).wait_recv()
        total = self.half[self.plane(0, 0)[0], :]
        for n in range(15):
            total = total + self.got_plane[n]
        self.got_z[self.z] = total
        for step in range(1, 8):
            self.along(step).start()

    def from_z(self):
        for step in range(1, 8):
            theirs = self.got_z.at[(self.z + 8 - step) % 8]
            self.copy(theirs, theirs, 15 + step, self.over_z_to(step)[1]).wait_recv()
        total = self.got_z[0]
        for z in range(1, 8):
            total = total + self.got_z[z]
        self.sums[self.core, self.plane(0, 0)[0], :] = total
        for n in range(15):
            self.back(n).start()

    def from_plane(self):
        for n in range(15):
            i, j = AROUND[n]
            theirs = self.sums.at[self.core, self.plane(4 - i, 4 - j)[0], :]
            self.copy(theirs, theirs, 23 + n, self.plane(i, j)[1]).wait_recv()
        self.back_pair().start()

    def end(self):
        theirs = self.sums.at[1 - self.core]
        self.copy(theirs, theirs, 38, self.partner()).wait_recv()

    def drain(self):
        self.pair().wait_send()
        for n in range(15):
            self.out(n).wait_send()
            self.back(n).wait_send()
        for step in range(1, 8):
            self.along(step).wait_send()
        self.back_pair().wait_send()


def exchange_kernel(refetch, object_ref, grad_ref, probe_ref, probe_grad_ref, out_ref, probe_out,
                    from_above, from_left, joined, half, got_half, got_plane, got_z, sums,
                    detour, down_sems, right_sems, reduce_sems, detour_sems, *sems):
    row, col = place()
    reduce = Reduce(
        probe_grad_ref, half, got_half, got_plane, got_z, sums, reduce_sems, row, col)
    barrier = pltpu.get_barrier_semaphore()
    greet_neighbours(barrier, row, col)
    greet_detour(barrier, row, col, DOWN_DETOUR)
    if refetch:
        greet_detour(barrier, row, col, UP_DETOUR)
    for device in reduce.peers():
        pl.semaphore_signal(barrier, inc=1, device_id=device, device_id_type=MESH)
    stops = [is_at(row, col, DOWN_DETOUR[hop]) for hop in range(3)]
    sends_down, takes_above = row < N_ROW - 1, row > 0
    sends_right, takes_left = col < N_COL - 1, col > 0
    if refetch:
        halo = Halo(out_ref, *sems, row, col)
        halo.clear_edges()

    @pl.when(row == 0)
    def _():
        for channel in range(2):
            for block in range(5):
                from_above[channel, block] = jnp.zeros((256, 128), F32)

    @pl.when(col == 0)
    def _():
        for channel in range(2):
            for block in range(2):
                from_left[channel, block] = jnp.zeros((TILE, 128), F32)

    greeted = 23 + neighbour_count(row, col) + detour_count(row, col, DOWN_DETOUR)
    if refetch:
        greeted = greeted + detour_count(row, col, UP_DETOUR)
    pl.semaphore_wait(barrier, greeted)

    def down(index, part):
        blocks = pl.ds(3, 2) if part == 0 else pl.ds(0, 3)
        start, rows = CHUNKS[index]
        return remote(
            grad_ref.at[:, blocks, pl.ds(384 + start, rows), :],
            from_above.at[:, blocks, pl.ds(start, rows), :],
            down_sems.at[0, part, index], down_sems.at[1, part, index],
            (jnp.minimum(row + 1, N_ROW - 1), col),
        )

    def detour_hop(hop, index):
        start, rows = CHUNKS[index]
        here = pl.ds(start, rows)
        source = detour.at[:, :, here, :] if hop else (
            grad_ref.at[:, pl.ds(0, 3), pl.ds(384 + start, rows), :])
        target = from_above.at[:, pl.ds(0, 3), here, :] if hop == 2 else detour.at[:, :, here, :]
        return remote(
            source, target, detour_sems.at[0, index],
            down_sems.at[1, 1, index] if hop == 2 else detour_sems.at[1, index],
            place_of(DOWN_DETOUR[hop + 1]),
        )

    def pass_on(index):
        for hop in (1, 2):
            @pl.when(stops[hop])
            def _(hop=hop):
                detour_hop(hop - 1, index).wait_recv()
                detour_hop(hop, index).start()

    sends_straight = sends_down & jnp.logical_not(stops[0])

    def send_corner(index):
        @pl.when(sends_down)
        def _():
            down(index, 0).start()

    def send_down(index):
        @pl.when(sends_straight)
        def _():
            down(index, 1).start()

        @pl.when(stops[0])
        def _():
            detour_hop(0, index).start()

    def right(index):
        start, rows = CHUNKS[index]
        if index in LOWS:
            source = grad_ref.at[:, pl.ds(3, 2), pl.ds(start, rows), :]
        else:
            source = joined.at[:, :, pl.ds(start, rows), :]
        return remote(
            source, from_left.at[:, :, pl.ds(start, rows), :],
            right_sems.at[0, index], right_sems.at[1, index],
            (row, jnp.minimum(col + 1, N_COL - 1)),
        )

    def send_right(index):
        @pl.when(sends_right)
        def _():
            right(index).start()

    def join(index):
        start, rows = CHUNKS[index]
        at = slice(start, start + rows)

        @pl.when(takes_above)
        def _():
            down(index, 0).wait_recv()

        for channel in range(2):
            for block in range(2):
                joined[channel, block, at] = (
                    grad_ref[channel, 3 + block, at] + from_above[channel, 3 + block, at])
        send_right(index)

    def update(index):
        start, rows = CHUNKS[index]
        at = slice(start, start + rows)
        if index < TOPS:
            @pl.when(takes_above)
            def _():
                down(index, 1).wait_recv()

        @pl.when(takes_left)
        def _():
            right(index).wait_recv()

        for channel in range(2):
            for block in range(3):
                grad = grad_ref[channel, block, at]
                if index < TOPS:
                    grad = grad + from_above[channel, block, at]
                if block < 2:
                    grad = grad + from_left[channel, block, at]
                value = object_ref[channel, block, at] - 0.1 * grad
                if refetch:
                    out_ref[channel, block, at] = value
                else:
                    out_ref[channel, at, block * 128:block * 128 + 128] = value
        if refetch:
            halo.send_left(index)
            if index < TOPS:
                halo.send_up(index)

    def forward(index):
        if refetch:
            halo.forward_corner(index)

    def pass_up(index):
        if refetch:
            halo.pass_on(index)

    reduce.begin()
    send_right(4)
    send_corner(0)
    send_corner(1)
    reduce.to_plane()
    send_corner(2)
    send_corner(3)
    for index in range(TOPS):
        send_down(index)
    join(0)
    join(1)
    pass_on(0)
    update(4)
    pass_on(1)
    reduce.to_z()
    join(2)
    join(3)
    send_right(5)
    pass_on(2)
    update(0)
    pass_on(3)
    update(1)
    reduce.from_z()
    forward(0)
    update(2)
    forward(1)
    update(3)
    update(5)
    pass_up(0)
    pass_up(1)
    reduce.from_plane()
    for index in (2, 3):
        forward(index)
        pass_up(index)
    reduce.end()
    step_size = 0.5 / math.sqrt(N_ROW * N_COL * 8)
    probe_out[...] = probe_ref[...] - step_size * sums[...]
    if refetch:
        halo.finish()
    reduce.drain()

    @pl.when(sends_down)
    def _():
        for index in range(TOPS):
            down(index, 0).wait_send()

    @pl.when(sends_straight)
    def _():
        for index in range(TOPS):
            down(index, 1).wait_send()

    for hop in range(3):
        @pl.when(stops[hop])
        def _(hop=hop):
            for index in range(TOPS):
                detour_hop(hop, index).wait_send()

    @pl.when(sends_right)
    def _():
        for index in range(EVERY):
            right(index).wait_send()


def exchange(refetch, ext, grad, probe, probe_grad):
    dma = pltpu.SemaphoreType.DMA
    out = (2, 5, EXT, 128) if refetch else (2, TILE, TILE)
    return pl.pallas_call(
        functools.partial(exchange_kernel, refetch),
        name=f"exchange{int(refetch)}",
        out_shape=(
            jax.ShapeDtypeStruct(out, F32), jax.ShapeDtypeStruct((2, PROBE, PROBE), F32)),
        in_specs=[VMEM_SPEC] * 4,
        out_specs=(VMEM_SPEC, VMEM_SPEC),
        scratch_shapes=[
            pltpu.VMEM((2, 5, 256, 128), F32),
            pltpu.VMEM((2, 2, TILE, 128), F32),
            pltpu.VMEM((2, 2, 256, 128), F32),
            pltpu.VMEM((256, 256), F32),
            pltpu.VMEM((256, 256), F32),
            pltpu.VMEM((15, 16, 256), F32),
            pltpu.VMEM((8, 16, 256), F32),
            pltpu.VMEM((2, 256, 256), F32),
            pltpu.VMEM((2, 3, 256, 128), F32),
            dma((2, 2, TOPS)),
            dma((2, EVERY)),
            dma((2, 39)),
            dma((2, TOPS)),
        ] + (halo_sems() if refetch else []),
        compiler_params=pltpu.CompilerParams(
            collective_id=1 + int(refetch), has_side_effects=True,
            vmem_limit_bytes=EXCHANGE_VMEM),
    )(ext, grad, probe, probe_grad)


def per_device(object_field, illumination, measured, positions, frame_counts, first_count):
    tables = jnp.asarray(dft_tables())
    order = jnp.asarray(deinterleave_table())
    positions = positions[0, 0].T
    probe = illumination
    ext, ordered = fetch(object_field, measured[0, 0], order)
    grad, probe_grad = frames(
        0, frame_counts, first_count, positions, ext, probe, ordered, tables)
    ext, probe = exchange(True, ext, grad, probe, probe_grad)
    grad, probe_grad = frames(
        1, frame_counts, first_count, positions, ext, probe, ordered, tables)
    new_object, probe = exchange(False, ext, grad, probe, probe_grad)
    return new_object, probe


def solution(mesh):
    in_specs = (
        P(None, "row", "col"),
        P(),
        P("row", "col", None, None, None),
        P("row", "col", None, None),
        P("row", "col"),
        P("row", "col"),
    )
    out_specs = (P(None, "row", "col"), P())
    return jax.shard_map(
        per_device, mesh=mesh, in_specs=in_specs, out_specs=out_specs, check_vma=False
    )
```

```python
import functools
import math

import jax
import jax.numpy as jnp
import numpy as np
from jax import lax
from jax.experimental import pallas as pl
from jax.experimental.pallas import tpu as pltpu
from jax.sharding import PartitionSpec as P

MESH = pl.DeviceIdType.MESH
TILE, PROBE, EXT = 384, 256, 640
N_ROW = N_COL = 16
F32, BF16 = jnp.float32, jnp.bfloat16
FETCH_VMEM, FRAMES_VMEM, EXCHANGE_VMEM = 14 << 20, 16 << 20, 18 << 20
VMEM_SPEC = pl.BlockSpec(memory_space=pltpu.VMEM)
SMEM_SPEC = pl.BlockSpec(memory_space=pltpu.SMEM)
HBM_SPEC = pl.BlockSpec(memory_space=pltpu.HBM)


def split_bf16(table):
    high = table.astype(np.float32).astype(BF16)
    low = (table - high.astype(np.float64)).astype(np.float32).astype(BF16)
    return high, low


def dft_tables():
    n = np.arange(128)[:, None]
    parts = []
    for parity in (0, 1):
        k = 2 * np.arange(128)[None, :] + parity
        angle = ((n * k) % 256) * (2.0 * np.pi / 256.0)
        c, s = np.cos(angle) / 16.0, np.sin(angle) / 16.0
        table = np.block([[c, -s], [s, c]])
        parts.append((split_bf16(table), split_bf16(table.T)))
    order = []
    for transposed in (0, 1):
        for parity in (0, 1):
            order.extend(parts[parity][transposed])
    return np.stack(order)


def deinterleave_table():
    table = np.zeros((256, 256), np.float32)
    index = np.arange(128)
    table[2 * index, index] = 1.0
    table[2 * index + 1, 128 + index] = 1.0
    return table.astype(BF16)


def place():
    row, col = lax.axis_index("row"), lax.axis_index("col")
    return row, col


def remote(src, dst, send_sem, recv_sem, device):
    return pltpu.make_async_remote_copy(
        src_ref=src, dst_ref=dst, send_sem=send_sem, recv_sem=recv_sem,
        device_id=device, device_id_type=MESH,
    )


UP_DETOURS = (((8, 15), (14, 15), (6, 7), (7, 15)),)
DOWN_DETOURS = (((7, 0), (1, 0), (9, 8), (8, 0)), ((7, 15), (1, 15), (9, 7), (8, 15)))


def is_at(row, col, device):
    return (row == device[0]) & (col == device[1])


def place_of(device):
    return jnp.int32(device[0]), jnp.int32(device[1])


class Detour:
    def __init__(self, paths, row, col):
        self.paths, self.row, self.col = paths, row, col
        self.first = [is_at(row, col, paths[0][stop]) for stop in range(4)]
        self.stops = [
            functools.reduce(jnp.logical_or, [is_at(row, col, path[stop]) for path in paths])
            for stop in range(4)
        ]

    def next_place(self, hop):
        row, col = place_of(self.paths[0][hop + 1])
        for path in self.paths[1:]:
            other_row, other_col = place_of(path[hop + 1])
            here = is_at(self.row, self.col, path[hop])
            row, col = jnp.where(here, other_row, row), jnp.where(here, other_col, col)
        return row, col

    def greet(self, barrier):
        for path in self.paths:
            for hop in range(3):
                for here, there in ((path[hop], path[hop + 1]), (path[hop + 1], path[hop])):
                    @pl.when(is_at(self.row, self.col, here))
                    def _(there=there):
                        pl.semaphore_signal(
                            barrier, inc=1, device_id=place_of(there), device_id_type=MESH)

    def count(self):
        one, two, none = jnp.int32(1), jnp.int32(2), jnp.int32(0)
        return jnp.where(self.stops[0] | self.stops[3], one, none) + jnp.where(
            self.stops[1] | self.stops[2], two, none)


def greet_neighbours(barrier, row, col):
    for has, device in (
        (row > 0, (row - 1, col)),
        (row < N_ROW - 1, (row + 1, col)),
        (col > 0, (row, col - 1)),
        (col < N_COL - 1, (row, col + 1)),
    ):
        @pl.when(has)
        def _(device=device):
            pl.semaphore_signal(barrier, inc=1, device_id=device, device_id_type=MESH)


def neighbour_count(row, col):
    one, none = jnp.int32(1), jnp.int32(0)
    has = (row > 0, row < N_ROW - 1, col > 0, col < N_COL - 1)
    return sum(jnp.where(h, one, none) for h in has)


CHUNKS = ((0, 64), (64, 64), (128, 64), (192, 64), (256, 64), (320, 64))
TOPS = 4
LOWS = (4, 5)
EVERY = 6


class Halo:
    def __init__(self, ext, way, detour, left_sems, up_sems, corner_sems, detour_sems, row, col):
        self.ext, self.row, self.col = ext, row, col
        self.left_sems, self.up_sems, self.corner_sems = left_sems, up_sems, corner_sems
        self.detour, self.detour_sems = detour, detour_sems
        self.way, self.stops = way, way.stops
        self.sends_left, self.takes_right = col > 0, col < N_COL - 1
        self.sends_up, self.takes_below = row > 0, row < N_ROW - 1
        self.sends_direct = self.sends_up & jnp.logical_not(self.stops[0])

    def left(self, index):
        start, rows = CHUNKS[index]
        return remote(
            self.ext.at[:, pl.ds(0, 2), pl.ds(start, rows), :],
            self.ext.at[:, pl.ds(3, 2), pl.ds(start, rows), :],
            self.left_sems.at[0, index], self.left_sems.at[1, index],
            (self.row, jnp.maximum(self.col - 1, 0)),
        )

    def over(self, index, blocks, sems):
        start, rows = CHUNKS[index]
        return remote(
            self.ext.at[:, blocks, pl.ds(start, rows), :],
            self.ext.at[:, blocks, pl.ds(384 + start, rows), :],
            sems.at[0, index], sems.at[1, index],
            (jnp.maximum(self.row - 1, 0), self.col),
        )

    def up(self, index):
        return self.over(index, pl.ds(0, 3), self.up_sems)

    def corner(self, index):
        return self.over(index, pl.ds(3, 2), self.corner_sems)

    def detour_hop(self, hop, index):
        start, rows = CHUNKS[index]
        first, last = hop == 0, hop == 2
        source = self.ext if first else self.detour
        target = self.ext.at[:, pl.ds(0, 3), pl.ds(384 + start, rows), :] if last else (
            self.detour.at[:, :, pl.ds(start, rows), :])
        return remote(
            source.at[:, pl.ds(0, 3), pl.ds(start, rows), :], target,
            self.detour_sems.at[0, index],
            self.up_sems.at[1, index] if last else self.detour_sems.at[1, index],
            self.way.next_place(hop),
        )

    def pass_on(self, index):
        for hop in (1, 2):
            @pl.when(self.stops[hop])
            def _(hop=hop):
                self.detour_hop(hop - 1, index).wait_recv()
                self.detour_hop(hop, index).start()

    def clear_edges(self):
        @pl.when(self.col == N_COL - 1)
        def _():
            for channel in range(2):
                for block in (3, 4):
                    self.ext[channel, block] = jnp.zeros((EXT, 128), F32)

        @pl.when(self.row == N_ROW - 1)
        def _():
            for channel in range(2):
                for block in range(5):
                    self.ext[channel, block, 384:640] = jnp.zeros((256, 128), F32)

    def send_left(self, index):
        @pl.when(self.sends_left)
        def _():
            self.left(index).start()

    def send_up(self, index):
        @pl.when(self.sends_direct)
        def _():
            self.up(index).start()

        @pl.when(self.stops[0])
        def _():
            self.detour_hop(0, index).start()

    def forward_corner(self, index):
        @pl.when(self.takes_right)
        def _():
            self.left(index).wait_recv()

            @pl.when(self.sends_up)
            def _():
                self.corner(index).start()

    def finish(self):
        @pl.when(self.takes_right)
        def _():
            for index in LOWS:
                self.left(index).wait_recv()

        @pl.when(self.takes_below)
        def _():
            for index in range(TOPS):
                self.up(index).wait_recv()

        @pl.when(self.takes_below & self.takes_right)
        def _():
            for index in range(TOPS):
                self.corner(index).wait_recv()

        @pl.when(self.sends_left)
        def _():
            for index in range(EVERY):
                self.left(index).wait_send()

        @pl.when(self.sends_direct)
        def _():
            for index in range(TOPS):
                self.up(index).wait_send()

        for hop in range(3):
            @pl.when(self.stops[hop])
            def _(hop=hop):
                for index in range(TOPS):
                    self.detour_hop(hop, index).wait_send()

        @pl.when(self.sends_up & self.takes_right)
        def _():
            for index in range(TOPS):
                self.corner(index).wait_send()


def halo_sems():
    dma = pltpu.SemaphoreType.DMA
    return [pltpu.VMEM((2, 3, 256, 128), F32), dma((2, EVERY)), dma((2, TOPS)), dma((2, TOPS)),
            dma((2, TOPS))]


def fetch_kernel(object_ref, measured_ref, order_ref, ext_ref, sorted_ref,
                 turned, measured, load_sems, *sems):
    row, col = place()
    barrier = pltpu.get_barrier_semaphore()
    greet_neighbours(barrier, row, col)
    way = Detour(UP_DETOURS, row, col)
    way.greet(barrier)
    loads = []
    for channel in range(2):
        for block in range(3):
            load = pltpu.make_async_copy(
                object_ref.at[channel, :, pl.ds(block * 128, 128)],
                ext_ref.at[channel, block, pl.ds(0, TILE), :],
                load_sems.at[channel * 3 + block],
            )
            load.start()
            loads.append(load)
    load_frames = pltpu.make_async_copy(measured_ref, measured, load_sems.at[6])
    load_frames.start()
    halo = Halo(ext_ref, way, *sems, row, col)
    halo.clear_edges()
    for load in loads:
        load.wait()
    pl.semaphore_wait(barrier, neighbour_count(row, col) + way.count())
    for index in range(EVERY):
        halo.send_left(index)
    for index in range(TOPS):
        halo.send_up(index)

    def sort_frame(frame, carry):
        value = measured[frame]
        total = jnp.zeros((256, 256), F32)
        for _ in range(3):
            piece = value.astype(BF16)
            value = value - piece.astype(F32)
            total = total + jnp.dot(piece, order_ref[...], preferred_element_type=F32)
        for block in range(2):
            turned[block] = total[:, block * 128:block * 128 + 128]
        for block in range(2):
            for parity in range(2):
                sorted_ref[frame, parity, :, block * 128:block * 128 + 128] = (
                    turned[block, pl.ds(parity, 128, stride=2), :])
        return carry

    load_frames.wait()
    share = measured.shape[0] // TOPS
    for index in range(TOPS):
        lax.fori_loop(index * share, (index + 1) * share, sort_frame, 0)
        halo.pass_on(index)
        halo.forward_corner(index)
    halo.finish()


def fetch(object_field, measured, order):
    dma = pltpu.SemaphoreType.DMA
    count = measured.shape[0]
    return pl.pallas_call(
        fetch_kernel,
        name="fetch",
        out_shape=(
            jax.ShapeDtypeStruct((2, 5, EXT, 128), F32),
            jax.ShapeDtypeStruct((count, 2, 128, 256), F32),
        ),
        in_specs=[HBM_SPEC, HBM_SPEC, VMEM_SPEC],
        out_specs=(VMEM_SPEC, VMEM_SPEC),
        scratch_shapes=[
            pltpu.VMEM((2, 256, 128), F32), pltpu.VMEM((count, 256, 256), F32), dma((7,)),
        ] + halo_sems(),
        compiler_params=pltpu.CompilerParams(
            collective_id=0, has_side_effects=True, vmem_limit_bytes=FETCH_VMEM),
    )(*(pltpu.with_memory_space_constraint(a, pltpu.HBM) for a in (object_field, measured)), order)


def halves(value):
    high = value.astype(BF16)
    low = (value - high.astype(F32)).astype(BF16)
    return high, low


def dot(left, right):
    return jnp.dot(left, right, preferred_element_type=F32)


def times_table(value, tables, index):
    high, low = halves(value)
    return dot(high, tables[index]) + dot(low, tables[index]) + dot(high, tables[index + 1])


def table_times(tables, index, value):
    high, low = halves(value)
    return dot(tables[index], high) + dot(tables[index + 1], high) + dot(tables[index], low)


def beside(a, b):
    return jnp.concatenate([a, b], axis=1)


def above(a, b):
    return jnp.concatenate([a, b], axis=0)


def frames_kernel(batch, counts_ref, first_ref, positions_ref, ext_ref, probe_ref, sorted_ref,
                  tables, grad_ref, probe_grad_ref):
    live = counts_ref[0, 0]
    first = jnp.minimum(first_ref[0, 0], live)
    start, end = (0, first) if batch == 0 else (first, live)
    for channel in range(2):
        for block in range(5):
            grad_ref[channel, block] = jnp.zeros((EXT, 128), F32)
    probe_grad_ref[...] = jnp.zeros_like(probe_grad_ref)
    lanes = lax.broadcasted_iota(jnp.int32, (256, 128), 1)

    def add_frame(frame, carry):
        row_start = positions_ref[0, frame]
        col_start = positions_ref[1, frame]
        block0 = col_start // 128
        shift = col_start - block0 * 128
        rows = pl.ds(row_start, 256)
        back_shift = jnp.bitwise_and(128 - shift, 127)

        window = []
        for channel in range(2):
            turned = [
                pltpu.roll(ext_ref[channel, block0 + block, rows, :], back_shift, 1)
                for block in range(3)
            ]
            keep = lanes < 128 - shift
            window.append([jnp.where(keep, turned[b], turned[b + 1]) for b in range(2)])
        probe = [[probe_ref[channel, :, b * 128:b * 128 + 128] for b in range(2)]
                 for channel in range(2)]
        exit_re = [probe[0][b] * window[0][b] - probe[1][b] * window[1][b] for b in range(2)]
        exit_im = [probe[0][b] * window[1][b] + probe[1][b] * window[0][b] for b in range(2)]
        y0 = times_table(beside(exit_re[0] + exit_re[1], exit_im[0] + exit_im[1]), tables, 0)
        y1 = times_table(beside(exit_re[0] - exit_re[1], exit_im[0] - exit_im[1]), tables, 2)

        def stacked(t0, t1):
            return above(beside(t0[:, :128], t1[:, :128]), beside(t0[:, 128:], t1[:, 128:]))

        w0 = table_times(tables, 4, stacked(y0[:128] + y0[128:], y1[:128] + y1[128:]))
        w1 = table_times(tables, 6, stacked(y0[:128] - y0[128:], y1[:128] - y1[128:]))

        def weighted(w, parity):
            re, im = w[:128], w[128:]
            residue = re * re + im * im - sorted_ref[frame, parity]
            return above(residue * re, residue * im)

        u0 = table_times(tables, 0, weighted(w0, 0))
        u1 = table_times(tables, 2, weighted(w1, 1))
        top, bottom = u0 + u1, u0 - u1
        z_re = above(top[:128], bottom[:128])
        z_im = above(top[128:], bottom[128:])
        v0 = times_table(beside(z_re[:, :128], z_im[:, :128]), tables, 4)
        v1 = times_table(beside(z_re[:, 128:], z_im[:, 128:]), tables, 6)
        back_re = [v0[:, :128] + v1[:, :128], v0[:, :128] - v1[:, :128]]
        back_im = [v0[:, 128:] + v1[:, 128:], v0[:, 128:] - v1[:, 128:]]

        for b in range(2):
            at = slice(b * 128, b * 128 + 128)
            probe_grad_ref[0, :, at] += window[0][b] * back_re[b] + window[1][b] * back_im[b]
            probe_grad_ref[1, :, at] += window[0][b] * back_im[b] - window[1][b] * back_re[b]
        before = lanes < shift
        zero = jnp.zeros((256, 128), F32)
        for channel in range(2):
            if channel == 0:
                term = [probe[0][b] * back_re[b] + probe[1][b] * back_im[b] for b in range(2)]
            else:
                term = [probe[0][b] * back_im[b] - probe[1][b] * back_re[b] for b in range(2)]
            turned = [pltpu.roll(term[b], shift, 1) for b in range(2)]
            adds = [
                jnp.where(before, zero, turned[0]),
                jnp.where(before, turned[0], turned[1]),
                jnp.where(before, turned[1], zero),
            ]
            for block in range(3):
                at = (channel, block0 + block, rows, slice(None))
                grad_ref[at] = grad_ref[at] + adds[block]
        return carry

    lax.fori_loop(start, end, add_frame, 0)


def frames(batch, counts, first, positions, ext, probe, ordered, tables):
    return pl.pallas_call(
        functools.partial(frames_kernel, batch),
        name=f"frames{batch}",
        out_shape=(
            jax.ShapeDtypeStruct((2, 5, EXT, 128), F32),
            jax.ShapeDtypeStruct((2, PROBE, PROBE), F32),
        ),
        in_specs=[SMEM_SPEC, SMEM_SPEC, SMEM_SPEC] + [VMEM_SPEC] * 4,
        out_specs=(VMEM_SPEC, VMEM_SPEC),
        compiler_params=pltpu.CompilerParams(vmem_limit_bytes=FRAMES_VMEM),
    )(counts, first, positions, ext, probe, ordered, tables)


AROUND = tuple((i, j) for i in range(4) for j in range(4) if i or j)


class Reduce:
    def __init__(self, grad, half, got_half, got_plane, got_z, sums, sems, row, col):
        self.grad, self.half, self.got_half = grad, half, got_half
        self.got_plane, self.got_z, self.sums, self.sems = got_plane, got_z, sums, sems
        self.row, self.col, self.core = row, col, row % 2
        self.y = (row % 8) // 2
        self.x = (row // 8) * 2 + col // 8
        self.z = col % 8

    def partner(self):
        return (self.row + 1 - 2 * self.core, self.col)

    def plane(self, i, j):
        x, y = (self.x + i) % 4, (self.y + j) % 4
        device = ((x // 2) * 8 + y * 2 + self.core, (x % 2) * 8 + self.z)
        return pl.ds(pl.multiple_of((x * 4 + y) * 16, 16), 16), device

    def over_z_to(self, step):
        z = (self.z + step) % 8
        return z, (self.row, (self.col // 8) * 8 + z)

    def peers(self):
        found = [self.partner()]
        found += [self.plane(i, j)[1] for i, j in AROUND]
        found += [self.over_z_to(step)[1] for step in range(1, 8)]
        return found

    def copy(self, src, dst, index, device):
        return remote(src, dst, self.sems.at[0, index], self.sems.at[1, index], device)

    def pair(self):
        return self.copy(self.grad.at[1 - self.core], self.got_half, 0, self.partner())

    def out(self, n):
        rows, device = self.plane(*AROUND[n])
        return self.copy(self.half.at[rows, :], self.got_plane.at[n], 1 + n, device)

    def along(self, step):
        return self.copy(
            self.got_z.at[self.z], self.got_z.at[self.z], 15 + step, self.over_z_to(step)[1])

    def back(self, n):
        rows = self.plane(0, 0)[0]
        mine = self.sums.at[self.core, rows, :]
        return self.copy(mine, mine, 23 + n, self.plane(*AROUND[n])[1])

    def back_pair(self):
        mine = self.sums.at[self.core]
        return self.copy(mine, mine, 38, self.partner())

    def begin(self):
        self.pair().start()

    def to_plane(self):
        self.pair().wait_recv()
        self.half[...] = self.grad[self.core] + self.got_half[...]
        for n in range(15):
            self.out(n).start()

    def to_z(self):
        for n in range(15):
            self.out(n).wait_recv()
        total = self.half[self.plane(0, 0)[0], :]
        for n in range(15):
            total = total + self.got_plane[n]
        self.got_z[self.z] = total
        for step in range(1, 8):
            self.along(step).start()

    def from_z(self):
        for step in range(1, 8):
            theirs = self.got_z.at[(self.z + 8 - step) % 8]
            self.copy(theirs, theirs, 15 + step, self.over_z_to(step)[1]).wait_recv()
        total = self.got_z[0]
        for z in range(1, 8):
            total = total + self.got_z[z]
        self.sums[self.core, self.plane(0, 0)[0], :] = total
        for n in range(15):
            self.back(n).start()

    def from_plane(self):
        for n in range(15):
            i, j = AROUND[n]
            theirs = self.sums.at[self.core, self.plane(4 - i, 4 - j)[0], :]
            self.copy(theirs, theirs, 23 + n, self.plane(i, j)[1]).wait_recv()
        self.back_pair().start()

    def end(self):
        theirs = self.sums.at[1 - self.core]
        self.copy(theirs, theirs, 38, self.partner()).wait_recv()

    def drain(self):
        self.pair().wait_send()
        for n in range(15):
            self.out(n).wait_send()
            self.back(n).wait_send()
        for step in range(1, 8):
            self.along(step).wait_send()
        self.back_pair().wait_send()


def exchange_kernel(refetch, object_ref, grad_ref, probe_ref, probe_grad_ref, out_ref, probe_out,
                    from_above, from_left, joined, half, got_half, got_plane, got_z, sums,
                    detour, down_sems, right_sems, reduce_sems, detour_sems, *sems):
    row, col = place()
    reduce = Reduce(
        probe_grad_ref, half, got_half, got_plane, got_z, sums, reduce_sems, row, col)
    barrier = pltpu.get_barrier_semaphore()
    greet_neighbours(barrier, row, col)
    down_way = Detour(DOWN_DETOURS if refetch else DOWN_DETOURS[:1], row, col)
    down_way.greet(barrier)
    if refetch:
        up_way = Detour(UP_DETOURS, row, col)
        up_way.greet(barrier)
    for device in reduce.peers():
        pl.semaphore_signal(barrier, inc=1, device_id=device, device_id_type=MESH)
    stops = (down_way.first, down_way.stops)
    sends_down, takes_above = row < N_ROW - 1, row > 0
    sends_right, takes_left = col < N_COL - 1, col > 0
    if refetch:
        halo = Halo(out_ref, up_way, *sems, row, col)
        halo.clear_edges()

    @pl.when((row == 0) | (col == N_COL - 1))
    def _():
        for channel in range(2):
            for block in (3, 4):
                from_above[channel, block] = jnp.zeros((256, 128), F32)

    @pl.when(row == 0)
    def _():
        for channel in range(2):
            for block in range(3):
                from_above[channel, block] = jnp.zeros((256, 128), F32)

    @pl.when(col == 0)
    def _():
        for channel in range(2):
            for block in range(2):
                from_left[channel, block] = jnp.zeros((TILE, 128), F32)

    greeted = 23 + neighbour_count(row, col) + down_way.count()
    if refetch:
        greeted = greeted + up_way.count()
    pl.semaphore_wait(barrier, greeted)

    def down(index, part):
        blocks = pl.ds(3, 2) if part == 0 else pl.ds(0, 3)
        start, rows = CHUNKS[index]
        return remote(
            grad_ref.at[:, blocks, pl.ds(384 + start, rows), :],
            from_above.at[:, blocks, pl.ds(start, rows), :],
            down_sems.at[0, part, index], down_sems.at[1, part, index],
            (jnp.minimum(row + 1, N_ROW - 1), col),
        )

    def detour_hop(hop, index, part):
        start, rows = CHUNKS[index]
        blocks = pl.ds(3, 2) if part == 0 else pl.ds(0, 3)
        here = pl.ds(start, rows)
        source = detour.at[:, blocks, here, :] if hop else (
            grad_ref.at[:, blocks, pl.ds(384 + start, rows), :])
        target = (from_above if hop == 2 else detour).at[:, blocks, here, :]
        return remote(
            source, target, detour_sems.at[0, part, index],
            (down_sems if hop == 2 else detour_sems).at[1, part, index],
            down_way.next_place(hop),
        )

    def pass_on(index, part):
        for hop in (1, 2):
            @pl.when(stops[part][hop])
            def _(hop=hop):
                detour_hop(hop - 1, index, part).wait_recv()
                detour_hop(hop, index, part).start()

    needs = (sends_down & sends_right, sends_down)
    takes = (takes_above & sends_right, takes_above)
    straight = [needs[part] & jnp.logical_not(stops[part][0]) for part in range(2)]

    def send_down(index, part):
        @pl.when(straight[part])
        def _():
            down(index, part).start()

        @pl.when(stops[part][0])
        def _():
            detour_hop(0, index, part).start()

    def right(index):
        start, rows = CHUNKS[index]
        if index in LOWS:
            source = grad_ref.at[:, pl.ds(3, 2), pl.ds(start, rows), :]
        else:
            source = joined.at[:, :, pl.ds(start, rows), :]
        return remote(
            source, from_left.at[:, :, pl.ds(start, rows), :],
            right_sems.at[0, index], right_sems.at[1, index],
            (row, jnp.minimum(col + 1, N_COL - 1)),
        )

    def send_right(index):
        @pl.when(sends_right)
        def _():
            right(index).start()

    def join(index):
        start, rows = CHUNKS[index]
        at = slice(start, start + rows)

        @pl.when(takes[0])
        def _():
            down(index, 0).wait_recv()

        for channel in range(2):
            for block in range(2):
                joined[channel, block, at] = (
                    grad_ref[channel, 3 + block, at] + from_above[channel, 3 + block, at])
        send_right(index)

    def update(index):
        start, rows = CHUNKS[index]
        at = slice(start, start + rows)
        if index < TOPS:
            @pl.when(takes_above)
            def _():
                down(index, 1).wait_recv()

        @pl.when(takes_left)
        def _():
            right(index).wait_recv()

        for channel in range(2):
            for block in range(3):
                grad = grad_ref[channel, block, at]
                if index < TOPS:
                    grad = grad + from_above[channel, block, at]
                if block < 2:
                    grad = grad + from_left[channel, block, at]
                value = object_ref[channel, block, at] - 0.1 * grad
                if refetch:
                    out_ref[channel, block, at] = value
                else:
                    out_ref[channel, at, block * 128:block * 128 + 128] = value
        if refetch:
            halo.send_left(index)
            if index < TOPS:
                halo.send_up(index)

    def forward(index):
        if refetch:
            halo.forward_corner(index)

    def pass_up(index):
        if refetch:
            halo.pass_on(index)

    reduce.begin()
    send_right(4)
    send_right(5)
    send_down(0, 0)
    send_down(1, 0)
    reduce.to_plane()
    send_down(2, 0)
    send_down(3, 0)
    for index in range(TOPS):
        send_down(index, 1)
    pass_on(0, 0)
    pass_on(1, 0)
    update(4)
    reduce.to_z()
    join(0)
    join(1)
    pass_on(2, 0)
    pass_on(3, 0)
    join(2)
    join(3)
    pass_on(0, 1)
    pass_on(1, 1)
    if refetch:
        update(0)
        reduce.from_z()
        update(1)
        pass_on(2, 1)
        pass_on(3, 1)
        forward(0)
        update(2)
        pass_up(0)
        forward(1)
        update(3)
        update(5)
        pass_up(1)
        reduce.from_plane()
        for index in (2, 3):
            forward(index)
            pass_up(index)
    else:
        update(5)
        reduce.from_z()
        pass_on(2, 1)
        pass_on(3, 1)
        update(0)
        update(1)
        reduce.from_plane()
        update(2)
        update(3)
    reduce.end()
    step_size = 0.5 / math.sqrt(N_ROW * N_COL * 8)
    probe_out[...] = probe_ref[...] - step_size * sums[...]
    if refetch:
        halo.finish()
    reduce.drain()
    for part in range(2):
        @pl.when(straight[part])
        def _(part=part):
            for index in range(TOPS):
                down(index, part).wait_send()

        for hop in range(3):
            @pl.when(stops[part][hop])
            def _(hop=hop, part=part):
                for index in range(TOPS):
                    detour_hop(hop, index, part).wait_send()

    @pl.when(sends_right)
    def _():
        for index in range(EVERY):
            right(index).wait_send()


def exchange(refetch, ext, grad, probe, probe_grad):
    dma = pltpu.SemaphoreType.DMA
    out = (2, 5, EXT, 128) if refetch else (2, TILE, TILE)
    return pl.pallas_call(
        functools.partial(exchange_kernel, refetch),
        name=f"exchange{int(refetch)}",
        out_shape=(
            jax.ShapeDtypeStruct(out, F32), jax.ShapeDtypeStruct((2, PROBE, PROBE), F32)),
        in_specs=[VMEM_SPEC] * 4,
        out_specs=(VMEM_SPEC, VMEM_SPEC),
        scratch_shapes=[
            pltpu.VMEM((2, 5, 256, 128), F32),
            pltpu.VMEM((2, 2, TILE, 128), F32),
            pltpu.VMEM((2, 2, 256, 128), F32),
            pltpu.VMEM((256, 256), F32),
            pltpu.VMEM((256, 256), F32),
            pltpu.VMEM((15, 16, 256), F32),
            pltpu.VMEM((8, 16, 256), F32),
            pltpu.VMEM((2, 256, 256), F32),
            pltpu.VMEM((2, 5, 256, 128), F32),
            dma((2, 2, TOPS)),
            dma((2, EVERY)),
            dma((2, 39)),
            dma((2, 2, TOPS)),
        ] + (halo_sems() if refetch else []),
        compiler_params=pltpu.CompilerParams(
            collective_id=1 + int(refetch), has_side_effects=True,
            vmem_limit_bytes=EXCHANGE_VMEM),
    )(ext, grad, probe, probe_grad)


def per_device(object_field, illumination, measured, positions, frame_counts, first_count):
    tables = jnp.asarray(dft_tables())
    order = jnp.asarray(deinterleave_table())
    positions = positions[0, 0].T
    probe = illumination
    ext, ordered = fetch(object_field, measured[0, 0], order)
    grad, probe_grad = frames(
        0, frame_counts, first_count, positions, ext, probe, ordered, tables)
    ext, probe = exchange(True, ext, grad, probe, probe_grad)
    grad, probe_grad = frames(
        1, frame_counts, first_count, positions, ext, probe, ordered, tables)
    new_object, probe = exchange(False, ext, grad, probe, probe_grad)
    return new_object, probe


def solution(mesh):
    in_specs = (
        P(None, "row", "col"),
        P(),
        P("row", "col", None, None, None),
        P("row", "col", None, None),
        P("row", "col"),
        P("row", "col"),
    )
    out_specs = (P(None, "row", "col"), P())
    return jax.shard_map(
        per_device, mesh=mesh, in_specs=in_specs, out_specs=out_specs, check_vma=False
    )
```

```python
import functools
import math

import jax
import jax.numpy as jnp
import numpy as np
from jax import lax
from jax.experimental import pallas as pl
from jax.experimental.pallas import tpu as pltpu
from jax.sharding import PartitionSpec as P

MESH = pl.DeviceIdType.MESH
TILE, PROBE, EXT = 384, 256, 640
N_ROW = N_COL = 16
F32, BF16 = jnp.float32, jnp.bfloat16
FETCH_VMEM, FRAMES_VMEM, EXCHANGE_VMEM = 14 << 20, 16 << 20, 18 << 20
VMEM_SPEC = pl.BlockSpec(memory_space=pltpu.VMEM)
SMEM_SPEC = pl.BlockSpec(memory_space=pltpu.SMEM)
HBM_SPEC = pl.BlockSpec(memory_space=pltpu.HBM)


def split_bf16(table):
    high = table.astype(np.float32).astype(BF16)
    low = (table - high.astype(np.float64)).astype(np.float32).astype(BF16)
    return high, low


def dft_tables():
    n = np.arange(128)[:, None]
    parts = []
    for parity in (0, 1):
        k = 2 * np.arange(128)[None, :] + parity
        angle = ((n * k) % 256) * (2.0 * np.pi / 256.0)
        c, s = np.cos(angle) / 16.0, np.sin(angle) / 16.0
        table = np.block([[c, -s], [s, c]])
        parts.append((split_bf16(table), split_bf16(table.T)))
    order = []
    for transposed in (0, 1):
        for parity in (0, 1):
            order.extend(parts[parity][transposed])
    return np.stack(order)


def deinterleave_table():
    table = np.zeros((256, 256), np.float32)
    index = np.arange(128)
    table[2 * index, index] = 1.0
    table[2 * index + 1, 128 + index] = 1.0
    return table.astype(BF16)


def place():
    row, col = lax.axis_index("row"), lax.axis_index("col")
    return row, col


def remote(src, dst, send_sem, recv_sem, device):
    return pltpu.make_async_remote_copy(
        src_ref=src, dst_ref=dst, send_sem=send_sem, recv_sem=recv_sem,
        device_id=device, device_id_type=MESH,
    )


UP_DETOURS = (((8, 15), (14, 15), (6, 7), (7, 15)),)
DOWN_DETOURS = (((7, 0), (1, 0), (9, 8), (8, 0)), ((7, 15), (1, 15), (9, 7), (8, 15)))


def is_at(row, col, device):
    return (row == device[0]) & (col == device[1])


def place_of(device):
    return jnp.int32(device[0]), jnp.int32(device[1])


class Detour:
    def __init__(self, paths, row, col):
        self.paths, self.row, self.col = paths, row, col
        self.first = [is_at(row, col, paths[0][stop]) for stop in range(4)]
        self.stops = [
            functools.reduce(jnp.logical_or, [is_at(row, col, path[stop]) for path in paths])
            for stop in range(4)
        ]

    def next_place(self, hop):
        row, col = place_of(self.paths[0][hop + 1])
        for path in self.paths[1:]:
            other_row, other_col = place_of(path[hop + 1])
            here = is_at(self.row, self.col, path[hop])
            row, col = jnp.where(here, other_row, row), jnp.where(here, other_col, col)
        return row, col

    def greet(self, barrier):
        for path in self.paths:
            for hop in range(3):
                for here, there in ((path[hop], path[hop + 1]), (path[hop + 1], path[hop])):
                    @pl.when(is_at(self.row, self.col, here))
                    def _(there=there):
                        pl.semaphore_signal(
                            barrier, inc=1, device_id=place_of(there), device_id_type=MESH)

    def count(self):
        one, two, none = jnp.int32(1), jnp.int32(2), jnp.int32(0)
        return jnp.where(self.stops[0] | self.stops[3], one, none) + jnp.where(
            self.stops[1] | self.stops[2], two, none)


def greet_neighbours(barrier, row, col):
    for has, device in (
        (row > 0, (row - 1, col)),
        (row < N_ROW - 1, (row + 1, col)),
        (col > 0, (row, col - 1)),
        (col < N_COL - 1, (row, col + 1)),
    ):
        @pl.when(has)
        def _(device=device):
            pl.semaphore_signal(barrier, inc=1, device_id=device, device_id_type=MESH)


def neighbour_count(row, col):
    one, none = jnp.int32(1), jnp.int32(0)
    has = (row > 0, row < N_ROW - 1, col > 0, col < N_COL - 1)
    return sum(jnp.where(h, one, none) for h in has)


CHUNKS = ((0, 64), (64, 64), (128, 64), (192, 64), (256, 64), (320, 64))
TOPS = 4
LOWS = (4, 5)
EVERY = 6


class Halo:
    def __init__(self, ext, way, detour, left_sems, up_sems, corner_sems, detour_sems, row, col):
        self.ext, self.row, self.col = ext, row, col
        self.left_sems, self.up_sems, self.corner_sems = left_sems, up_sems, corner_sems
        self.detour, self.detour_sems = detour, detour_sems
        self.way, self.stops = way, way.stops
        self.sends_left, self.takes_right = col > 0, col < N_COL - 1
        self.sends_up, self.takes_below = row > 0, row < N_ROW - 1
        self.sends_direct = self.sends_up & jnp.logical_not(self.stops[0])

    def left(self, index):
        start, rows = CHUNKS[index]
        return remote(
            self.ext.at[:, pl.ds(0, 2), pl.ds(start, rows), :],
            self.ext.at[:, pl.ds(3, 2), pl.ds(start, rows), :],
            self.left_sems.at[0, index], self.left_sems.at[1, index],
            (self.row, jnp.maximum(self.col - 1, 0)),
        )

    def over(self, index, blocks, sems):
        start, rows = CHUNKS[index]
        return remote(
            self.ext.at[:, blocks, pl.ds(start, rows), :],
            self.ext.at[:, blocks, pl.ds(384 + start, rows), :],
            sems.at[0, index], sems.at[1, index],
            (jnp.maximum(self.row - 1, 0), self.col),
        )

    def up(self, index):
        return self.over(index, pl.ds(0, 3), self.up_sems)

    def corner(self, index):
        return self.over(index, pl.ds(3, 2), self.corner_sems)

    def detour_hop(self, hop, index):
        start, rows = CHUNKS[index]
        first, last = hop == 0, hop == 2
        source = self.ext if first else self.detour
        target = self.ext.at[:, pl.ds(0, 3), pl.ds(384 + start, rows), :] if last else (
            self.detour.at[:, :, pl.ds(start, rows), :])
        return remote(
            source.at[:, pl.ds(0, 3), pl.ds(start, rows), :], target,
            self.detour_sems.at[0, index],
            self.up_sems.at[1, index] if last else self.detour_sems.at[1, index],
            self.way.next_place(hop),
        )

    def pass_on(self, index):
        for hop in (1, 2):
            @pl.when(self.stops[hop])
            def _(hop=hop):
                self.detour_hop(hop - 1, index).wait_recv()
                self.detour_hop(hop, index).start()

    def clear_edges(self):
        @pl.when(self.col == N_COL - 1)
        def _():
            for channel in range(2):
                for block in (3, 4):
                    self.ext[channel, block] = jnp.zeros((EXT, 128), F32)

        @pl.when(self.row == N_ROW - 1)
        def _():
            for channel in range(2):
                for block in range(5):
                    self.ext[channel, block, 384:640] = jnp.zeros((256, 128), F32)

    def send_left(self, index):
        @pl.when(self.sends_left)
        def _():
            self.left(index).start()

    def send_up(self, index):
        @pl.when(self.sends_direct)
        def _():
            self.up(index).start()

        @pl.when(self.stops[0])
        def _():
            self.detour_hop(0, index).start()

    def forward_corner(self, index):
        @pl.when(self.takes_right)
        def _():
            self.left(index).wait_recv()

            @pl.when(self.sends_up)
            def _():
                self.corner(index).start()

    def finish(self):
        @pl.when(self.takes_right)
        def _():
            for index in LOWS:
                self.left(index).wait_recv()

        @pl.when(self.takes_below)
        def _():
            for index in range(TOPS):
                self.up(index).wait_recv()

        @pl.when(self.takes_below & self.takes_right)
        def _():
            for index in range(TOPS):
                self.corner(index).wait_recv()

        @pl.when(self.sends_left)
        def _():
            for index in range(EVERY):
                self.left(index).wait_send()

        @pl.when(self.sends_direct)
        def _():
            for index in range(TOPS):
                self.up(index).wait_send()

        for hop in range(3):
            @pl.when(self.stops[hop])
            def _(hop=hop):
                for index in range(TOPS):
                    self.detour_hop(hop, index).wait_send()

        @pl.when(self.sends_up & self.takes_right)
        def _():
            for index in range(TOPS):
                self.corner(index).wait_send()


def halo_sems():
    dma = pltpu.SemaphoreType.DMA
    return [pltpu.VMEM((2, 3, 256, 128), F32), dma((2, EVERY)), dma((2, TOPS)), dma((2, TOPS)),
            dma((2, TOPS))]


def fetch_kernel(object_ref, measured_ref, order_ref, ext_ref, sorted_ref,
                 turned, measured, load_sems, *sems):
    row, col = place()
    barrier = pltpu.get_barrier_semaphore()
    greet_neighbours(barrier, row, col)
    way = Detour(UP_DETOURS, row, col)
    way.greet(barrier)
    loads = []
    for channel in range(2):
        for block in range(3):
            load = pltpu.make_async_copy(
                object_ref.at[channel, :, pl.ds(block * 128, 128)],
                ext_ref.at[channel, block, pl.ds(0, TILE), :],
                load_sems.at[channel * 3 + block],
            )
            load.start()
            loads.append(load)
    load_frames = pltpu.make_async_copy(measured_ref, measured, load_sems.at[6])
    load_frames.start()
    halo = Halo(ext_ref, way, *sems, row, col)
    halo.clear_edges()
    for load in loads:
        load.wait()
    pl.semaphore_wait(barrier, neighbour_count(row, col) + way.count())
    for index in range(EVERY):
        halo.send_left(index)
    for index in range(TOPS):
        halo.send_up(index)

    def sort_frame(frame, carry):
        value = measured[frame]
        total = jnp.zeros((256, 256), F32)
        for _ in range(3):
            piece = value.astype(BF16)
            value = value - piece.astype(F32)
            total = total + jnp.dot(piece, order_ref[...], preferred_element_type=F32)
        for block in range(2):
            turned[block] = total[:, block * 128:block * 128 + 128]
        for block in range(2):
            for parity in range(2):
                sorted_ref[frame, parity, :, block * 128:block * 128 + 128] = (
                    turned[block, pl.ds(parity, 128, stride=2), :])
        return carry

    load_frames.wait()
    share = measured.shape[0] // TOPS
    for index in range(TOPS):
        lax.fori_loop(index * share, (index + 1) * share, sort_frame, 0)
        halo.pass_on(index)
        halo.forward_corner(index)
    halo.finish()


def fetch(object_field, measured, order):
    dma = pltpu.SemaphoreType.DMA
    count = measured.shape[0]
    return pl.pallas_call(
        fetch_kernel,
        name="fetch",
        out_shape=(
            jax.ShapeDtypeStruct((2, 5, EXT, 128), F32),
            jax.ShapeDtypeStruct((count, 2, 128, 256), F32),
        ),
        in_specs=[HBM_SPEC, HBM_SPEC, VMEM_SPEC],
        out_specs=(VMEM_SPEC, VMEM_SPEC),
        scratch_shapes=[
            pltpu.VMEM((2, 256, 128), F32), pltpu.VMEM((count, 256, 256), F32), dma((7,)),
        ] + halo_sems(),
        compiler_params=pltpu.CompilerParams(
            collective_id=0, has_side_effects=True, vmem_limit_bytes=FETCH_VMEM),
    )(*(pltpu.with_memory_space_constraint(a, pltpu.HBM) for a in (object_field, measured)), order)


def halves(value):
    high = value.astype(BF16)
    low = (value - high.astype(F32)).astype(BF16)
    return high, low


def dot(left, right):
    return jnp.dot(left, right, preferred_element_type=F32)


def times_table(value, tables, index):
    high, low = halves(value)
    return dot(high, tables[index]) + dot(low, tables[index]) + dot(high, tables[index + 1])


def table_times(tables, index, value):
    high, low = halves(value)
    return dot(tables[index], high) + dot(tables[index + 1], high) + dot(tables[index], low)


def beside(a, b):
    return jnp.concatenate([a, b], axis=1)


def above(a, b):
    return jnp.concatenate([a, b], axis=0)


def frames_kernel(batch, counts_ref, first_ref, positions_ref, ext_ref, probe_ref, sorted_ref,
                  tables, grad_ref, probe_grad_ref):
    live = counts_ref[0, 0]
    first = jnp.minimum(first_ref[0, 0], live)
    start, end = (0, first) if batch == 0 else (first, live)
    for channel in range(2):
        for block in range(5):
            grad_ref[channel, block] = jnp.zeros((EXT, 128), F32)
    probe_grad_ref[...] = jnp.zeros_like(probe_grad_ref)
    lanes = lax.broadcasted_iota(jnp.int32, (256, 128), 1)

    def load_window(frame):
        row_start, col_start = positions_ref[0, frame], positions_ref[1, frame]
        block0 = col_start // 128
        shift = col_start - block0 * 128
        rows = pl.ds(row_start, 256)
        back_shift = jnp.bitwise_and(128 - shift, 127)
        keep = lanes < 128 - shift
        window = []
        for channel in range(2):
            turned = [
                pltpu.roll(ext_ref[channel, block0 + block, rows, :], back_shift, 1)
                for block in range(3)
            ]
            window.append([jnp.where(keep, turned[b], turned[b + 1]) for b in range(2)])
        return window, block0, shift, rows

    def load_probe():
        return [[probe_ref[channel, :, b * 128:b * 128 + 128] for b in range(2)]
                for channel in range(2)]

    def stacked(t0, t1):
        return above(beside(t0[:, :128], t1[:, :128]), beside(t0[:, 128:], t1[:, 128:]))

    def across(window):
        probe = load_probe()
        re = [probe[0][b] * window[0][b] - probe[1][b] * window[1][b] for b in range(2)]
        im = [probe[0][b] * window[1][b] + probe[1][b] * window[0][b] for b in range(2)]
        return (times_table(beside(re[0] + re[1], im[0] + im[1]), tables, 0),
                times_table(beside(re[0] - re[1], im[0] - im[1]), tables, 2))

    def along(y):
        y0, y1 = y
        return (table_times(tables, 4, stacked(y0[:128] + y0[128:], y1[:128] + y1[128:])),
                table_times(tables, 6, stacked(y0[:128] - y0[128:], y1[:128] - y1[128:])))

    def along_back(w, frame, valid):
        parts = []
        for parity in range(2):
            re, im = w[parity][:128], w[parity][128:]
            residue = re * re + im * im - sorted_ref[frame, parity]
            residue = jnp.where(valid, residue, jnp.zeros_like(residue))
            parts.append(table_times(tables, 2 * parity, above(residue * re, residue * im)))
        return parts

    def across_back(u):
        top, bottom = u[0] + u[1], u[0] - u[1]
        z_re = above(top[:128], bottom[:128])
        z_im = above(top[128:], bottom[128:])
        v0 = times_table(beside(z_re[:, :128], z_im[:, :128]), tables, 4)
        v1 = times_table(beside(z_re[:, 128:], z_im[:, 128:]), tables, 6)
        return ([v0[:, :128] + v1[:, :128], v0[:, :128] - v1[:, :128]],
                [v0[:, 128:] + v1[:, 128:], v0[:, 128:] - v1[:, 128:]])

    def add_probe_terms(windows, backs):
        for b in range(2):
            at = slice(b * 128, b * 128 + 128)
            re, im = probe_grad_ref[0, :, at], probe_grad_ref[1, :, at]
            for window, (back_re, back_im) in zip(windows, backs):
                re = re + (window[0][b] * back_re[b] + window[1][b] * back_im[b])
                im = im + (window[0][b] * back_im[b] - window[1][b] * back_re[b])
            probe_grad_ref[0, :, at] = re
            probe_grad_ref[1, :, at] = im

    def add_object_terms(place, back):
        block0, shift, rows = place
        back_re, back_im = back
        probe = load_probe()
        before = lanes < shift
        zero = jnp.zeros((256, 128), F32)
        for channel in range(2):
            if channel == 0:
                term = [probe[0][b] * back_re[b] + probe[1][b] * back_im[b] for b in range(2)]
            else:
                term = [probe[0][b] * back_im[b] - probe[1][b] * back_re[b] for b in range(2)]
            turned = [pltpu.roll(term[b], shift, 1) for b in range(2)]
            adds = [
                jnp.where(before, zero, turned[0]),
                jnp.where(before, turned[0], turned[1]),
                jnp.where(before, turned[1], zero),
            ]
            for block in range(3):
                at = (channel, block0 + block, rows, slice(None))
                grad_ref[at] = grad_ref[at] + adds[block]

    last = positions_ref.shape[1] - 1

    def add_pair(pair, carry):
        slots = [start + pair * 2 + k for k in range(2)]
        valid = [slot < end for slot in slots]
        slots = [jnp.minimum(slot, last) for slot in slots]
        windows, places = [], []
        for slot in slots:
            window, *spot = load_window(slot)
            windows.append(window)
            places.append(spot)
        y = [across(window) for window in windows]
        w = [along(each) for each in y]
        u = [along_back(w[k], slots[k], valid[k]) for k in range(2)]
        backs = [across_back(each) for each in u]
        add_probe_terms(windows, backs)
        for k in range(2):
            add_object_terms(places[k], backs[k])
        return carry

    lax.fori_loop(0, (end - start + 1) // 2, add_pair, 0)


def frames(batch, counts, first, positions, ext, probe, ordered, tables):
    return pl.pallas_call(
        functools.partial(frames_kernel, batch),
        name=f"frames{batch}",
        out_shape=(
            jax.ShapeDtypeStruct((2, 5, EXT, 128), F32),
            jax.ShapeDtypeStruct((2, PROBE, PROBE), F32),
        ),
        in_specs=[SMEM_SPEC, SMEM_SPEC, SMEM_SPEC] + [VMEM_SPEC] * 4,
        out_specs=(VMEM_SPEC, VMEM_SPEC),
        compiler_params=pltpu.CompilerParams(vmem_limit_bytes=FRAMES_VMEM),
    )(counts, first, positions, ext, probe, ordered, tables)


AROUND = tuple((i, j) for i in range(4) for j in range(4) if i or j)


class Reduce:
    def __init__(self, grad, half, got_half, got_plane, got_z, sums, sems, row, col):
        self.grad, self.half, self.got_half = grad, half, got_half
        self.got_plane, self.got_z, self.sums, self.sems = got_plane, got_z, sums, sems
        self.row, self.col, self.core = row, col, row % 2
        self.y = (row % 8) // 2
        self.x = (row // 8) * 2 + col // 8
        self.z = col % 8

    def partner(self):
        return (self.row + 1 - 2 * self.core, self.col)

    def plane(self, i, j):
        x, y = (self.x + i) % 4, (self.y + j) % 4
        device = ((x // 2) * 8 + y * 2 + self.core, (x % 2) * 8 + self.z)
        return pl.ds(pl.multiple_of((x * 4 + y) * 16, 16), 16), device

    def over_z_to(self, step):
        z = (self.z + step) % 8
        return z, (self.row, (self.col // 8) * 8 + z)

    def peers(self):
        found = [self.partner()]
        found += [self.plane(i, j)[1] for i, j in AROUND]
        found += [self.over_z_to(step)[1] for step in range(1, 8)]
        return found

    def copy(self, src, dst, index, device):
        return remote(src, dst, self.sems.at[0, index], self.sems.at[1, index], device)

    def pair(self):
        return self.copy(self.grad.at[1 - self.core], self.got_half, 0, self.partner())

    def out(self, n):
        rows, device = self.plane(*AROUND[n])
        return self.copy(self.half.at[rows, :], self.got_plane.at[n], 1 + n, device)

    def along(self, step):
        return self.copy(
            self.got_z.at[self.z], self.got_z.at[self.z], 15 + step, self.over_z_to(step)[1])

    def back(self, n):
        rows = self.plane(0, 0)[0]
        mine = self.sums.at[self.core, rows, :]
        return self.copy(mine, mine, 23 + n, self.plane(*AROUND[n])[1])

    def back_pair(self):
        mine = self.sums.at[self.core]
        return self.copy(mine, mine, 38, self.partner())

    def begin(self):
        self.pair().start()

    def to_plane(self):
        self.pair().wait_recv()
        self.half[...] = self.grad[self.core] + self.got_half[...]
        for n in range(15):
            self.out(n).start()

    def to_z(self):
        for n in range(15):
            self.out(n).wait_recv()
        total = self.half[self.plane(0, 0)[0], :]
        for n in range(15):
            total = total + self.got_plane[n]
        self.got_z[self.z] = total
        for step in range(1, 8):
            self.along(step).start()

    def from_z(self):
        for step in range(1, 8):
            theirs = self.got_z.at[(self.z + 8 - step) % 8]
            self.copy(theirs, theirs, 15 + step, self.over_z_to(step)[1]).wait_recv()
        total = self.got_z[0]
        for z in range(1, 8):
            total = total + self.got_z[z]
        self.sums[self.core, self.plane(0, 0)[0], :] = total
        for n in range(15):
            self.back(n).start()

    def from_plane(self):
        for n in range(15):
            i, j = AROUND[n]
            theirs = self.sums.at[self.core, self.plane(4 - i, 4 - j)[0], :]
            self.copy(theirs, theirs, 23 + n, self.plane(i, j)[1]).wait_recv()
        self.back_pair().start()

    def end(self):
        theirs = self.sums.at[1 - self.core]
        self.copy(theirs, theirs, 38, self.partner()).wait_recv()

    def drain(self):
        self.pair().wait_send()
        for n in range(15):
            self.out(n).wait_send()
            self.back(n).wait_send()
        for step in range(1, 8):
            self.along(step).wait_send()
        self.back_pair().wait_send()


def exchange_kernel(refetch, object_ref, grad_ref, probe_ref, probe_grad_ref, out_ref, probe_out,
                    from_above, from_left, joined, half, got_half, got_plane, got_z, sums,
                    detour, down_sems, right_sems, reduce_sems, detour_sems, *sems):
    row, col = place()
    reduce = Reduce(
        probe_grad_ref, half, got_half, got_plane, got_z, sums, reduce_sems, row, col)
    barrier = pltpu.get_barrier_semaphore()
    greet_neighbours(barrier, row, col)
    down_way = Detour(DOWN_DETOURS if refetch else DOWN_DETOURS[:1], row, col)
    down_way.greet(barrier)
    if refetch:
        up_way = Detour(UP_DETOURS, row, col)
        up_way.greet(barrier)
    for device in reduce.peers():
        pl.semaphore_signal(barrier, inc=1, device_id=device, device_id_type=MESH)
    stops = (down_way.first, down_way.stops)
    sends_down, takes_above = row < N_ROW - 1, row > 0
    sends_right, takes_left = col < N_COL - 1, col > 0
    if refetch:
        halo = Halo(out_ref, up_way, *sems, row, col)
        halo.clear_edges()

    @pl.when((row == 0) | (col == N_COL - 1))
    def _():
        for channel in range(2):
            for block in (3, 4):
                from_above[channel, block] = jnp.zeros((256, 128), F32)

    @pl.when(row == 0)
    def _():
        for channel in range(2):
            for block in range(3):
                from_above[channel, block] = jnp.zeros((256, 128), F32)

    @pl.when(col == 0)
    def _():
        for channel in range(2):
            for block in range(2):
                from_left[channel, block] = jnp.zeros((TILE, 128), F32)

    greeted = 23 + neighbour_count(row, col) + down_way.count()
    if refetch:
        greeted = greeted + up_way.count()
    pl.semaphore_wait(barrier, greeted)

    def down(index, part):
        blocks = pl.ds(3, 2) if part == 0 else pl.ds(0, 3)
        start, rows = CHUNKS[index]
        return remote(
            grad_ref.at[:, blocks, pl.ds(384 + start, rows), :],
            from_above.at[:, blocks, pl.ds(start, rows), :],
            down_sems.at[0, part, index], down_sems.at[1, part, index],
            (jnp.minimum(row + 1, N_ROW - 1), col),
        )

    def detour_hop(hop, index, part):
        start, rows = CHUNKS[index]
        blocks = pl.ds(3, 2) if part == 0 else pl.ds(0, 3)
        here = pl.ds(start, rows)
        source = detour.at[:, blocks, here, :] if hop else (
            grad_ref.at[:, blocks, pl.ds(384 + start, rows), :])
        target = (from_above if hop == 2 else detour).at[:, blocks, here, :]
        return remote(
            source, target, detour_sems.at[0, part, index],
            (down_sems if hop == 2 else detour_sems).at[1, part, index],
            down_way.next_place(hop),
        )

    def pass_on(index, part):
        for hop in (1, 2):
            @pl.when(stops[part][hop])
            def _(hop=hop):
                detour_hop(hop - 1, index, part).wait_recv()
                detour_hop(hop, index, part).start()

    needs = (sends_down & sends_right, sends_down)
    takes = (takes_above & sends_right, takes_above)
    straight = [needs[part] & jnp.logical_not(stops[part][0]) for part in range(2)]

    def send_down(index, part):
        @pl.when(straight[part])
        def _():
            down(index, part).start()

        @pl.when(stops[part][0])
        def _():
            detour_hop(0, index, part).start()

    def right(index):
        start, rows = CHUNKS[index]
        if index in LOWS:
            source = grad_ref.at[:, pl.ds(3, 2), pl.ds(start, rows), :]
        else:
            source = joined.at[:, :, pl.ds(start, rows), :]
        return remote(
            source, from_left.at[:, :, pl.ds(start, rows), :],
            right_sems.at[0, index], right_sems.at[1, index],
            (row, jnp.minimum(col + 1, N_COL - 1)),
        )

    def send_right(index):
        @pl.when(sends_right)
        def _():
            right(index).start()

    def join(index):
        start, rows = CHUNKS[index]
        at = slice(start, start + rows)

        @pl.when(takes[0])
        def _():
            down(index, 0).wait_recv()

        for channel in range(2):
            for block in range(2):
                joined[channel, block, at] = (
                    grad_ref[channel, 3 + block, at] + from_above[channel, 3 + block, at])
        send_right(index)

    def update(index):
        start, rows = CHUNKS[index]
        at = slice(start, start + rows)
        if index < TOPS:
            @pl.when(takes_above)
            def _():
                down(index, 1).wait_recv()

        @pl.when(takes_left)
        def _():
            right(index).wait_recv()

        for channel in range(2):
            for block in range(3):
                grad = grad_ref[channel, block, at]
                if index < TOPS:
                    grad = grad + from_above[channel, block, at]
                if block < 2:
                    grad = grad + from_left[channel, block, at]
                value = object_ref[channel, block, at] - 0.1 * grad
                if refetch:
                    out_ref[channel, block, at] = value
                else:
                    out_ref[channel, at, block * 128:block * 128 + 128] = value
        if refetch:
            halo.send_left(index)
            if index < TOPS:
                halo.send_up(index)

    def forward(index):
        if refetch:
            halo.forward_corner(index)

    def pass_up(index):
        if refetch:
            halo.pass_on(index)

    reduce.begin()
    send_right(4)
    send_right(5)
    send_down(0, 0)
    send_down(1, 0)
    reduce.to_plane()
    send_down(2, 0)
    send_down(3, 0)
    for index in range(TOPS):
        send_down(index, 1)
    pass_on(0, 0)
    pass_on(1, 0)
    update(4)
    reduce.to_z()
    late = down_way.stops[3]
    on_time = jnp.logical_not(late)
    pl.when(late)(reduce.from_z)
    join(0)
    join(1)
    pass_on(2, 0)
    pass_on(3, 0)
    join(2)
    join(3)
    pass_on(0, 1)
    pass_on(1, 1)
    if refetch:
        update(0)
        pl.when(late)(reduce.from_plane)
        pl.when(on_time)(reduce.from_z)
        update(1)
        pass_on(2, 1)
        pass_on(3, 1)
        forward(0)
        update(2)
        forward(1)
        update(3)
        update(5)
        pl.when(on_time)(reduce.from_plane)
        pass_up(0)
        pass_up(1)
        forward(2)
        forward(3)
        pass_up(2)
        pass_up(3)
    else:
        update(5)
        pl.when(on_time)(reduce.from_z)
        pl.when(late)(reduce.from_plane)
        pass_on(2, 1)
        pass_on(3, 1)
        update(0)
        update(1)
        pl.when(on_time)(reduce.from_plane)
        update(2)
        update(3)
    reduce.end()
    step_size = 0.5 / math.sqrt(N_ROW * N_COL * 8)
    probe_out[...] = probe_ref[...] - step_size * sums[...]
    if refetch:
        halo.finish()
    reduce.drain()
    for part in range(2):
        @pl.when(straight[part])
        def _(part=part):
            for index in range(TOPS):
                down(index, part).wait_send()

        for hop in range(3):
            @pl.when(stops[part][hop])
            def _(hop=hop, part=part):
                for index in range(TOPS):
                    detour_hop(hop, index, part).wait_send()

    @pl.when(sends_right)
    def _():
        for index in range(EVERY):
            right(index).wait_send()


def exchange(refetch, ext, grad, probe, probe_grad):
    dma = pltpu.SemaphoreType.DMA
    out = (2, 5, EXT, 128) if refetch else (2, TILE, TILE)
    return pl.pallas_call(
        functools.partial(exchange_kernel, refetch),
        name=f"exchange{int(refetch)}",
        out_shape=(
            jax.ShapeDtypeStruct(out, F32), jax.ShapeDtypeStruct((2, PROBE, PROBE), F32)),
        in_specs=[VMEM_SPEC] * 4,
        out_specs=(VMEM_SPEC, VMEM_SPEC),
        scratch_shapes=[
            pltpu.VMEM((2, 5, 256, 128), F32),
            pltpu.VMEM((2, 2, TILE, 128), F32),
            pltpu.VMEM((2, 2, 256, 128), F32),
            pltpu.VMEM((256, 256), F32),
            pltpu.VMEM((256, 256), F32),
            pltpu.VMEM((15, 16, 256), F32),
            pltpu.VMEM((8, 16, 256), F32),
            pltpu.VMEM((2, 256, 256), F32),
            pltpu.VMEM((2, 5, 256, 128), F32),
            dma((2, 2, TOPS)),
            dma((2, EVERY)),
            dma((2, 39)),
            dma((2, 2, TOPS)),
        ] + (halo_sems() if refetch else []),
        compiler_params=pltpu.CompilerParams(
            collective_id=1 + int(refetch), has_side_effects=True,
            vmem_limit_bytes=EXCHANGE_VMEM),
    )(ext, grad, probe, probe_grad)


def per_device(object_field, illumination, measured, positions, frame_counts, first_count):
    tables = jnp.asarray(dft_tables())
    order = jnp.asarray(deinterleave_table())
    positions = positions[0, 0].T
    probe = illumination
    ext, ordered = fetch(object_field, measured[0, 0], order)
    grad, probe_grad = frames(
        0, frame_counts, first_count, positions, ext, probe, ordered, tables)
    ext, probe = exchange(True, ext, grad, probe, probe_grad)
    grad, probe_grad = frames(
        1, frame_counts, first_count, positions, ext, probe, ordered, tables)
    new_object, probe = exchange(False, ext, grad, probe, probe_grad)
    return new_object, probe


def solution(mesh):
    in_specs = (
        P(None, "row", "col"),
        P(),
        P("row", "col", None, None, None),
        P("row", "col", None, None),
        P("row", "col"),
        P("row", "col"),
    )
    out_specs = (P(None, "row", "col"), P())
    return jax.shard_map(
        per_device, mesh=mesh, in_specs=in_specs, out_specs=out_specs, check_vma=False
    )
```

```python
import functools
import math

import jax
import jax.numpy as jnp
import numpy as np
from jax import lax
from jax.experimental import pallas as pl
from jax.experimental.pallas import tpu as pltpu
from jax.sharding import PartitionSpec as P

MESH = pl.DeviceIdType.MESH
TILE, PROBE, EXT = 384, 256, 640
N_ROW = N_COL = 16
F32, BF16 = jnp.float32, jnp.bfloat16
FETCH_VMEM, FRAMES_VMEM, EXCHANGE_VMEM = 14 << 20, 16 << 20, 18 << 20
VMEM_SPEC = pl.BlockSpec(memory_space=pltpu.VMEM)
SMEM_SPEC = pl.BlockSpec(memory_space=pltpu.SMEM)
HBM_SPEC = pl.BlockSpec(memory_space=pltpu.HBM)


def split_bf16(table):
    high = table.astype(np.float32).astype(BF16)
    low = (table - high.astype(np.float64)).astype(np.float32).astype(BF16)
    return high, low


def dft_tables():
    n = np.arange(128)[:, None]
    parts = []
    for parity in (0, 1):
        k = 2 * np.arange(128)[None, :] + parity
        angle = ((n * k) % 256) * (2.0 * np.pi / 256.0)
        c, s = np.cos(angle) / 16.0, np.sin(angle) / 16.0
        table = np.block([[c, -s], [s, c]])
        parts.append((split_bf16(table), split_bf16(table.T)))
    order = []
    for transposed in (0, 1):
        for parity in (0, 1):
            order.extend(parts[parity][transposed])
    return np.stack(order)


def deinterleave_table():
    table = np.zeros((256, 256), np.float32)
    index = np.arange(128)
    table[2 * index, index] = 1.0
    table[2 * index + 1, 128 + index] = 1.0
    return table.astype(BF16)


def place():
    row, col = lax.axis_index("row"), lax.axis_index("col")
    return row, col


def remote(src, dst, send_sem, recv_sem, device):
    return pltpu.make_async_remote_copy(
        src_ref=src, dst_ref=dst, send_sem=send_sem, recv_sem=recv_sem,
        device_id=device, device_id_type=MESH,
    )


UP_DETOURS = (((8, 15), (14, 15), (6, 7), (7, 15)),)
DOWN_DETOURS = (((7, 0), (1, 0), (9, 8), (8, 0)), ((7, 15), (1, 15), (9, 7), (8, 15)))


def is_at(row, col, device):
    return (row == device[0]) & (col == device[1])


def place_of(device):
    return jnp.int32(device[0]), jnp.int32(device[1])


class Detour:
    def __init__(self, paths, row, col):
        self.paths, self.row, self.col = paths, row, col
        self.each = [[is_at(row, col, path[stop]) for stop in range(4)] for path in paths]
        self.stops = [functools.reduce(jnp.logical_or, marks) for marks in zip(*self.each)]

    def next_place(self, hop):
        row, col = place_of(self.paths[0][hop + 1])
        for path in self.paths[1:]:
            other_row, other_col = place_of(path[hop + 1])
            here = is_at(self.row, self.col, path[hop])
            row, col = jnp.where(here, other_row, row), jnp.where(here, other_col, col)
        return row, col

    def greet(self, barrier):
        for path in self.paths:
            for hop in range(3):
                for here, there in ((path[hop], path[hop + 1]), (path[hop + 1], path[hop])):
                    @pl.when(is_at(self.row, self.col, here))
                    def _(there=there):
                        pl.semaphore_signal(
                            barrier, inc=1, device_id=place_of(there), device_id_type=MESH)

    def count(self):
        one, two, none = jnp.int32(1), jnp.int32(2), jnp.int32(0)
        return jnp.where(self.stops[0] | self.stops[3], one, none) + jnp.where(
            self.stops[1] | self.stops[2], two, none)


def greet_neighbours(barrier, row, col):
    for has, device in (
        (row > 0, (row - 1, col)),
        (row < N_ROW - 1, (row + 1, col)),
        (col > 0, (row, col - 1)),
        (col < N_COL - 1, (row, col + 1)),
    ):
        @pl.when(has)
        def _(device=device):
            pl.semaphore_signal(barrier, inc=1, device_id=device, device_id_type=MESH)


def neighbour_count(row, col):
    one, none = jnp.int32(1), jnp.int32(0)
    has = (row > 0, row < N_ROW - 1, col > 0, col < N_COL - 1)
    return sum(jnp.where(h, one, none) for h in has)


CHUNKS = ((0, 64), (64, 64), (128, 64), (192, 64), (256, 64), (320, 64))
TOPS = 4
LOWS = (4, 5)
EVERY = 6


class Halo:
    def __init__(self, ext, way, detour, left_sems, up_sems, corner_sems, detour_sems, row, col):
        self.ext, self.row, self.col = ext, row, col
        self.left_sems, self.up_sems, self.corner_sems = left_sems, up_sems, corner_sems
        self.detour, self.detour_sems = detour, detour_sems
        self.way, self.stops = way, way.stops
        self.sends_left, self.takes_right = col > 0, col < N_COL - 1
        self.sends_up, self.takes_below = row > 0, row < N_ROW - 1
        self.sends_direct = self.sends_up & jnp.logical_not(self.stops[0])

    def left(self, index):
        start, rows = CHUNKS[index]
        return remote(
            self.ext.at[:, pl.ds(0, 2), pl.ds(start, rows), :],
            self.ext.at[:, pl.ds(3, 2), pl.ds(start, rows), :],
            self.left_sems.at[0, index], self.left_sems.at[1, index],
            (self.row, jnp.maximum(self.col - 1, 0)),
        )

    def over(self, index, blocks, sems):
        start, rows = CHUNKS[index]
        return remote(
            self.ext.at[:, blocks, pl.ds(start, rows), :],
            self.ext.at[:, blocks, pl.ds(384 + start, rows), :],
            sems.at[0, index], sems.at[1, index],
            (jnp.maximum(self.row - 1, 0), self.col),
        )

    def up(self, index):
        return self.over(index, pl.ds(0, 3), self.up_sems)

    def corner(self, index):
        return self.over(index, pl.ds(3, 2), self.corner_sems)

    def detour_hop(self, hop, index):
        start, rows = CHUNKS[index]
        first, last = hop == 0, hop == 2
        source = self.ext if first else self.detour
        target = self.ext.at[:, pl.ds(0, 3), pl.ds(384 + start, rows), :] if last else (
            self.detour.at[:, :, pl.ds(start, rows), :])
        return remote(
            source.at[:, pl.ds(0, 3), pl.ds(start, rows), :], target,
            self.detour_sems.at[0, index],
            self.up_sems.at[1, index] if last else self.detour_sems.at[1, index],
            self.way.next_place(hop),
        )

    def pass_on(self, index):
        for hop in (1, 2):
            @pl.when(self.stops[hop])
            def _(hop=hop):
                self.detour_hop(hop - 1, index).wait_recv()
                self.detour_hop(hop, index).start()

    def clear_edges(self):
        @pl.when(self.col == N_COL - 1)
        def _():
            for channel in range(2):
                for block in (3, 4):
                    self.ext[channel, block] = jnp.zeros((EXT, 128), F32)

        @pl.when(self.row == N_ROW - 1)
        def _():
            for channel in range(2):
                for block in range(5):
                    self.ext[channel, block, 384:640] = jnp.zeros((256, 128), F32)

    def send_left(self, index):
        @pl.when(self.sends_left)
        def _():
            self.left(index).start()

    def send_up(self, index):
        @pl.when(self.sends_direct)
        def _():
            self.up(index).start()

        @pl.when(self.stops[0])
        def _():
            self.detour_hop(0, index).start()

    def forward_corner(self, index):
        @pl.when(self.takes_right)
        def _():
            self.left(index).wait_recv()

            @pl.when(self.sends_up)
            def _():
                self.corner(index).start()

    def finish(self):
        @pl.when(self.takes_right)
        def _():
            for index in LOWS:
                self.left(index).wait_recv()

        @pl.when(self.takes_below)
        def _():
            for index in range(TOPS):
                self.up(index).wait_recv()

        @pl.when(self.takes_below & self.takes_right)
        def _():
            for index in range(TOPS):
                self.corner(index).wait_recv()

        @pl.when(self.sends_left)
        def _():
            for index in range(EVERY):
                self.left(index).wait_send()

        @pl.when(self.sends_direct)
        def _():
            for index in range(TOPS):
                self.up(index).wait_send()

        for hop in range(3):
            @pl.when(self.stops[hop])
            def _(hop=hop):
                for index in range(TOPS):
                    self.detour_hop(hop, index).wait_send()

        @pl.when(self.sends_up & self.takes_right)
        def _():
            for index in range(TOPS):
                self.corner(index).wait_send()


def halo_sems():
    dma = pltpu.SemaphoreType.DMA
    return [pltpu.VMEM((2, 3, 256, 128), F32), dma((2, EVERY)), dma((2, TOPS)), dma((2, TOPS)),
            dma((2, TOPS))]


def fetch_kernel(object_ref, measured_ref, order_ref, ext_ref, sorted_ref,
                 turned, measured, load_sems, *sems):
    row, col = place()
    barrier = pltpu.get_barrier_semaphore()
    greet_neighbours(barrier, row, col)
    way = Detour(UP_DETOURS, row, col)
    way.greet(barrier)
    loads = []
    for channel in range(2):
        for block in range(3):
            load = pltpu.make_async_copy(
                object_ref.at[channel, :, pl.ds(block * 128, 128)],
                ext_ref.at[channel, block, pl.ds(0, TILE), :],
                load_sems.at[channel * 3 + block],
            )
            load.start()
            loads.append(load)
    load_frames = pltpu.make_async_copy(measured_ref, measured, load_sems.at[6])
    load_frames.start()
    halo = Halo(ext_ref, way, *sems, row, col)
    halo.clear_edges()
    for load in loads:
        load.wait()
    pl.semaphore_wait(barrier, neighbour_count(row, col) + way.count())
    for index in range(EVERY):
        halo.send_left(index)
    for index in range(TOPS):
        halo.send_up(index)

    def sort_frame(frame, carry):
        value = measured[frame]
        total = jnp.zeros((256, 256), F32)
        for _ in range(3):
            piece = value.astype(BF16)
            value = value - piece.astype(F32)
            total = total + jnp.dot(piece, order_ref[...], preferred_element_type=F32)
        for block in range(2):
            turned[block] = total[:, block * 128:block * 128 + 128]
        for block in range(2):
            for parity in range(2):
                sorted_ref[frame, parity, :, block * 128:block * 128 + 128] = (
                    turned[block, pl.ds(parity, 128, stride=2), :])
        return carry

    load_frames.wait()
    share = measured.shape[0] // TOPS
    for index in range(TOPS):
        lax.fori_loop(index * share, (index + 1) * share, sort_frame, 0)
        halo.pass_on(index)
        halo.forward_corner(index)
    halo.finish()


def fetch(object_field, measured, order):
    dma = pltpu.SemaphoreType.DMA
    count = measured.shape[0]
    return pl.pallas_call(
        fetch_kernel,
        name="fetch",
        out_shape=(
            jax.ShapeDtypeStruct((2, 5, EXT, 128), F32),
            jax.ShapeDtypeStruct((count, 2, 128, 256), F32),
        ),
        in_specs=[HBM_SPEC, HBM_SPEC, VMEM_SPEC],
        out_specs=(VMEM_SPEC, VMEM_SPEC),
        scratch_shapes=[
            pltpu.VMEM((2, 256, 128), F32), pltpu.VMEM((count, 256, 256), F32), dma((7,)),
        ] + halo_sems(),
        compiler_params=pltpu.CompilerParams(
            collective_id=0, has_side_effects=True, vmem_limit_bytes=FETCH_VMEM),
    )(*(pltpu.with_memory_space_constraint(a, pltpu.HBM) for a in (object_field, measured)), order)


def halves(value):
    high = value.astype(BF16)
    low = (value - high.astype(F32)).astype(BF16)
    return high, low


def dot(left, right):
    return jnp.dot(left, right, preferred_element_type=F32)


def times_table(value, tables, index):
    high, low = halves(value)
    return dot(high, tables[index]) + dot(low, tables[index]) + dot(high, tables[index + 1])


def table_times(tables, index, value):
    high, low = halves(value)
    return dot(tables[index], high) + dot(tables[index + 1], high) + dot(tables[index], low)


def beside(a, b):
    return jnp.concatenate([a, b], axis=1)


def above(a, b):
    return jnp.concatenate([a, b], axis=0)


def frames_kernel(batch, counts_ref, first_ref, positions_ref, ext_ref, probe_ref, sorted_ref,
                  tables, grad_ref, probe_grad_ref):
    live = counts_ref[0, 0]
    first = jnp.minimum(first_ref[0, 0], live)
    start, end = (0, first) if batch == 0 else (first, live)
    for channel in range(2):
        for block in range(5):
            grad_ref[channel, block] = jnp.zeros((EXT, 128), F32)
    probe_grad_ref[...] = jnp.zeros_like(probe_grad_ref)
    lanes = lax.broadcasted_iota(jnp.int32, (256, 128), 1)

    def load_window(frame):
        row_start, col_start = positions_ref[0, frame], positions_ref[1, frame]
        block0 = col_start // 128
        shift = col_start - block0 * 128
        rows = pl.ds(row_start, 256)
        back_shift = jnp.bitwise_and(128 - shift, 127)
        keep = lanes < 128 - shift
        window = []
        for channel in range(2):
            turned = [
                pltpu.roll(ext_ref[channel, block0 + block, rows, :], back_shift, 1)
                for block in range(3)
            ]
            window.append([jnp.where(keep, turned[b], turned[b + 1]) for b in range(2)])
        return window, block0, shift, rows

    def load_probe():
        return [[probe_ref[channel, :, b * 128:b * 128 + 128] for b in range(2)]
                for channel in range(2)]

    def stacked(t0, t1):
        return above(beside(t0[:, :128], t1[:, :128]), beside(t0[:, 128:], t1[:, 128:]))

    def across(window):
        probe = load_probe()
        re = [probe[0][b] * window[0][b] - probe[1][b] * window[1][b] for b in range(2)]
        im = [probe[0][b] * window[1][b] + probe[1][b] * window[0][b] for b in range(2)]
        return (times_table(beside(re[0] + re[1], im[0] + im[1]), tables, 0),
                times_table(beside(re[0] - re[1], im[0] - im[1]), tables, 2))

    def along(y):
        y0, y1 = y
        return (table_times(tables, 4, stacked(y0[:128] + y0[128:], y1[:128] + y1[128:])),
                table_times(tables, 6, stacked(y0[:128] - y0[128:], y1[:128] - y1[128:])))

    def along_back(w, frame, valid):
        parts = []
        for parity in range(2):
            re, im = w[parity][:128], w[parity][128:]
            residue = re * re + im * im - sorted_ref[frame, parity]
            residue = jnp.where(valid, residue, jnp.zeros_like(residue))
            parts.append(table_times(tables, 2 * parity, above(residue * re, residue * im)))
        return parts

    def across_back(u):
        top, bottom = u[0] + u[1], u[0] - u[1]
        z_re = above(top[:128], bottom[:128])
        z_im = above(top[128:], bottom[128:])
        v0 = times_table(beside(z_re[:, :128], z_im[:, :128]), tables, 4)
        v1 = times_table(beside(z_re[:, 128:], z_im[:, 128:]), tables, 6)
        return ([v0[:, :128] + v1[:, :128], v0[:, :128] - v1[:, :128]],
                [v0[:, 128:] + v1[:, 128:], v0[:, 128:] - v1[:, 128:]])

    def add_probe_terms(windows, backs):
        for b in range(2):
            at = slice(b * 128, b * 128 + 128)
            re, im = probe_grad_ref[0, :, at], probe_grad_ref[1, :, at]
            for window, (back_re, back_im) in zip(windows, backs):
                re = re + (window[0][b] * back_re[b] + window[1][b] * back_im[b])
                im = im + (window[0][b] * back_im[b] - window[1][b] * back_re[b])
            probe_grad_ref[0, :, at] = re
            probe_grad_ref[1, :, at] = im

    def add_object_terms(place, back):
        block0, shift, rows = place
        back_re, back_im = back
        probe = load_probe()
        before = lanes < shift
        zero = jnp.zeros((256, 128), F32)
        for channel in range(2):
            if channel == 0:
                term = [probe[0][b] * back_re[b] + probe[1][b] * back_im[b] for b in range(2)]
            else:
                term = [probe[0][b] * back_im[b] - probe[1][b] * back_re[b] for b in range(2)]
            turned = [pltpu.roll(term[b], shift, 1) for b in range(2)]
            adds = [
                jnp.where(before, zero, turned[0]),
                jnp.where(before, turned[0], turned[1]),
                jnp.where(before, turned[1], zero),
            ]
            for block in range(3):
                at = (channel, block0 + block, rows, slice(None))
                grad_ref[at] = grad_ref[at] + adds[block]

    last = positions_ref.shape[1] - 1

    def add_pair(pair, carry):
        slots = [start + pair * 2 + k for k in range(2)]
        valid = [slot < end for slot in slots]
        slots = [jnp.minimum(slot, last) for slot in slots]
        windows, places = [], []
        for slot in slots:
            window, *spot = load_window(slot)
            windows.append(window)
            places.append(spot)
        y = [across(window) for window in windows]
        w = [along(each) for each in y]
        u = [along_back(w[k], slots[k], valid[k]) for k in range(2)]
        backs = [across_back(each) for each in u]
        add_probe_terms(windows, backs)
        for k in range(2):
            add_object_terms(places[k], backs[k])
        return carry

    lax.fori_loop(0, (end - start + 1) // 2, add_pair, 0)


def frames(batch, counts, first, positions, ext, probe, ordered, tables):
    return pl.pallas_call(
        functools.partial(frames_kernel, batch),
        name=f"frames{batch}",
        out_shape=(
            jax.ShapeDtypeStruct((2, 5, EXT, 128), F32),
            jax.ShapeDtypeStruct((2, PROBE, PROBE), F32),
        ),
        in_specs=[SMEM_SPEC, SMEM_SPEC, SMEM_SPEC] + [VMEM_SPEC] * 4,
        out_specs=(VMEM_SPEC, VMEM_SPEC),
        compiler_params=pltpu.CompilerParams(vmem_limit_bytes=FRAMES_VMEM),
    )(counts, first, positions, ext, probe, ordered, tables)


AROUND = tuple((i, j) for i in range(4) for j in range(4) if i or j)


class Reduce:
    def __init__(self, grad, half, got_half, got_plane, got_z, sums, sems, row, col):
        self.grad, self.half, self.got_half = grad, half, got_half
        self.got_plane, self.got_z, self.sums, self.sems = got_plane, got_z, sums, sems
        self.row, self.col, self.core = row, col, row % 2
        self.y = (row % 8) // 2
        self.x = (row // 8) * 2 + col // 8
        self.z = col % 8

    def partner(self):
        return (self.row + 1 - 2 * self.core, self.col)

    def plane(self, i, j):
        x, y = (self.x + i) % 4, (self.y + j) % 4
        device = ((x // 2) * 8 + y * 2 + self.core, (x % 2) * 8 + self.z)
        return pl.ds(pl.multiple_of((x * 4 + y) * 16, 16), 16), device

    def over_z_to(self, step):
        z = (self.z + step) % 8
        return z, (self.row, (self.col // 8) * 8 + z)

    def peers(self):
        found = [self.partner()]
        found += [self.plane(i, j)[1] for i, j in AROUND]
        found += [self.over_z_to(step)[1] for step in range(1, 8)]
        return found

    def copy(self, src, dst, index, device):
        return remote(src, dst, self.sems.at[0, index], self.sems.at[1, index], device)

    def pair(self):
        return self.copy(self.grad.at[1 - self.core], self.got_half, 0, self.partner())

    def out(self, n):
        rows, device = self.plane(*AROUND[n])
        return self.copy(self.half.at[rows, :], self.got_plane.at[n], 1 + n, device)

    def along(self, step):
        return self.copy(
            self.got_z.at[self.z], self.got_z.at[self.z], 15 + step, self.over_z_to(step)[1])

    def back(self, n):
        rows = self.plane(0, 0)[0]
        mine = self.sums.at[self.core, rows, :]
        return self.copy(mine, mine, 23 + n, self.plane(*AROUND[n])[1])

    def back_pair(self):
        mine = self.sums.at[self.core]
        return self.copy(mine, mine, 38, self.partner())

    def begin(self):
        self.pair().start()

    def to_plane(self):
        self.pair().wait_recv()
        self.half[...] = self.grad[self.core] + self.got_half[...]
        for n in range(15):
            self.out(n).start()

    def to_z(self):
        for n in range(15):
            self.out(n).wait_recv()
        total = self.half[self.plane(0, 0)[0], :]
        for n in range(15):
            total = total + self.got_plane[n]
        self.got_z[self.z] = total
        for step in range(1, 8):
            self.along(step).start()

    def from_z(self):
        for step in range(1, 8):
            theirs = self.got_z.at[(self.z + 8 - step) % 8]
            self.copy(theirs, theirs, 15 + step, self.over_z_to(step)[1]).wait_recv()
        total = self.got_z[0]
        for z in range(1, 8):
            total = total + self.got_z[z]
        self.sums[self.core, self.plane(0, 0)[0], :] = total
        for n in range(15):
            self.back(n).start()

    def from_plane(self):
        for n in range(15):
            i, j = AROUND[n]
            theirs = self.sums.at[self.core, self.plane(4 - i, 4 - j)[0], :]
            self.copy(theirs, theirs, 23 + n, self.plane(i, j)[1]).wait_recv()
        self.back_pair().start()

    def end(self):
        theirs = self.sums.at[1 - self.core]
        self.copy(theirs, theirs, 38, self.partner()).wait_recv()

    def drain(self):
        self.pair().wait_send()
        for n in range(15):
            self.out(n).wait_send()
            self.back(n).wait_send()
        for step in range(1, 8):
            self.along(step).wait_send()
        self.back_pair().wait_send()


def exchange_kernel(refetch, object_ref, grad_ref, probe_ref, probe_grad_ref, out_ref, probe_out,
                    from_above, from_left, joined, half, got_half, got_plane, got_z, sums,
                    detour, down_sems, right_sems, reduce_sems, detour_sems, *sems):
    row, col = place()
    reduce = Reduce(
        probe_grad_ref, half, got_half, got_plane, got_z, sums, reduce_sems, row, col)
    barrier = pltpu.get_barrier_semaphore()
    greet_neighbours(barrier, row, col)
    down_way = Detour(DOWN_DETOURS if refetch else DOWN_DETOURS[:1], row, col)
    down_way.greet(barrier)
    if refetch:
        up_way = Detour(UP_DETOURS, row, col)
        up_way.greet(barrier)
    for device in reduce.peers():
        pl.semaphore_signal(barrier, inc=1, device_id=device, device_id_type=MESH)
    stops = (down_way.each[0], down_way.each[-1])
    sends_down, takes_above = row < N_ROW - 1, row > 0
    sends_right, takes_left = col < N_COL - 1, col > 0
    if refetch:
        halo = Halo(out_ref, up_way, *sems, row, col)
        halo.clear_edges()

    @pl.when((row == 0) | (col == N_COL - 1))
    def _():
        for channel in range(2):
            for block in (3, 4):
                from_above[channel, block] = jnp.zeros((256, 128), F32)

    @pl.when(row == 0)
    def _():
        for channel in range(2):
            for block in range(3):
                from_above[channel, block] = jnp.zeros((256, 128), F32)

    @pl.when(col == 0)
    def _():
        for channel in range(2):
            for block in range(2):
                from_left[channel, block] = jnp.zeros((TILE, 128), F32)

    greeted = 23 + neighbour_count(row, col) + down_way.count()
    if refetch:
        greeted = greeted + up_way.count()
    pl.semaphore_wait(barrier, greeted)

    def down(index, part):
        blocks = pl.ds(3, 2) if part == 0 else pl.ds(0, 3)
        start, rows = CHUNKS[index]
        return remote(
            grad_ref.at[:, blocks, pl.ds(384 + start, rows), :],
            from_above.at[:, blocks, pl.ds(start, rows), :],
            down_sems.at[0, part, index], down_sems.at[1, part, index],
            (jnp.minimum(row + 1, N_ROW - 1), col),
        )

    def detour_hop(hop, index, part):
        start, rows = CHUNKS[index]
        blocks = pl.ds(3, 2) if part == 0 else pl.ds(0, 3)
        here = pl.ds(start, rows)
        source = detour.at[:, blocks, here, :] if hop else (
            grad_ref.at[:, blocks, pl.ds(384 + start, rows), :])
        target = (from_above if hop == 2 else detour).at[:, blocks, here, :]
        return remote(
            source, target, detour_sems.at[0, part, index],
            (down_sems if hop == 2 else detour_sems).at[1, part, index],
            down_way.next_place(hop),
        )

    def pass_on(index, part):
        for hop in (1, 2):
            @pl.when(stops[part][hop])
            def _(hop=hop):
                detour_hop(hop - 1, index, part).wait_recv()
                detour_hop(hop, index, part).start()

    needs = (sends_down & sends_right, sends_down)
    takes = (takes_above & sends_right, takes_above)
    straight = [needs[part] & jnp.logical_not(stops[part][0]) for part in range(2)]

    def send_down(index, part):
        @pl.when(straight[part])
        def _():
            down(index, part).start()

        @pl.when(stops[part][0])
        def _():
            detour_hop(0, index, part).start()

    def right(index):
        start, rows = CHUNKS[index]
        if index in LOWS:
            source = grad_ref.at[:, pl.ds(3, 2), pl.ds(start, rows), :]
        else:
            source = joined.at[:, :, pl.ds(start, rows), :]
        return remote(
            source, from_left.at[:, :, pl.ds(start, rows), :],
            right_sems.at[0, index], right_sems.at[1, index],
            (row, jnp.minimum(col + 1, N_COL - 1)),
        )

    def send_right(index):
        @pl.when(sends_right)
        def _():
            right(index).start()

    def join(index):
        start, rows = CHUNKS[index]
        at = slice(start, start + rows)

        @pl.when(takes[0])
        def _():
            down(index, 0).wait_recv()

        for channel in range(2):
            for block in range(2):
                joined[channel, block, at] = (
                    grad_ref[channel, 3 + block, at] + from_above[channel, 3 + block, at])
        send_right(index)

    def update(index):
        start, rows = CHUNKS[index]
        at = slice(start, start + rows)
        if index < TOPS:
            @pl.when(takes_above)
            def _():
                down(index, 1).wait_recv()

        @pl.when(takes_left)
        def _():
            right(index).wait_recv()

        for channel in range(2):
            for block in range(3):
                grad = grad_ref[channel, block, at]
                if index < TOPS:
                    grad = grad + from_above[channel, block, at]
                if block < 2:
                    grad = grad + from_left[channel, block, at]
                value = object_ref[channel, block, at] - 0.1 * grad
                if refetch:
                    out_ref[channel, block, at] = value
                else:
                    out_ref[channel, at, block * 128:block * 128 + 128] = value
        if refetch:
            halo.send_left(index)
            if index < TOPS:
                halo.send_up(index)

    def forward(index):
        if refetch:
            halo.forward_corner(index)

    def pass_up(index):
        if refetch:
            halo.pass_on(index)

    reduce.begin()
    send_right(4)
    send_right(5)
    send_down(0, 0)
    send_down(1, 0)
    reduce.to_plane()
    send_down(2, 0)
    send_down(3, 0)
    for index in range(TOPS):
        send_down(index, 1)
    pass_on(0, 0)
    pass_on(1, 0)
    update(4)
    reduce.to_z()
    late = down_way.stops[3]
    on_time = jnp.logical_not(late)
    pl.when(late)(reduce.from_z)
    join(0)
    join(1)
    pass_on(2, 0)
    pass_on(3, 0)
    join(2)
    join(3)
    pass_on(0, 1)
    pass_on(1, 1)
    if refetch:
        pl.when(late)(reduce.from_plane)
        update(0)
        pl.when(on_time)(reduce.from_z)
        update(1)
        pass_on(2, 1)
        pass_on(3, 1)
        forward(0)
        update(2)
        forward(1)
        update(3)
        update(5)
        pl.when(on_time)(reduce.from_plane)
        pass_up(0)
        pass_up(1)
        forward(2)
        forward(3)
        pass_up(2)
        pass_up(3)
    else:
        update(5)
        pl.when(on_time)(reduce.from_z)
        pl.when(late)(reduce.from_plane)
        pass_on(2, 1)
        pass_on(3, 1)
        update(0)
        update(1)
        pl.when(on_time)(reduce.from_plane)
        update(2)
        update(3)
    reduce.end()
    step_size = 0.5 / math.sqrt(N_ROW * N_COL * 8)
    probe_out[...] = probe_ref[...] - step_size * sums[...]
    if refetch:
        halo.finish()
    reduce.drain()
    for part in range(2):
        @pl.when(straight[part])
        def _(part=part):
            for index in range(TOPS):
                down(index, part).wait_send()

        for hop in range(3):
            @pl.when(stops[part][hop])
            def _(hop=hop, part=part):
                for index in range(TOPS):
                    detour_hop(hop, index, part).wait_send()

    @pl.when(sends_right)
    def _():
        for index in range(EVERY):
            right(index).wait_send()


def exchange(refetch, ext, grad, probe, probe_grad):
    dma = pltpu.SemaphoreType.DMA
    out = (2, 5, EXT, 128) if refetch else (2, TILE, TILE)
    return pl.pallas_call(
        functools.partial(exchange_kernel, refetch),
        name=f"exchange{int(refetch)}",
        out_shape=(
            jax.ShapeDtypeStruct(out, F32), jax.ShapeDtypeStruct((2, PROBE, PROBE), F32)),
        in_specs=[VMEM_SPEC] * 4,
        out_specs=(VMEM_SPEC, VMEM_SPEC),
        scratch_shapes=[
            pltpu.VMEM((2, 5, 256, 128), F32),
            pltpu.VMEM((2, 2, TILE, 128), F32),
            pltpu.VMEM((2, 2, 256, 128), F32),
            pltpu.VMEM((256, 256), F32),
            pltpu.VMEM((256, 256), F32),
            pltpu.VMEM((15, 16, 256), F32),
            pltpu.VMEM((8, 16, 256), F32),
            pltpu.VMEM((2, 256, 256), F32),
            pltpu.VMEM((2, 5, 256, 128), F32),
            dma((2, 2, TOPS)),
            dma((2, EVERY)),
            dma((2, 39)),
            dma((2, 2, TOPS)),
        ] + (halo_sems() if refetch else []),
        compiler_params=pltpu.CompilerParams(
            collective_id=1 + int(refetch), has_side_effects=True,
            vmem_limit_bytes=EXCHANGE_VMEM),
    )(ext, grad, probe, probe_grad)


def per_device(object_field, illumination, measured, positions, frame_counts, first_count):
    tables = jnp.asarray(dft_tables())
    order = jnp.asarray(deinterleave_table())
    positions = positions[0, 0].T
    probe = illumination
    ext, ordered = fetch(object_field, measured[0, 0], order)
    grad, probe_grad = frames(
        0, frame_counts, first_count, positions, ext, probe, ordered, tables)
    ext, probe = exchange(True, ext, grad, probe, probe_grad)
    grad, probe_grad = frames(
        1, frame_counts, first_count, positions, ext, probe, ordered, tables)
    new_object, probe = exchange(False, ext, grad, probe, probe_grad)
    return new_object, probe


def solution(mesh):
    in_specs = (
        P(None, "row", "col"),
        P(),
        P("row", "col", None, None, None),
        P("row", "col", None, None),
        P("row", "col"),
        P("row", "col"),
    )
    out_specs = (P(None, "row", "col"), P())
    return jax.shard_map(
        per_device, mesh=mesh, in_specs=in_specs, out_specs=out_specs, check_vma=False
    )
```

```python
import functools
import math

import jax
import jax.numpy as jnp
import numpy as np
from jax import lax
from jax.experimental import pallas as pl
from jax.experimental.pallas import tpu as pltpu
from jax.sharding import PartitionSpec as P

MESH = pl.DeviceIdType.MESH
TILE, PROBE, EXT = 384, 256, 640
N_ROW = N_COL = 16
F32, BF16 = jnp.float32, jnp.bfloat16
FETCH_VMEM, FRAMES_VMEM, EXCHANGE_VMEM = 14 << 20, 16 << 20, 18 << 20
VMEM_SPEC = pl.BlockSpec(memory_space=pltpu.VMEM)
SMEM_SPEC = pl.BlockSpec(memory_space=pltpu.SMEM)
HBM_SPEC = pl.BlockSpec(memory_space=pltpu.HBM)


def split_bf16(table):
    high = table.astype(np.float32).astype(BF16)
    low = (table - high.astype(np.float64)).astype(np.float32).astype(BF16)
    return high, low


def dft_tables():
    n = np.arange(128)[:, None]
    parts = []
    for parity in (0, 1):
        k = 2 * np.arange(128)[None, :] + parity
        angle = ((n * k) % 256) * (2.0 * np.pi / 256.0)
        c, s = np.cos(angle) / 16.0, np.sin(angle) / 16.0
        table = np.block([[c, -s], [s, c]])
        parts.append((split_bf16(table), split_bf16(table.T)))
    order = []
    for transposed in (0, 1):
        for parity in (0, 1):
            order.extend(parts[parity][transposed])
    return np.stack(order)


def deinterleave_table():
    row = lax.broadcasted_iota(jnp.int32, (256, 256), 0)
    col = lax.broadcasted_iota(jnp.int32, (256, 256), 1)
    source = jnp.where(col < 128, 2 * col, 2 * col - 255)
    return jnp.where(row == source, 1.0, 0.0).astype(BF16)


def place():
    row, col = lax.axis_index("row"), lax.axis_index("col")
    return row, col


def remote(src, dst, send_sem, recv_sem, device):
    return pltpu.make_async_remote_copy(
        src_ref=src, dst_ref=dst, send_sem=send_sem, recv_sem=recv_sem,
        device_id=device, device_id_type=MESH,
    )


UP_DETOURS = (((8, 15), (14, 15), (6, 7), (7, 15)),)
DOWN_DETOURS = (((7, 0), (1, 0), (9, 8), (8, 0)), ((7, 15), (1, 15), (9, 7), (8, 15)))


def is_at(row, col, device):
    return (row == device[0]) & (col == device[1])


def place_of(device):
    return jnp.int32(device[0]), jnp.int32(device[1])


class Detour:
    def __init__(self, paths, row, col):
        self.paths, self.row, self.col = paths, row, col
        self.each = [[is_at(row, col, path[stop]) for stop in range(4)] for path in paths]
        self.stops = [functools.reduce(jnp.logical_or, marks) for marks in zip(*self.each)]

    def next_place(self, hop):
        row, col = place_of(self.paths[0][hop + 1])
        for path in self.paths[1:]:
            other_row, other_col = place_of(path[hop + 1])
            here = is_at(self.row, self.col, path[hop])
            row, col = jnp.where(here, other_row, row), jnp.where(here, other_col, col)
        return row, col

    def greet(self, barrier):
        for path in self.paths:
            for hop in range(3):
                for here, there in ((path[hop], path[hop + 1]), (path[hop + 1], path[hop])):
                    @pl.when(is_at(self.row, self.col, here))
                    def _(there=there):
                        pl.semaphore_signal(
                            barrier, inc=1, device_id=place_of(there), device_id_type=MESH)

    def count(self):
        one, two, none = jnp.int32(1), jnp.int32(2), jnp.int32(0)
        return jnp.where(self.stops[0] | self.stops[3], one, none) + jnp.where(
            self.stops[1] | self.stops[2], two, none)


def greet_neighbours(barrier, row, col):
    for has, device in (
        (row > 0, (row - 1, col)),
        (row < N_ROW - 1, (row + 1, col)),
        (col > 0, (row, col - 1)),
        (col < N_COL - 1, (row, col + 1)),
    ):
        @pl.when(has)
        def _(device=device):
            pl.semaphore_signal(barrier, inc=1, device_id=device, device_id_type=MESH)


def neighbour_count(row, col):
    one, none = jnp.int32(1), jnp.int32(0)
    has = (row > 0, row < N_ROW - 1, col > 0, col < N_COL - 1)
    return sum(jnp.where(h, one, none) for h in has)


CHUNKS = ((0, 64), (64, 64), (128, 64), (192, 64), (256, 64), (320, 64))
TOPS = 4
LOWS = (4, 5)
EVERY = 6


class Halo:
    def __init__(self, ext, way, detour, left_sems, up_sems, corner_sems, detour_sems, row, col):
        self.ext, self.row, self.col = ext, row, col
        self.left_sems, self.up_sems, self.corner_sems = left_sems, up_sems, corner_sems
        self.detour, self.detour_sems = detour, detour_sems
        self.way, self.stops = way, way.stops
        self.sends_left, self.takes_right = col > 0, col < N_COL - 1
        self.sends_up, self.takes_below = row > 0, row < N_ROW - 1
        self.sends_direct = self.sends_up & jnp.logical_not(self.stops[0])

    def left(self, index):
        start, rows = CHUNKS[index]
        return remote(
            self.ext.at[:, pl.ds(0, 2), pl.ds(start, rows), :],
            self.ext.at[:, pl.ds(3, 2), pl.ds(start, rows), :],
            self.left_sems.at[0, index], self.left_sems.at[1, index],
            (self.row, jnp.maximum(self.col - 1, 0)),
        )

    def over(self, index, blocks, sems):
        start, rows = CHUNKS[index]
        return remote(
            self.ext.at[:, blocks, pl.ds(start, rows), :],
            self.ext.at[:, blocks, pl.ds(384 + start, rows), :],
            sems.at[0, index], sems.at[1, index],
            (jnp.maximum(self.row - 1, 0), self.col),
        )

    def up(self, index):
        return self.over(index, pl.ds(0, 3), self.up_sems)

    def corner(self, index):
        return self.over(index, pl.ds(3, 2), self.corner_sems)

    def detour_hop(self, hop, index):
        start, rows = CHUNKS[index]
        first, last = hop == 0, hop == 2
        source = self.ext if first else self.detour
        target = self.ext.at[:, pl.ds(0, 3), pl.ds(384 + start, rows), :] if last else (
            self.detour.at[:, :, pl.ds(start, rows), :])
        return remote(
            source.at[:, pl.ds(0, 3), pl.ds(start, rows), :], target,
            self.detour_sems.at[0, index],
            self.up_sems.at[1, index] if last else self.detour_sems.at[1, index],
            self.way.next_place(hop),
        )

    def pass_on(self, index):
        for hop in (1, 2):
            @pl.when(self.stops[hop])
            def _(hop=hop):
                self.detour_hop(hop - 1, index).wait_recv()
                self.detour_hop(hop, index).start()

    def clear_edges(self):
        @pl.when(self.col == N_COL - 1)
        def _():
            for channel in range(2):
                for block in (3, 4):
                    self.ext[channel, block] = jnp.zeros((EXT, 128), F32)

        @pl.when(self.row == N_ROW - 1)
        def _():
            for channel in range(2):
                for block in range(5):
                    self.ext[channel, block, 384:640] = jnp.zeros((256, 128), F32)

    def send_left(self, index):
        @pl.when(self.sends_left)
        def _():
            self.left(index).start()

    def send_up(self, index):
        @pl.when(self.sends_direct)
        def _():
            self.up(index).start()

        @pl.when(self.stops[0])
        def _():
            self.detour_hop(0, index).start()

    def forward_corner(self, index):
        @pl.when(self.takes_right)
        def _():
            self.left(index).wait_recv()

            @pl.when(self.sends_up)
            def _():
                self.corner(index).start()

    def finish(self):
        @pl.when(self.takes_right)
        def _():
            for index in LOWS:
                self.left(index).wait_recv()

        @pl.when(self.takes_below)
        def _():
            for index in range(TOPS):
                self.up(index).wait_recv()

        @pl.when(self.takes_below & self.takes_right)
        def _():
            for index in range(TOPS):
                self.corner(index).wait_recv()

        @pl.when(self.sends_left)
        def _():
            for index in range(EVERY):
                self.left(index).wait_send()

        @pl.when(self.sends_direct)
        def _():
            for index in range(TOPS):
                self.up(index).wait_send()

        for hop in range(3):
            @pl.when(self.stops[hop])
            def _(hop=hop):
                for index in range(TOPS):
                    self.detour_hop(hop, index).wait_send()

        @pl.when(self.sends_up & self.takes_right)
        def _():
            for index in range(TOPS):
                self.corner(index).wait_send()


def halo_sems():
    dma = pltpu.SemaphoreType.DMA
    return [pltpu.VMEM((2, 3, 256, 128), F32), dma((2, EVERY)), dma((2, TOPS)), dma((2, TOPS)),
            dma((2, TOPS))]


def fetch_kernel(object_ref, measured_ref, ext_ref, sorted_ref,
                 order, turned, measured, load_sems, *sems):
    row, col = place()
    barrier = pltpu.get_barrier_semaphore()
    greet_neighbours(barrier, row, col)
    way = Detour(UP_DETOURS, row, col)
    way.greet(barrier)
    loads = []
    for channel in range(2):
        for block in range(3):
            load = pltpu.make_async_copy(
                object_ref.at[channel, :, pl.ds(block * 128, 128)],
                ext_ref.at[channel, block, pl.ds(0, TILE), :],
                load_sems.at[channel * 3 + block],
            )
            load.start()
            loads.append(load)
    load_frames = pltpu.make_async_copy(measured_ref, measured, load_sems.at[6])
    load_frames.start()
    halo = Halo(ext_ref, way, *sems, row, col)
    halo.clear_edges()
    for load in loads:
        load.wait()
    pl.semaphore_wait(barrier, neighbour_count(row, col) + way.count())
    for index in range(EVERY):
        halo.send_left(index)
    for index in range(TOPS):
        halo.send_up(index)

    def sort_frame(frame, carry):
        value = measured[frame]
        total = jnp.zeros((256, 256), F32)
        for _ in range(3):
            piece = value.astype(BF16)
            value = value - piece.astype(F32)
            total = total + jnp.dot(piece, order[...], preferred_element_type=F32)
        for block in range(2):
            turned[block] = total[:, block * 128:block * 128 + 128]
        for block in range(2):
            for parity in range(2):
                sorted_ref[frame, parity, :, block * 128:block * 128 + 128] = (
                    turned[block, pl.ds(parity, 128, stride=2), :])
        return carry

    order[...] = deinterleave_table()
    load_frames.wait()
    share = measured.shape[0] // TOPS
    for index in range(TOPS):
        lax.fori_loop(index * share, (index + 1) * share, sort_frame, 0)
        halo.pass_on(index)
        halo.forward_corner(index)
    halo.finish()


def fetch(object_field, measured):
    dma = pltpu.SemaphoreType.DMA
    count = measured.shape[0]
    return pl.pallas_call(
        fetch_kernel,
        name="fetch",
        out_shape=(
            jax.ShapeDtypeStruct((2, 5, EXT, 128), F32),
            jax.ShapeDtypeStruct((count, 2, 128, 256), F32),
        ),
        in_specs=[HBM_SPEC, HBM_SPEC],
        out_specs=(VMEM_SPEC, VMEM_SPEC),
        scratch_shapes=[
            pltpu.VMEM((256, 256), BF16), pltpu.VMEM((2, 256, 128), F32),
            pltpu.VMEM((count, 256, 256), F32), dma((7,)),
        ] + halo_sems(),
        compiler_params=pltpu.CompilerParams(
            collective_id=0, has_side_effects=True, vmem_limit_bytes=FETCH_VMEM),
    )(*(pltpu.with_memory_space_constraint(a, pltpu.HBM) for a in (object_field, measured)))


def halves(value):
    high = value.astype(BF16)
    low = (value - high.astype(F32)).astype(BF16)
    return high, low


def dot(left, right):
    return jnp.dot(left, right, preferred_element_type=F32)


def times_table(value, tables, index):
    high, low = halves(value)
    return dot(high, tables[index]) + dot(low, tables[index]) + dot(high, tables[index + 1])


def table_times(tables, index, value):
    high, low = halves(value)
    return dot(tables[index], high) + dot(tables[index + 1], high) + dot(tables[index], low)


def beside(a, b):
    return jnp.concatenate([a, b], axis=1)


def above(a, b):
    return jnp.concatenate([a, b], axis=0)


def frames_kernel(batch, counts_ref, first_ref, positions_ref, ext_ref, probe_ref, sorted_ref,
                  tables, grad_ref, probe_grad_ref):
    live = counts_ref[0, 0]
    first = jnp.minimum(first_ref[0, 0], live)
    start, end = (0, first) if batch == 0 else (first, live)
    for channel in range(2):
        for block in range(5):
            grad_ref[channel, block] = jnp.zeros((EXT, 128), F32)
    probe_grad_ref[...] = jnp.zeros_like(probe_grad_ref)
    lanes = lax.broadcasted_iota(jnp.int32, (256, 128), 1)

    def load_window(frame):
        row_start, col_start = positions_ref[0, frame], positions_ref[1, frame]
        block0 = col_start // 128
        shift = col_start - block0 * 128
        rows = pl.ds(row_start, 256)
        back_shift = jnp.bitwise_and(128 - shift, 127)
        keep = lanes < 128 - shift
        window = []
        for channel in range(2):
            turned = [
                pltpu.roll(ext_ref[channel, block0 + block, rows, :], back_shift, 1)
                for block in range(3)
            ]
            window.append([jnp.where(keep, turned[b], turned[b + 1]) for b in range(2)])
        return window, block0, shift, rows

    def load_probe():
        return [[probe_ref[channel, :, b * 128:b * 128 + 128] for b in range(2)]
                for channel in range(2)]

    def stacked(t0, t1):
        return above(beside(t0[:, :128], t1[:, :128]), beside(t0[:, 128:], t1[:, 128:]))

    def across(window):
        probe = load_probe()
        re = [probe[0][b] * window[0][b] - probe[1][b] * window[1][b] for b in range(2)]
        im = [probe[0][b] * window[1][b] + probe[1][b] * window[0][b] for b in range(2)]
        return (times_table(beside(re[0] + re[1], im[0] + im[1]), tables, 0),
                times_table(beside(re[0] - re[1], im[0] - im[1]), tables, 2))

    def along(y):
        y0, y1 = y
        return (table_times(tables, 4, stacked(y0[:128] + y0[128:], y1[:128] + y1[128:])),
                table_times(tables, 6, stacked(y0[:128] - y0[128:], y1[:128] - y1[128:])))

    def along_back(w, frame, valid):
        parts = []
        for parity in range(2):
            re, im = w[parity][:128], w[parity][128:]
            residue = re * re + im * im - sorted_ref[frame, parity]
            residue = jnp.where(valid, residue, jnp.zeros_like(residue))
            parts.append(table_times(tables, 2 * parity, above(residue * re, residue * im)))
        return parts

    def across_back(u):
        top, bottom = u[0] + u[1], u[0] - u[1]
        z_re = above(top[:128], bottom[:128])
        z_im = above(top[128:], bottom[128:])
        v0 = times_table(beside(z_re[:, :128], z_im[:, :128]), tables, 4)
        v1 = times_table(beside(z_re[:, 128:], z_im[:, 128:]), tables, 6)
        return ([v0[:, :128] + v1[:, :128], v0[:, :128] - v1[:, :128]],
                [v0[:, 128:] + v1[:, 128:], v0[:, 128:] - v1[:, 128:]])

    def add_probe_terms(windows, backs):
        for b in range(2):
            at = slice(b * 128, b * 128 + 128)
            re, im = probe_grad_ref[0, :, at], probe_grad_ref[1, :, at]
            for window, (back_re, back_im) in zip(windows, backs):
                re = re + (window[0][b] * back_re[b] + window[1][b] * back_im[b])
                im = im + (window[0][b] * back_im[b] - window[1][b] * back_re[b])
            probe_grad_ref[0, :, at] = re
            probe_grad_ref[1, :, at] = im

    def add_object_terms(place, back):
        block0, shift, rows = place
        back_re, back_im = back
        probe = load_probe()
        before = lanes < shift
        zero = jnp.zeros((256, 128), F32)
        for channel in range(2):
            if channel == 0:
                term = [probe[0][b] * back_re[b] + probe[1][b] * back_im[b] for b in range(2)]
            else:
                term = [probe[0][b] * back_im[b] - probe[1][b] * back_re[b] for b in range(2)]
            turned = [pltpu.roll(term[b], shift, 1) for b in range(2)]
            adds = [
                jnp.where(before, zero, turned[0]),
                jnp.where(before, turned[0], turned[1]),
                jnp.where(before, turned[1], zero),
            ]
            for block in range(3):
                at = (channel, block0 + block, rows, slice(None))
                grad_ref[at] = grad_ref[at] + adds[block]

    last = positions_ref.shape[1] - 1

    def add_pair(pair, carry):
        slots = [start + pair * 2 + k for k in range(2)]
        valid = [slot < end for slot in slots]
        slots = [jnp.minimum(slot, last) for slot in slots]
        windows, places = [], []
        for slot in slots:
            window, *spot = load_window(slot)
            windows.append(window)
            places.append(spot)
        y = [across(window) for window in windows]
        w = [along(each) for each in y]
        u = [along_back(w[k], slots[k], valid[k]) for k in range(2)]
        backs = [across_back(each) for each in u]
        add_probe_terms(windows, backs)
        for k in range(2):
            add_object_terms(places[k], backs[k])
        return carry

    lax.fori_loop(0, (end - start + 1) // 2, add_pair, 0)


def frames(batch, counts, first, positions, ext, probe, ordered, tables):
    return pl.pallas_call(
        functools.partial(frames_kernel, batch),
        name=f"frames{batch}",
        out_shape=(
            jax.ShapeDtypeStruct((2, 5, EXT, 128), F32),
            jax.ShapeDtypeStruct((2, PROBE, PROBE), F32),
        ),
        in_specs=[SMEM_SPEC, SMEM_SPEC, SMEM_SPEC] + [VMEM_SPEC] * 4,
        out_specs=(VMEM_SPEC, VMEM_SPEC),
        compiler_params=pltpu.CompilerParams(vmem_limit_bytes=FRAMES_VMEM),
    )(counts, first, positions, ext, probe, ordered, tables)


AROUND = tuple((i, j) for i in range(4) for j in range(4) if i or j)


class Reduce:
    def __init__(self, grad, half, got_half, got_plane, got_z, sums, sems, row, col):
        self.grad, self.half, self.got_half = grad, half, got_half
        self.got_plane, self.got_z, self.sums, self.sems = got_plane, got_z, sums, sems
        self.row, self.col, self.core = row, col, row % 2
        self.y = (row % 8) // 2
        self.x = (row // 8) * 2 + col // 8
        self.z = col % 8

    def partner(self):
        return (self.row + 1 - 2 * self.core, self.col)

    def plane(self, i, j):
        x, y = (self.x + i) % 4, (self.y + j) % 4
        device = ((x // 2) * 8 + y * 2 + self.core, (x % 2) * 8 + self.z)
        return pl.ds(pl.multiple_of((x * 4 + y) * 16, 16), 16), device

    def over_z_to(self, step):
        z = (self.z + step) % 8
        return z, (self.row, (self.col // 8) * 8 + z)

    def peers(self):
        found = [self.partner()]
        found += [self.plane(i, j)[1] for i, j in AROUND]
        found += [self.over_z_to(step)[1] for step in range(1, 8)]
        return found

    def copy(self, src, dst, index, device):
        return remote(src, dst, self.sems.at[0, index], self.sems.at[1, index], device)

    def pair(self):
        return self.copy(self.grad.at[1 - self.core], self.got_half, 0, self.partner())

    def out(self, n):
        rows, device = self.plane(*AROUND[n])
        return self.copy(self.half.at[rows, :], self.got_plane.at[n], 1 + n, device)

    def along(self, step):
        return self.copy(
            self.got_z.at[self.z], self.got_z.at[self.z], 15 + step, self.over_z_to(step)[1])

    def back(self, n):
        rows = self.plane(0, 0)[0]
        mine = self.sums.at[self.core, rows, :]
        return self.copy(mine, mine, 23 + n, self.plane(*AROUND[n])[1])

    def back_pair(self):
        mine = self.sums.at[self.core]
        return self.copy(mine, mine, 38, self.partner())

    def begin(self):
        self.pair().start()

    def to_plane(self):
        self.pair().wait_recv()
        self.half[...] = self.grad[self.core] + self.got_half[...]
        for n in range(15):
            self.out(n).start()

    def to_z(self):
        for n in range(15):
            self.out(n).wait_recv()
        total = self.half[self.plane(0, 0)[0], :]
        for n in range(15):
            total = total + self.got_plane[n]
        self.got_z[self.z] = total
        for step in range(1, 8):
            self.along(step).start()

    def from_z(self):
        for step in range(1, 8):
            theirs = self.got_z.at[(self.z + 8 - step) % 8]
            self.copy(theirs, theirs, 15 + step, self.over_z_to(step)[1]).wait_recv()
        total = self.got_z[0]
        for z in range(1, 8):
            total = total + self.got_z[z]
        self.sums[self.core, self.plane(0, 0)[0], :] = total
        for n in range(15):
            self.back(n).start()

    def from_plane(self):
        for n in range(15):
            i, j = AROUND[n]
            theirs = self.sums.at[self.core, self.plane(4 - i, 4 - j)[0], :]
            self.copy(theirs, theirs, 23 + n, self.plane(i, j)[1]).wait_recv()
        self.back_pair().start()

    def end(self):
        theirs = self.sums.at[1 - self.core]
        self.copy(theirs, theirs, 38, self.partner()).wait_recv()

    def drain(self):
        self.pair().wait_send()
        for n in range(15):
            self.out(n).wait_send()
            self.back(n).wait_send()
        for step in range(1, 8):
            self.along(step).wait_send()
        self.back_pair().wait_send()


def exchange_kernel(refetch, object_ref, grad_ref, probe_ref, probe_grad_ref, out_ref, probe_out,
                    from_above, from_left, joined, half, got_half, got_plane, got_z, sums,
                    detour, down_sems, right_sems, reduce_sems, detour_sems, *sems):
    row, col = place()
    reduce = Reduce(
        probe_grad_ref, half, got_half, got_plane, got_z, sums, reduce_sems, row, col)
    barrier = pltpu.get_barrier_semaphore()
    greet_neighbours(barrier, row, col)
    down_way = Detour(DOWN_DETOURS if refetch else DOWN_DETOURS[:1], row, col)
    down_way.greet(barrier)
    if refetch:
        up_way = Detour(UP_DETOURS, row, col)
        up_way.greet(barrier)
    for device in reduce.peers():
        pl.semaphore_signal(barrier, inc=1, device_id=device, device_id_type=MESH)

    def stops(index, part):
        first, second = down_way.each[0], down_way.each[-1]
        if part == 0 or not refetch:
            return first
        return down_way.stops if index < 2 else second

    sends_down, takes_above = row < N_ROW - 1, row > 0
    sends_right, takes_left = col < N_COL - 1, col > 0
    if refetch:
        halo = Halo(out_ref, up_way, *sems, row, col)
        halo.clear_edges()

    @pl.when((row == 0) | (col == N_COL - 1))
    def _():
        for channel in range(2):
            for block in (3, 4):
                from_above[channel, block] = jnp.zeros((256, 128), F32)

    @pl.when(row == 0)
    def _():
        for channel in range(2):
            for block in range(3):
                from_above[channel, block] = jnp.zeros((256, 128), F32)

    @pl.when(col == 0)
    def _():
        for channel in range(2):
            for block in range(2):
                from_left[channel, block] = jnp.zeros((TILE, 128), F32)

    greeted = 23 + neighbour_count(row, col) + down_way.count()
    if refetch:
        greeted = greeted + up_way.count()
    pl.semaphore_wait(barrier, greeted)

    def down(index, part):
        blocks = pl.ds(3, 2) if part == 0 else pl.ds(0, 3)
        start, rows = CHUNKS[index]
        return remote(
            grad_ref.at[:, blocks, pl.ds(384 + start, rows), :],
            from_above.at[:, blocks, pl.ds(start, rows), :],
            down_sems.at[0, part, index], down_sems.at[1, part, index],
            (jnp.minimum(row + 1, N_ROW - 1), col),
        )

    def detour_hop(hop, index, part):
        start, rows = CHUNKS[index]
        blocks = pl.ds(3, 2) if part == 0 else pl.ds(0, 3)
        here = pl.ds(start, rows)
        source = detour.at[:, blocks, here, :] if hop else (
            grad_ref.at[:, blocks, pl.ds(384 + start, rows), :])
        target = (from_above if hop == 2 else detour).at[:, blocks, here, :]
        return remote(
            source, target, detour_sems.at[0, part, index],
            (down_sems if hop == 2 else detour_sems).at[1, part, index],
            down_way.next_place(hop),
        )

    def pass_on(index, part):
        for hop in (1, 2):
            @pl.when(stops(index, part)[hop])
            def _(hop=hop):
                detour_hop(hop - 1, index, part).wait_recv()
                detour_hop(hop, index, part).start()

    needs = (sends_down & sends_right, sends_down)
    takes = (takes_above & sends_right, takes_above)

    def straight(index, part):
        return needs[part] & jnp.logical_not(stops(index, part)[0])

    def send_down(index, part):
        @pl.when(straight(index, part))
        def _():
            down(index, part).start()

        @pl.when(stops(index, part)[0])
        def _():
            detour_hop(0, index, part).start()

    def right(index):
        start, rows = CHUNKS[index]
        if index in LOWS:
            source = grad_ref.at[:, pl.ds(3, 2), pl.ds(start, rows), :]
        else:
            source = joined.at[:, :, pl.ds(start, rows), :]
        return remote(
            source, from_left.at[:, :, pl.ds(start, rows), :],
            right_sems.at[0, index], right_sems.at[1, index],
            (row, jnp.minimum(col + 1, N_COL - 1)),
        )

    def send_right(index):
        @pl.when(sends_right)
        def _():
            right(index).start()

    def join(index):
        start, rows = CHUNKS[index]
        at = slice(start, start + rows)

        @pl.when(takes[0])
        def _():
            down(index, 0).wait_recv()

        for channel in range(2):
            for block in range(2):
                joined[channel, block, at] = (
                    grad_ref[channel, 3 + block, at] + from_above[channel, 3 + block, at])
        send_right(index)

    def update(index):
        start, rows = CHUNKS[index]
        at = slice(start, start + rows)
        if index < TOPS:
            @pl.when(takes_above)
            def _():
                down(index, 1).wait_recv()

        @pl.when(takes_left)
        def _():
            right(index).wait_recv()

        for channel in range(2):
            for block in range(3):
                grad = grad_ref[channel, block, at]
                if index < TOPS:
                    grad = grad + from_above[channel, block, at]
                if block < 2:
                    grad = grad + from_left[channel, block, at]
                value = object_ref[channel, block, at] - 0.1 * grad
                if refetch:
                    out_ref[channel, block, at] = value
                else:
                    out_ref[channel, at, block * 128:block * 128 + 128] = value
        if refetch:
            halo.send_left(index)
            if index < TOPS:
                halo.send_up(index)

    def forward(index):
        if refetch:
            halo.forward_corner(index)

    def pass_up(index):
        if refetch:
            halo.pass_on(index)

    reduce.begin()
    send_right(4)
    send_down(0, 0)
    reduce.to_plane()
    send_right(5)
    send_down(1, 0)
    send_down(2, 0)
    send_down(3, 0)
    for index in range(TOPS):
        send_down(index, 1)
    pass_on(0, 0)
    pass_on(1, 0)
    update(4)
    reduce.to_z()
    late = down_way.stops[3]
    on_time = jnp.logical_not(late)
    pl.when(late)(reduce.from_z)
    join(0)
    join(1)
    pass_on(2, 0)
    pass_on(3, 0)
    join(2)
    join(3)
    pass_on(0, 1)
    pass_on(1, 1)
    if refetch:
        pl.when(late)(reduce.from_plane)
        update(0)
        pl.when(on_time)(reduce.from_z)
        update(1)
        pass_on(2, 1)
        pass_on(3, 1)
        forward(0)
        update(2)
        forward(1)
        update(3)
        update(5)
        pl.when(on_time)(reduce.from_plane)
        pass_up(0)
        pass_up(1)
        forward(2)
        forward(3)
        pass_up(2)
        pass_up(3)
    else:
        update(5)
        pl.when(on_time)(reduce.from_z)
        pl.when(late)(reduce.from_plane)
        pass_on(2, 1)
        pass_on(3, 1)
        update(0)
        update(1)
        pl.when(on_time)(reduce.from_plane)
        update(2)
        update(3)
    reduce.end()
    step_size = 0.5 / math.sqrt(N_ROW * N_COL * 8)
    probe_out[...] = probe_ref[...] - step_size * sums[...]
    if refetch:
        halo.finish()
    reduce.drain()
    for index, part in [(index, part) for part in range(2) for index in range(TOPS)]:
        @pl.when(straight(index, part))
        def _(index=index, part=part):
            down(index, part).wait_send()

        for hop in range(3):
            @pl.when(stops(index, part)[hop])
            def _(hop=hop, index=index, part=part):
                detour_hop(hop, index, part).wait_send()

    @pl.when(sends_right)
    def _():
        for index in range(EVERY):
            right(index).wait_send()


def exchange(refetch, ext, grad, probe, probe_grad):
    dma = pltpu.SemaphoreType.DMA
    out = (2, 5, EXT, 128) if refetch else (2, TILE, TILE)
    return pl.pallas_call(
        functools.partial(exchange_kernel, refetch),
        name=f"exchange{int(refetch)}",
        out_shape=(
            jax.ShapeDtypeStruct(out, F32), jax.ShapeDtypeStruct((2, PROBE, PROBE), F32)),
        in_specs=[VMEM_SPEC] * 4,
        out_specs=(VMEM_SPEC, VMEM_SPEC),
        scratch_shapes=[
            pltpu.VMEM((2, 5, 256, 128), F32),
            pltpu.VMEM((2, 2, TILE, 128), F32),
            pltpu.VMEM((2, 2, 256, 128), F32),
            pltpu.VMEM((256, 256), F32),
            pltpu.VMEM((256, 256), F32),
            pltpu.VMEM((15, 16, 256), F32),
            pltpu.VMEM((8, 16, 256), F32),
            pltpu.VMEM((2, 256, 256), F32),
            pltpu.VMEM((2, 5, 256, 128), F32),
            dma((2, 2, TOPS)),
            dma((2, EVERY)),
            dma((2, 39)),
            dma((2, 2, TOPS)),
        ] + (halo_sems() if refetch else []),
        compiler_params=pltpu.CompilerParams(
            collective_id=1 + int(refetch), has_side_effects=True,
            vmem_limit_bytes=EXCHANGE_VMEM),
    )(ext, grad, probe, probe_grad)


def per_device(object_field, illumination, measured, positions, frame_counts, first_count):
    tables = jnp.asarray(dft_tables())
    positions = positions[0, 0].T
    probe = illumination
    ext, ordered = fetch(object_field, measured[0, 0])
    grad, probe_grad = frames(
        0, frame_counts, first_count, positions, ext, probe, ordered, tables)
    ext, probe = exchange(True, ext, grad, probe, probe_grad)
    grad, probe_grad = frames(
        1, frame_counts, first_count, positions, ext, probe, ordered, tables)
    new_object, probe = exchange(False, ext, grad, probe, probe_grad)
    return new_object, probe


def solution(mesh):
    in_specs = (
        P(None, "row", "col"),
        P(),
        P("row", "col", None, None, None),
        P("row", "col", None, None),
        P("row", "col"),
        P("row", "col"),
    )
    out_specs = (P(None, "row", "col"), P())
    return jax.shard_map(
        per_device, mesh=mesh, in_specs=in_specs, out_specs=out_specs, check_vma=False
    )
```

```python
import functools
import math

import jax
import jax.numpy as jnp
import numpy as np
from jax import lax
from jax.experimental import pallas as pl
from jax.experimental.pallas import tpu as pltpu
from jax.sharding import PartitionSpec as P

MESH = pl.DeviceIdType.MESH
TILE, PROBE, EXT = 384, 256, 640
N_ROW = N_COL = 16
F32, BF16 = jnp.float32, jnp.bfloat16
FETCH_VMEM, FRAMES_VMEM, EXCHANGE_VMEM = 14 << 20, 16 << 20, 18 << 20
VMEM_SPEC = pl.BlockSpec(memory_space=pltpu.VMEM)
SMEM_SPEC = pl.BlockSpec(memory_space=pltpu.SMEM)
HBM_SPEC = pl.BlockSpec(memory_space=pltpu.HBM)


def split_bf16(table):
    high = table.astype(np.float32).astype(BF16)
    low = (table - high.astype(np.float64)).astype(np.float32).astype(BF16)
    return high, low


def dft_tables():
    n = np.arange(128)[:, None]
    parts = []
    for parity in (0, 1):
        k = 2 * np.arange(128)[None, :] + parity
        angle = ((n * k) % 256) * (2.0 * np.pi / 256.0)
        c, s = np.cos(angle) / 16.0, np.sin(angle) / 16.0
        table = np.block([[c, -s], [s, c]])
        parts.append((split_bf16(table), split_bf16(table.T)))
    order = []
    for transposed in (0, 1):
        for parity in (0, 1):
            order.extend(parts[parity][transposed])
    return np.stack(order)


def deinterleave_table():
    row = lax.broadcasted_iota(jnp.int32, (256, 256), 0)
    col = lax.broadcasted_iota(jnp.int32, (256, 256), 1)
    source = jnp.where(col < 128, 2 * col, 2 * col - 255)
    return jnp.where(row == source, 1.0, 0.0).astype(BF16)


def place():
    row, col = lax.axis_index("row"), lax.axis_index("col")
    return row, col


def remote(src, dst, send_sem, recv_sem, device):
    return pltpu.make_async_remote_copy(
        src_ref=src, dst_ref=dst, send_sem=send_sem, recv_sem=recv_sem,
        device_id=device, device_id_type=MESH,
    )


UP_DETOURS = (((8, 15), (14, 15), (6, 7), (7, 15)),)
DOWN_DETOURS = (((7, 0), (1, 0), (9, 8), (8, 0)), ((7, 15), (1, 15), (9, 7), (8, 15)))


def is_at(row, col, device):
    return (row == device[0]) & (col == device[1])


def place_of(device):
    return jnp.int32(device[0]), jnp.int32(device[1])


class Detour:
    def __init__(self, paths, row, col):
        self.paths, self.row, self.col = paths, row, col
        self.each = [[is_at(row, col, path[stop]) for stop in range(4)] for path in paths]
        self.stops = [functools.reduce(jnp.logical_or, marks) for marks in zip(*self.each)]

    def next_place(self, hop):
        row, col = place_of(self.paths[0][hop + 1])
        for path in self.paths[1:]:
            other_row, other_col = place_of(path[hop + 1])
            here = is_at(self.row, self.col, path[hop])
            row, col = jnp.where(here, other_row, row), jnp.where(here, other_col, col)
        return row, col

    def greet(self, barrier):
        for path in self.paths:
            for hop in range(3):
                for here, there in ((path[hop], path[hop + 1]), (path[hop + 1], path[hop])):
                    @pl.when(is_at(self.row, self.col, here))
                    def _(there=there):
                        pl.semaphore_signal(
                            barrier, inc=1, device_id=place_of(there), device_id_type=MESH)

    def count(self):
        one, two, none = jnp.int32(1), jnp.int32(2), jnp.int32(0)
        return jnp.where(self.stops[0] | self.stops[3], one, none) + jnp.where(
            self.stops[1] | self.stops[2], two, none)


def greet_neighbours(barrier, row, col):
    for has, device in (
        (row > 0, (row - 1, col)),
        (row < N_ROW - 1, (row + 1, col)),
        (col > 0, (row, col - 1)),
        (col < N_COL - 1, (row, col + 1)),
    ):
        @pl.when(has)
        def _(device=device):
            pl.semaphore_signal(barrier, inc=1, device_id=device, device_id_type=MESH)


def neighbour_count(row, col):
    one, none = jnp.int32(1), jnp.int32(0)
    has = (row > 0, row < N_ROW - 1, col > 0, col < N_COL - 1)
    return sum(jnp.where(h, one, none) for h in has)


CHUNKS = ((0, 64), (64, 64), (128, 64), (192, 64), (256, 64), (320, 64))
TOPS = 4
LOWS = (4, 5)
EVERY = 6


class Halo:
    def __init__(self, ext, way, detours, detour, left_sems, up_sems, corner_sems, detour_sems,
                 row, col):
        self.ext, self.row, self.col = ext, row, col
        self.left_sems, self.up_sems, self.corner_sems = left_sems, up_sems, corner_sems
        self.detour, self.detour_sems = detour, detour_sems
        self.way, self.stops = way, way.stops if detours else [row < 0] * 4
        self.sends_left, self.takes_right = col > 0, col < N_COL - 1
        self.sends_up, self.takes_below = row > 0, row < N_ROW - 1
        self.sends_direct = self.sends_up & jnp.logical_not(self.stops[0])

    def left(self, index):
        start, rows = CHUNKS[index]
        return remote(
            self.ext.at[:, pl.ds(0, 2), pl.ds(start, rows), :],
            self.ext.at[:, pl.ds(3, 2), pl.ds(start, rows), :],
            self.left_sems.at[0, index], self.left_sems.at[1, index],
            (self.row, jnp.maximum(self.col - 1, 0)),
        )

    def over(self, index, blocks, sems):
        start, rows = CHUNKS[index]
        return remote(
            self.ext.at[:, blocks, pl.ds(start, rows), :],
            self.ext.at[:, blocks, pl.ds(384 + start, rows), :],
            sems.at[0, index], sems.at[1, index],
            (jnp.maximum(self.row - 1, 0), self.col),
        )

    def up(self, index):
        return self.over(index, pl.ds(0, 3), self.up_sems)

    def corner(self, index):
        return self.over(index, pl.ds(3, 2), self.corner_sems)

    def detour_hop(self, hop, index):
        start, rows = CHUNKS[index]
        first, last = hop == 0, hop == 2
        source = self.ext if first else self.detour
        target = self.ext.at[:, pl.ds(0, 3), pl.ds(384 + start, rows), :] if last else (
            self.detour.at[:, :, pl.ds(start, rows), :])
        return remote(
            source.at[:, pl.ds(0, 3), pl.ds(start, rows), :], target,
            self.detour_sems.at[0, index],
            self.up_sems.at[1, index] if last else self.detour_sems.at[1, index],
            self.way.next_place(hop),
        )

    def pass_on(self, index):
        for hop in (1, 2):
            @pl.when(self.stops[hop])
            def _(hop=hop):
                self.detour_hop(hop - 1, index).wait_recv()
                self.detour_hop(hop, index).start()

    def clear_edges(self):
        @pl.when(self.col == N_COL - 1)
        def _():
            for channel in range(2):
                for block in (3, 4):
                    self.ext[channel, block] = jnp.zeros((EXT, 128), F32)

        @pl.when(self.row == N_ROW - 1)
        def _():
            for channel in range(2):
                for block in range(5):
                    self.ext[channel, block, 384:640] = jnp.zeros((256, 128), F32)

    def send_left(self, index):
        @pl.when(self.sends_left)
        def _():
            self.left(index).start()

    def send_up(self, index):
        @pl.when(self.sends_direct)
        def _():
            self.up(index).start()

        @pl.when(self.stops[0])
        def _():
            self.detour_hop(0, index).start()

    def forward_corner(self, index):
        @pl.when(self.takes_right)
        def _():
            self.left(index).wait_recv()

            @pl.when(self.sends_up)
            def _():
                self.corner(index).start()

    def finish(self):
        @pl.when(self.takes_right)
        def _():
            for index in LOWS:
                self.left(index).wait_recv()

        @pl.when(self.takes_below)
        def _():
            for index in range(TOPS):
                self.up(index).wait_recv()

        @pl.when(self.takes_below & self.takes_right)
        def _():
            for index in range(TOPS):
                self.corner(index).wait_recv()

        @pl.when(self.sends_left)
        def _():
            for index in range(EVERY):
                self.left(index).wait_send()

        @pl.when(self.sends_direct)
        def _():
            for index in range(TOPS):
                self.up(index).wait_send()

        for hop in range(3):
            @pl.when(self.stops[hop])
            def _(hop=hop):
                for index in range(TOPS):
                    self.detour_hop(hop, index).wait_send()

        @pl.when(self.sends_up & self.takes_right)
        def _():
            for index in range(TOPS):
                self.corner(index).wait_send()


def halo_sems():
    dma = pltpu.SemaphoreType.DMA
    return [pltpu.VMEM((2, 3, 256, 128), F32), dma((2, EVERY)), dma((2, TOPS)), dma((2, TOPS)),
            dma((2, TOPS))]


def fetch_kernel(object_ref, measured_ref, ext_ref, sorted_ref,
                 order, turned, measured, load_sems, *sems):
    row, col = place()
    barrier = pltpu.get_barrier_semaphore()
    greet_neighbours(barrier, row, col)
    way = Detour(UP_DETOURS, row, col)
    way.greet(barrier)
    loads = []
    for channel in range(2):
        for block in range(3):
            load = pltpu.make_async_copy(
                object_ref.at[channel, :, pl.ds(block * 128, 128)],
                ext_ref.at[channel, block, pl.ds(0, TILE), :],
                load_sems.at[channel * 3 + block],
            )
            load.start()
            loads.append(load)
    load_frames = pltpu.make_async_copy(measured_ref, measured, load_sems.at[6])
    load_frames.start()
    halo = Halo(ext_ref, way, True, *sems, row, col)
    halo.clear_edges()
    for load in loads:
        load.wait()
    pl.semaphore_wait(barrier, neighbour_count(row, col) + way.count())
    for index in range(EVERY):
        halo.send_left(index)
    for index in range(TOPS):
        halo.send_up(index)

    def sort_frame(frame, carry):
        value = measured[frame]
        total = jnp.zeros((256, 256), F32)
        for _ in range(3):
            piece = value.astype(BF16)
            value = value - piece.astype(F32)
            total = total + jnp.dot(piece, order[...], preferred_element_type=F32)
        for block in range(2):
            turned[block] = total[:, block * 128:block * 128 + 128]
        for block in range(2):
            for parity in range(2):
                sorted_ref[frame, parity, :, block * 128:block * 128 + 128] = (
                    turned[block, pl.ds(parity, 128, stride=2), :])
        return carry

    order[...] = deinterleave_table()
    load_frames.wait()
    share = measured.shape[0] // TOPS
    for index in range(TOPS):
        lax.fori_loop(index * share, (index + 1) * share, sort_frame, 0)
        halo.pass_on(index)
        halo.forward_corner(index)
    halo.finish()


def fetch(object_field, measured):
    dma = pltpu.SemaphoreType.DMA
    count = measured.shape[0]
    return pl.pallas_call(
        fetch_kernel,
        name="fetch",
        out_shape=(
            jax.ShapeDtypeStruct((2, 5, EXT, 128), F32),
            jax.ShapeDtypeStruct((count, 2, 128, 256), F32),
        ),
        in_specs=[HBM_SPEC, HBM_SPEC],
        out_specs=(VMEM_SPEC, VMEM_SPEC),
        scratch_shapes=[
            pltpu.VMEM((256, 256), BF16), pltpu.VMEM((2, 256, 128), F32),
            pltpu.VMEM((count, 256, 256), F32), dma((7,)),
        ] + halo_sems(),
        compiler_params=pltpu.CompilerParams(
            collective_id=0, has_side_effects=True, vmem_limit_bytes=FETCH_VMEM),
    )(*(pltpu.with_memory_space_constraint(a, pltpu.HBM) for a in (object_field, measured)))


def halves(value):
    high = value.astype(BF16)
    low = (value - high.astype(F32)).astype(BF16)
    return high, low


def dot(left, right):
    return jnp.dot(left, right, preferred_element_type=F32)


def times_table(value, tables, index):
    high, low = halves(value)
    return dot(high, tables[index]) + dot(low, tables[index]) + dot(high, tables[index + 1])


def table_times(tables, index, value):
    high, low = halves(value)
    return dot(tables[index], high) + dot(tables[index + 1], high) + dot(tables[index], low)


def beside(a, b):
    return jnp.concatenate([a, b], axis=1)


def above(a, b):
    return jnp.concatenate([a, b], axis=0)


def frames_kernel(batch, counts_ref, first_ref, positions_ref, ext_ref, probe_ref, sorted_ref,
                  tables, grad_ref, probe_grad_ref):
    live = counts_ref[0, 0]
    first = jnp.minimum(first_ref[0, 0], live)
    start, end = (0, first) if batch == 0 else (first, live)
    for channel in range(2):
        for block in range(5):
            grad_ref[channel, block] = jnp.zeros((EXT, 128), F32)
    probe_grad_ref[...] = jnp.zeros_like(probe_grad_ref)
    lanes = lax.broadcasted_iota(jnp.int32, (256, 128), 1)

    def load_window(frame):
        row_start, col_start = positions_ref[0, frame], positions_ref[1, frame]
        block0 = col_start // 128
        shift = col_start - block0 * 128
        rows = pl.ds(row_start, 256)
        back_shift = jnp.bitwise_and(128 - shift, 127)
        keep = lanes < 128 - shift
        window = []
        for channel in range(2):
            turned = [
                pltpu.roll(ext_ref[channel, block0 + block, rows, :], back_shift, 1)
                for block in range(3)
            ]
            window.append([jnp.where(keep, turned[b], turned[b + 1]) for b in range(2)])
        return window, block0, shift, rows

    def load_probe():
        return [[probe_ref[channel, :, b * 128:b * 128 + 128] for b in range(2)]
                for channel in range(2)]

    def stacked(t0, t1):
        return above(beside(t0[:, :128], t1[:, :128]), beside(t0[:, 128:], t1[:, 128:]))

    def across(window):
        probe = load_probe()
        re = [probe[0][b] * window[0][b] - probe[1][b] * window[1][b] for b in range(2)]
        im = [probe[0][b] * window[1][b] + probe[1][b] * window[0][b] for b in range(2)]
        return (times_table(beside(re[0] + re[1], im[0] + im[1]), tables, 0),
                times_table(beside(re[0] - re[1], im[0] - im[1]), tables, 2))

    def along(y):
        y0, y1 = y
        return (table_times(tables, 4, stacked(y0[:128] + y0[128:], y1[:128] + y1[128:])),
                table_times(tables, 6, stacked(y0[:128] - y0[128:], y1[:128] - y1[128:])))

    def along_back(w, frame, valid):
        parts = []
        for parity in range(2):
            re, im = w[parity][:128], w[parity][128:]
            residue = re * re + im * im - sorted_ref[frame, parity]
            residue = jnp.where(valid, residue, jnp.zeros_like(residue))
            parts.append(table_times(tables, 2 * parity, above(residue * re, residue * im)))
        return parts

    def across_back(u):
        top, bottom = u[0] + u[1], u[0] - u[1]
        z_re = above(top[:128], bottom[:128])
        z_im = above(top[128:], bottom[128:])
        v0 = times_table(beside(z_re[:, :128], z_im[:, :128]), tables, 4)
        v1 = times_table(beside(z_re[:, 128:], z_im[:, 128:]), tables, 6)
        return ([v0[:, :128] + v1[:, :128], v0[:, :128] - v1[:, :128]],
                [v0[:, 128:] + v1[:, 128:], v0[:, 128:] - v1[:, 128:]])

    def add_probe_terms(windows, backs):
        for b in range(2):
            at = slice(b * 128, b * 128 + 128)
            re, im = probe_grad_ref[0, :, at], probe_grad_ref[1, :, at]
            for window, (back_re, back_im) in zip(windows, backs):
                re = re + (window[0][b] * back_re[b] + window[1][b] * back_im[b])
                im = im + (window[0][b] * back_im[b] - window[1][b] * back_re[b])
            probe_grad_ref[0, :, at] = re
            probe_grad_ref[1, :, at] = im

    def add_object_terms(place, back):
        block0, shift, rows = place
        back_re, back_im = back
        probe = load_probe()
        before = lanes < shift
        zero = jnp.zeros((256, 128), F32)
        for channel in range(2):
            if channel == 0:
                term = [probe[0][b] * back_re[b] + probe[1][b] * back_im[b] for b in range(2)]
            else:
                term = [probe[0][b] * back_im[b] - probe[1][b] * back_re[b] for b in range(2)]
            turned = [pltpu.roll(term[b], shift, 1) for b in range(2)]
            adds = [
                jnp.where(before, zero, turned[0]),
                jnp.where(before, turned[0], turned[1]),
                jnp.where(before, turned[1], zero),
            ]
            for block in range(3):
                at = (channel, block0 + block, rows, slice(None))
                grad_ref[at] = grad_ref[at] + adds[block]

    last = positions_ref.shape[1] - 1

    def add_pair(pair, carry):
        slots = [start + pair * 2 + k for k in range(2)]
        valid = [slot < end for slot in slots]
        slots = [jnp.minimum(slot, last) for slot in slots]
        windows, places = [], []
        for slot in slots:
            window, *spot = load_window(slot)
            windows.append(window)
            places.append(spot)
        y = [across(window) for window in windows]
        w = [along(each) for each in y]
        u = [along_back(w[k], slots[k], valid[k]) for k in range(2)]
        backs = [across_back(each) for each in u]
        add_probe_terms(windows, backs)
        for k in range(2):
            add_object_terms(places[k], backs[k])
        return carry

    lax.fori_loop(0, (end - start + 1) // 2, add_pair, 0)


def frames(batch, counts, first, positions, ext, probe, ordered, tables):
    return pl.pallas_call(
        functools.partial(frames_kernel, batch),
        name=f"frames{batch}",
        out_shape=(
            jax.ShapeDtypeStruct((2, 5, EXT, 128), F32),
            jax.ShapeDtypeStruct((2, PROBE, PROBE), F32),
        ),
        in_specs=[SMEM_SPEC, SMEM_SPEC, SMEM_SPEC] + [VMEM_SPEC] * 4,
        out_specs=(VMEM_SPEC, VMEM_SPEC),
        compiler_params=pltpu.CompilerParams(vmem_limit_bytes=FRAMES_VMEM),
    )(counts, first, positions, ext, probe, ordered, tables)


AROUND = tuple((i, j) for i in range(4) for j in range(4) if i or j)


class Reduce:
    def __init__(self, grad, half, got_half, got_plane, got_z, sums, sems, row, col):
        self.grad, self.half, self.got_half = grad, half, got_half
        self.got_plane, self.got_z, self.sums, self.sems = got_plane, got_z, sums, sems
        self.row, self.col, self.core = row, col, row % 2
        self.y = (row % 8) // 2
        self.x = (row // 8) * 2 + col // 8
        self.z = col % 8

    def partner(self):
        return (self.row + 1 - 2 * self.core, self.col)

    def plane(self, i, j):
        x, y = (self.x + i) % 4, (self.y + j) % 4
        device = ((x // 2) * 8 + y * 2 + self.core, (x % 2) * 8 + self.z)
        return pl.ds(pl.multiple_of((x * 4 + y) * 16, 16), 16), device

    def over_z_to(self, step):
        z = (self.z + step) % 8
        return z, (self.row, (self.col // 8) * 8 + z)

    def peers(self):
        found = [self.partner()]
        found += [self.plane(i, j)[1] for i, j in AROUND]
        found += [self.over_z_to(step)[1] for step in range(1, 8)]
        return found

    def copy(self, src, dst, index, device):
        return remote(src, dst, self.sems.at[0, index], self.sems.at[1, index], device)

    def pair(self):
        return self.copy(self.grad.at[1 - self.core], self.got_half, 0, self.partner())

    def out(self, n):
        rows, device = self.plane(*AROUND[n])
        return self.copy(self.half.at[rows, :], self.got_plane.at[n], 1 + n, device)

    def along(self, step):
        return self.copy(
            self.got_z.at[self.z], self.got_z.at[self.z], 15 + step, self.over_z_to(step)[1])

    def back(self, n):
        rows = self.plane(0, 0)[0]
        mine = self.sums.at[self.core, rows, :]
        return self.copy(mine, mine, 23 + n, self.plane(*AROUND[n])[1])

    def back_pair(self):
        mine = self.sums.at[self.core]
        return self.copy(mine, mine, 38, self.partner())

    def begin(self):
        self.pair().start()

    def to_plane(self):
        self.pair().wait_recv()
        self.half[...] = self.grad[self.core] + self.got_half[...]
        for n in range(15):
            self.out(n).start()

    def to_z(self):
        for n in range(15):
            self.out(n).wait_recv()
        total = self.half[self.plane(0, 0)[0], :]
        for n in range(15):
            total = total + self.got_plane[n]
        self.got_z[self.z] = total
        for step in range(1, 8):
            self.along(step).start()

    def from_z(self):
        for step in range(1, 8):
            theirs = self.got_z.at[(self.z + 8 - step) % 8]
            self.copy(theirs, theirs, 15 + step, self.over_z_to(step)[1]).wait_recv()
        total = self.got_z[0]
        for z in range(1, 8):
            total = total + self.got_z[z]
        self.sums[self.core, self.plane(0, 0)[0], :] = total
        for n in range(15):
            self.back(n).start()

    def from_plane(self):
        for n in range(15):
            i, j = AROUND[n]
            theirs = self.sums.at[self.core, self.plane(4 - i, 4 - j)[0], :]
            self.copy(theirs, theirs, 23 + n, self.plane(i, j)[1]).wait_recv()
        self.back_pair().start()

    def end(self):
        theirs = self.sums.at[1 - self.core]
        self.copy(theirs, theirs, 38, self.partner()).wait_recv()

    def drain(self):
        self.pair().wait_send()
        for n in range(15):
            self.out(n).wait_send()
            self.back(n).wait_send()
        for step in range(1, 8):
            self.along(step).wait_send()
        self.back_pair().wait_send()


def exchange_kernel(refetch, object_ref, grad_ref, probe_ref, probe_grad_ref, out_ref, probe_out,
                    from_above, from_left, joined, half, got_half, got_plane, got_z, sums,
                    detour, down_sems, right_sems, reduce_sems, detour_sems, *sems):
    row, col = place()
    reduce = Reduce(
        probe_grad_ref, half, got_half, got_plane, got_z, sums, reduce_sems, row, col)
    barrier = pltpu.get_barrier_semaphore()
    greet_neighbours(barrier, row, col)
    down_way = Detour(DOWN_DETOURS if refetch else DOWN_DETOURS[:1], row, col)
    down_way.greet(barrier)
    if refetch:
        up_way = Detour(UP_DETOURS, row, col)
    for device in reduce.peers():
        pl.semaphore_signal(barrier, inc=1, device_id=device, device_id_type=MESH)

    def stops(index, part):
        first, second = down_way.each[0], down_way.each[-1]
        if part == 0 or not refetch:
            return first
        return second

    sends_down, takes_above = row < N_ROW - 1, row > 0
    sends_right, takes_left = col < N_COL - 1, col > 0
    if refetch:
        halo = Halo(out_ref, up_way, False, *sems, row, col)
        halo.clear_edges()

    @pl.when((row == 0) | (col == N_COL - 1))
    def _():
        for channel in range(2):
            for block in (3, 4):
                from_above[channel, block] = jnp.zeros((256, 128), F32)

    @pl.when(row == 0)
    def _():
        for channel in range(2):
            for block in range(3):
                from_above[channel, block] = jnp.zeros((256, 128), F32)

    @pl.when(col == 0)
    def _():
        for channel in range(2):
            for block in range(2):
                from_left[channel, block] = jnp.zeros((TILE, 128), F32)

    greeted = 23 + neighbour_count(row, col) + down_way.count()
    pl.semaphore_wait(barrier, greeted)

    def down(index, part):
        blocks = pl.ds(3, 2) if part == 0 else pl.ds(0, 3)
        start, rows = CHUNKS[index]
        return remote(
            grad_ref.at[:, blocks, pl.ds(384 + start, rows), :],
            from_above.at[:, blocks, pl.ds(start, rows), :],
            down_sems.at[0, part, index], down_sems.at[1, part, index],
            (jnp.minimum(row + 1, N_ROW - 1), col),
        )

    def detour_hop(hop, index, part):
        start, rows = CHUNKS[index]
        blocks = pl.ds(3, 2) if part == 0 else pl.ds(0, 3)
        here = pl.ds(start, rows)
        source = detour.at[:, blocks, here, :] if hop else (
            grad_ref.at[:, blocks, pl.ds(384 + start, rows), :])
        target = (from_above if hop == 2 else detour).at[:, blocks, here, :]
        return remote(
            source, target, detour_sems.at[0, part, index],
            (down_sems if hop == 2 else detour_sems).at[1, part, index],
            down_way.next_place(hop),
        )

    def pass_on(index, part):
        for hop in (1, 2):
            @pl.when(stops(index, part)[hop])
            def _(hop=hop):
                detour_hop(hop - 1, index, part).wait_recv()
                detour_hop(hop, index, part).start()

    needs = (sends_down & sends_right, sends_down)
    takes = (takes_above & sends_right, takes_above)

    def straight(index, part):
        return needs[part] & jnp.logical_not(stops(index, part)[0])

    def send_down(index, part):
        @pl.when(straight(index, part))
        def _():
            down(index, part).start()

        @pl.when(stops(index, part)[0])
        def _():
            detour_hop(0, index, part).start()

    def right(index):
        start, rows = CHUNKS[index]
        if index in LOWS:
            source = grad_ref.at[:, pl.ds(3, 2), pl.ds(start, rows), :]
        else:
            source = joined.at[:, :, pl.ds(start, rows), :]
        return remote(
            source, from_left.at[:, :, pl.ds(start, rows), :],
            right_sems.at[0, index], right_sems.at[1, index],
            (row, jnp.minimum(col + 1, N_COL - 1)),
        )

    def send_right(index):
        @pl.when(sends_right)
        def _():
            right(index).start()

    def join(index):
        start, rows = CHUNKS[index]
        at = slice(start, start + rows)

        @pl.when(takes[0])
        def _():
            down(index, 0).wait_recv()

        for channel in range(2):
            for block in range(2):
                joined[channel, block, at] = (
                    grad_ref[channel, 3 + block, at] + from_above[channel, 3 + block, at])
        send_right(index)

    def update(index):
        start, rows = CHUNKS[index]
        at = slice(start, start + rows)
        if index < TOPS:
            @pl.when(takes_above)
            def _():
                down(index, 1).wait_recv()

        @pl.when(takes_left)
        def _():
            right(index).wait_recv()

        for channel in range(2):
            for block in range(3):
                grad = grad_ref[channel, block, at]
                if index < TOPS:
                    grad = grad + from_above[channel, block, at]
                if block < 2:
                    grad = grad + from_left[channel, block, at]
                value = object_ref[channel, block, at] - 0.1 * grad
                if refetch:
                    out_ref[channel, block, at] = value
                else:
                    out_ref[channel, at, block * 128:block * 128 + 128] = value
        if refetch:
            halo.send_left(index)
            if index < TOPS:
                halo.send_up(index)

    def forward(index):
        if refetch:
            halo.forward_corner(index)

    reduce.begin()
    send_right(4)
    send_down(0, 0)
    reduce.to_plane()
    send_right(5)
    send_down(1, 0)
    send_down(2, 0)
    send_down(3, 0)
    for index in range(TOPS):
        send_down(index, 1)
    pass_on(0, 0)
    pass_on(1, 0)
    update(4)
    reduce.to_z()
    late = down_way.stops[3]
    on_time = jnp.logical_not(late)
    pl.when(late)(reduce.from_z)
    join(0)
    join(1)
    pass_on(2, 0)
    pass_on(3, 0)
    join(2)
    join(3)
    pass_on(0, 1)
    pass_on(1, 1)
    if refetch:
        pl.when(late)(reduce.from_plane)
        update(0)
        pl.when(on_time)(reduce.from_z)
        update(1)
        pass_on(2, 1)
        pass_on(3, 1)
        forward(0)
        update(2)
        forward(1)
        update(3)
        update(5)
        pl.when(on_time)(reduce.from_plane)
        forward(2)
        forward(3)
    else:
        update(5)
        pl.when(on_time)(reduce.from_z)
        pl.when(late)(reduce.from_plane)
        pass_on(2, 1)
        pass_on(3, 1)
        update(0)
        update(1)
        pl.when(on_time)(reduce.from_plane)
        update(2)
        update(3)
    reduce.end()
    step_size = 0.5 / math.sqrt(N_ROW * N_COL * 8)
    probe_out[...] = probe_ref[...] - step_size * sums[...]
    if refetch:
        halo.finish()
    reduce.drain()
    for index, part in [(index, part) for part in range(2) for index in range(TOPS)]:
        @pl.when(straight(index, part))
        def _(index=index, part=part):
            down(index, part).wait_send()

        for hop in range(3):
            @pl.when(stops(index, part)[hop])
            def _(hop=hop, index=index, part=part):
                detour_hop(hop, index, part).wait_send()

    @pl.when(sends_right)
    def _():
        for index in range(EVERY):
            right(index).wait_send()


def exchange(refetch, ext, grad, probe, probe_grad):
    dma = pltpu.SemaphoreType.DMA
    out = (2, 5, EXT, 128) if refetch else (2, TILE, TILE)
    return pl.pallas_call(
        functools.partial(exchange_kernel, refetch),
        name=f"exchange{int(refetch)}",
        out_shape=(
            jax.ShapeDtypeStruct(out, F32), jax.ShapeDtypeStruct((2, PROBE, PROBE), F32)),
        in_specs=[VMEM_SPEC] * 4,
        out_specs=(VMEM_SPEC, VMEM_SPEC),
        scratch_shapes=[
            pltpu.VMEM((2, 5, 256, 128), F32),
            pltpu.VMEM((2, 2, TILE, 128), F32),
            pltpu.VMEM((2, 2, 256, 128), F32),
            pltpu.VMEM((256, 256), F32),
            pltpu.VMEM((256, 256), F32),
            pltpu.VMEM((15, 16, 256), F32),
            pltpu.VMEM((8, 16, 256), F32),
            pltpu.VMEM((2, 256, 256), F32),
            pltpu.VMEM((2, 5, 256, 128), F32),
            dma((2, 2, TOPS)),
            dma((2, EVERY)),
            dma((2, 39)),
            dma((2, 2, TOPS)),
        ] + (halo_sems() if refetch else []),
        compiler_params=pltpu.CompilerParams(
            collective_id=1 + int(refetch), has_side_effects=True,
            vmem_limit_bytes=EXCHANGE_VMEM),
    )(ext, grad, probe, probe_grad)


def per_device(object_field, illumination, measured, positions, frame_counts, first_count):
    tables = jnp.asarray(dft_tables())
    positions = positions[0, 0].T
    probe = illumination
    ext, ordered = fetch(object_field, measured[0, 0])
    grad, probe_grad = frames(
        0, frame_counts, first_count, positions, ext, probe, ordered, tables)
    ext, probe = exchange(True, ext, grad, probe, probe_grad)
    grad, probe_grad = frames(
        1, frame_counts, first_count, positions, ext, probe, ordered, tables)
    new_object, probe = exchange(False, ext, grad, probe, probe_grad)
    return new_object, probe


def solution(mesh):
    in_specs = (
        P(None, "row", "col"),
        P(),
        P("row", "col", None, None, None),
        P("row", "col", None, None),
        P("row", "col"),
        P("row", "col"),
    )
    out_specs = (P(None, "row", "col"), P())
    return jax.shard_map(
        per_device, mesh=mesh, in_specs=in_specs, out_specs=out_specs, check_vma=False
    )
```
